8 devices in a mesh: rep: 2 (over z, y), model: 4 (over x, core).
Axes of the slice: x: 2, y: 2, z: 1, core: 2. Of those that a mesh axis runs over, the one named last changes fastest.
Arguments:
- x_real: bfloat16 [1024, 1280], P('rep'), parts along dimension 0
- x_fake: bfloat16 [1024, 1280], P('rep'), parts along dimension 0
- weight0: bfloat16 [10240, 1280], P(('rep', 'model')), parts along dimension 0
- weight1: bfloat16 [2560, 5120], P(('rep', 'model')), parts along dimension 0
- weight2: bfloat16 [2560, 1280], P(('rep', 'model')), parts along dimension 0
- u_left0: float32 [10240], P(('rep', 'model')), parts along dimension 0
- u_left1: float32 [2560], P(('rep', 'model')), parts along dimension 0
- u_left2: float32 [2560], P(('rep', 'model')), parts along dimension 0
- t_real: bfloat16 [1024, 1280], P('rep', 'model'), parts along dimension 0
- t_fake: bfloat16 [1024, 1280], P('rep', 'model'), parts along dimension 0
Outputs:
- output 1: float32 [2], P('rep'), parts along dimension 0
- output 2: float32 [1024, 1280], P('rep'), parts along dimension 0
- output 3: float32 [1024, 1280], P('rep'), parts along dimension 0
- output 4: float32 [10240, 1280], P(('rep', 'model')), parts along dimension 0
- output 5: float32 [2560, 5120], P(('rep', 'model')), parts along dimension 0
- output 6: float32 [2560, 1280], P(('rep', 'model')), parts along dimension 0
- output 7: float32 [10240], P(('rep', 'model')), parts along dimension 0
- output 8: float32 [2560], P(('rep', 'model')), parts along dimension 0
- output 9: float32 [2560], P(('rep', 'model')), parts along dimension 0
- output 10: float32 [2560], P('rep'), parts along dimension 0
- output 11: float32 [10240], P('rep'), parts along dimension 0
- output 12: float32 [2560], P('rep'), parts along dimension 0
- output 13: float32 [6], P('rep'), parts along dimension 0
There are 2 independent parts. The reference program is written for one: setup_inputs(seed, part) draws one part's arguments, and reference() takes and returns one part's arrays. A program takes and returns all parts, laid end to end along the dimension named above; each array names one.
All inputs are finite; a program needn't handle non-finite values.
Results may differ from the reference program's by a relative error of at most 0.0189091.
Values are sent between devices in bfloat16 or wider.
A program may use at most 1 GiB of HBM per device.

```python
import math
import jax
import jax.numpy as jnp

ROWS = 512
D0 = 1280
D1 = 5120
D2 = 1280
D3 = 1280
SLOPE = 0.2
EPSILON = 1e-12


def spike_gain(d_out, d_in):
    strength = 1.0 + math.sqrt(d_out / d_in)
    top_value = math.sqrt((strength * strength + 1.0) * (strength * strength + d_out / d_in)) / strength
    return strength, top_value


def unit_vector(raw_vec):
    return raw_vec / jnp.sqrt(jnp.sum(raw_vec * raw_vec))


def spiked_layer(layer_key, d_out, d_in):
    key_bulk, key_left, key_right, key_other, key_mix = jax.random.split(layer_key, 5)
    strength, top_value = spike_gain(d_out, d_in)
    left_vec = unit_vector(jax.random.normal(key_left, (d_out,), jnp.float32))
    right_vec = unit_vector(jax.random.normal(key_right, (d_in,), jnp.float32))
    bulk_part = jax.random.normal(key_bulk, (d_out, d_in), jnp.float32) / math.sqrt(d_in)
    weight = bulk_part + strength * left_vec[:, None] * right_vec[None, :]
    other_vec = jax.random.normal(key_other, (d_out,), jnp.float32)
    other_vec = unit_vector(other_vec - jnp.sum(other_vec * left_vec) * left_vec)
    mix_cos = jax.random.uniform(key_mix, (), jnp.float32, 0.5, 0.8)
    u_left = mix_cos * left_vec + jnp.sqrt(1.0 - mix_cos * mix_cos) * other_vec
    return weight.astype(jnp.bfloat16), u_left, top_value


def setup_inputs(seed: int = 0, part: int = 0) -> dict:
    base_key = jax.random.fold_in(jax.random.key(seed), part)
    key_real, key_fake, key_treal, key_tfake, key_zero, key_one, key_two = jax.random.split(base_key, 7)
    widths = (D0, D1, D2, D3)
    layers = [spiked_layer(layer_key, widths[layer_no + 1], widths[layer_no]) for layer_no, layer_key in enumerate((key_zero, key_one, key_two))]
    x_scale = layers[0][2] * layers[1][2] * layers[2][2] / 0.52
    x_real = x_scale * jax.random.normal(key_real, (ROWS, D0), jnp.float32)
    x_fake = x_scale * jax.random.normal(key_fake, (ROWS, D0), jnp.float32)
    t_real = 1.0 + 0.5 * jax.random.normal(key_treal, (ROWS, D3), jnp.float32)
    t_fake = -1.0 + 0.5 * jax.random.normal(key_tfake, (ROWS, D3), jnp.float32)
    return {
        "x_real": x_real.astype(jnp.bfloat16),
        "x_fake": x_fake.astype(jnp.bfloat16),
        "weight0": layers[0][0],
        "weight1": layers[1][0],
        "weight2": layers[2][0],
        "u_left0": layers[0][1],
        "u_left1": layers[1][1],
        "u_left2": layers[2][1],
        "t_real": t_real.astype(jnp.bfloat16),
        "t_fake": t_fake.astype(jnp.bfloat16),
    }


def leaky_relu(values):
    return jnp.where(values > 0, values, SLOPE * values)


def leaky_slope(values):
    return jnp.where(values > 0, 1.0, SLOPE)


def power_step(weight, u_left):
    p_vec = jnp.dot(u_left.astype(jnp.bfloat16), weight, preferred_element_type=jnp.float32)
    v_new = p_vec / jnp.maximum(jnp.sqrt(jnp.sum(p_vec * p_vec)), EPSILON)
    s_vec = jnp.dot(weight, v_new.astype(jnp.bfloat16), preferred_element_type=jnp.float32)
    sigma_val = jnp.sqrt(jnp.sum(s_vec * s_vec))
    return s_vec / sigma_val, v_new, sigma_val


def reference(x_real, x_fake, weight0, weight1, weight2, u_left0, u_left1, u_left2, t_real, t_fake):
    weights = (weight0, weight1, weight2)
    powered = [power_step(weight, u_left) for weight, u_left in zip(weights, (u_left0, u_left1, u_left2))]
    layer_in = jnp.concatenate([x_real, x_fake], axis=0)
    inputs = []
    outputs = []
    for layer_no in range(3):
        inputs.append(layer_in)
        y_val = jnp.dot(layer_in, weights[layer_no].T, preferred_element_type=jnp.float32) / powered[layer_no][2]
        outputs.append(y_val)
        if layer_no < 2:
            layer_in = leaky_relu(y_val).astype(jnp.bfloat16)
    target = jnp.concatenate([t_real, t_fake], axis=0).astype(jnp.float32)
    upstream = outputs[2] - target
    loss_val = 0.5 * jnp.sum(upstream * upstream) / ROWS
    dweights = [None, None, None]
    back_sum = upstream
    for layer_no in (2, 1, 0):
        u_new, v_new, sigma_val = powered[layer_no]
        up_half = upstream.astype(jnp.bfloat16)
        outer_sum = jnp.dot(up_half.T, inputs[layer_no], preferred_element_type=jnp.float32)
        corr_sum = jnp.sum(upstream * outputs[layer_no])
        dweights[layer_no] = (outer_sum - corr_sum * u_new[:, None] * v_new[None, :]) / (ROWS * sigma_val)
        back_sum = jnp.dot(up_half, weights[layer_no], preferred_element_type=jnp.float32) / sigma_val
        if layer_no > 0:
            upstream = back_sum * leaky_slope(outputs[layer_no - 1])
    sigmas = jnp.stack([step_out[2] for step_out in powered])
    return (loss_val.reshape(1), back_sum[:ROWS], back_sum[ROWS:], dweights[0], dweights[1], dweights[2], powered[0][0], powered[1][0], powered[2][0], powered[0][1], powered[1][1], powered[2][1], sigmas)
```

```python
import jax
import jax.numpy as jnp
from jax import lax
from jax.sharding import PartitionSpec as P

SLOPE = 0.2
EPSILON = 1e-12
ORDER = (0, 2, 1, 3)


def leaky_relu(values):
    return jnp.where(values > 0, values, SLOPE * values)


def leaky_slope(values):
    return jnp.where(values > 0, 1.0, SLOPE)


def dot_t(left, right):
    return lax.dot_general(left, right, (((1,), (1,)), ((), ())), preferred_element_type=jnp.float32)


def dot_n(left, right):
    return lax.dot_general(left, right, (((1,), (0,)), ((), ())), preferred_element_type=jnp.float32)


def t_dot(left, right):
    return lax.dot_general(left, right, (((0,), (0,)), ((), ())), preferred_element_type=jnp.float32)


def swap(values, bits):
    return lax.ppermute(values, "model", [(dev, dev ^ bits) for dev in range(4)])


def half(values):
    return values.astype(jnp.bfloat16)


def solution(mesh):
    rows_spec = P("rep", None)
    weight_spec = P(("rep", "model"), None)
    left_spec = P(("rep", "model"))
    target_spec = P("rep", "model")
    group_spec = P("rep")

    def local_step(x_real, x_fake, weight0, weight1, weight2, u_left0, u_left1, u_left2, t_real, t_fake):
        me = lax.axis_index("model")
        core = me % 2
        n_rows = x_real.shape[0]
        o_blk = weight1.shape[0]
        i_blk = weight1.shape[1] // 4

        def w1_block(bits):
            return lax.dynamic_slice(weight1, (0, (me ^ bits) * i_blk), (o_blk, i_blk))

        w1_in = {bits: swap(w1_block(bits), bits) if bits else w1_block(0) for bits in (2, 3, 1, 0)}
        w1_loc = jnp.concatenate([w1_in[bits] for bits in ORDER], axis=0)

        weights = (weight0, weight1, weight2)
        u_lefts = (u_left0, u_left1, u_left2)
        p_parts = [jnp.dot(half(u_left), weight, preferred_element_type=jnp.float32) for weight, u_left in zip(weights, u_lefts)]
        p_vecs = lax.psum(p_parts, "model")
        v_news = [p_vec / jnp.maximum(jnp.sqrt(jnp.sum(p_vec * p_vec)), EPSILON) for p_vec in p_vecs]
        s_vecs = [jnp.dot(weight, half(v_new), preferred_element_type=jnp.float32) for weight, v_new in zip(weights, v_news)]
        norms = lax.psum(jnp.stack([jnp.sum(s_vec * s_vec) for s_vec in s_vecs]), "model")
        sigmas = jnp.sqrt(norms)
        u_news = [s_vec / sigmas[layer_no] for layer_no, s_vec in enumerate(s_vecs)]
        sig0, sig1, sig2 = sigmas[0], sigmas[1], sigmas[2]

        def own_columns(values):
            return jnp.concatenate([lax.dynamic_slice(values, (0, (me ^ bits) * o_blk), (values.shape[0], o_blk)) for bits in ORDER], axis=1)

        w2_loc = own_columns(jnp.concatenate([weight2, swap(weight2, 2)], axis=0))
        x0s = (x_real, x_fake)
        targets = [jnp.concatenate([target, swap(target, 2)], axis=1).astype(jnp.float32) for target in (t_real, t_fake)]
        wide = 2 * o_blk

        y0s = [dot_t(x0, weight0) / sig0 for x0 in x0s]
        x1s = [half(leaky_relu(y0)) for y0 in y0s]
        sums = []
        for x1 in x1s:
            part = dot_t(x1, w1_loc)
            sums.append(half(part[:, :wide] + swap(part[:, wide:], 1)))
        chains = []
        for batch_no in range(2):
            arrived = swap(sums[batch_no], 2)
            arrived = jnp.concatenate([arrived[:, o_blk:], arrived[:, :o_blk]], axis=1)
            y1 = (sums[batch_no].astype(jnp.float32) + arrived.astype(jnp.float32)) / sig1
            x2h = half(leaky_relu(y1))
            x2 = jnp.concatenate([x2h, swap(x2h, 1)], axis=1)
            y2 = dot_t(x2, w2_loc) / sig2
            e2 = y2 - targets[batch_no]
            e2h = half(e2)
            h2_part = half(dot_n(e2h, w2_loc))
            h2 = (h2_part[:, :wide].astype(jnp.float32) + swap(h2_part[:, wide:], 1).astype(jnp.float32)) / sig2
            e1 = h2 * leaky_slope(y1)
            e1h = half(e1)
            e1f = jnp.concatenate([e1h, swap(e1h, 1)], axis=1)
            h1 = dot_n(e1f, w1_loc) / sig1
            y0 = y0s[batch_no]
            e0 = h1 * leaky_slope(y0)
            e0h = half(e0)
            h0_part = half(dot_n(e0h, weight0))
            q_rows = n_rows // 2
            mine = lax.dynamic_slice(h0_part, (core * q_rows, 0), (q_rows, h0_part.shape[1]))
            theirs = lax.dynamic_slice(h0_part, ((1 - core) * q_rows, 0), (q_rows, h0_part.shape[1]))
            chip = half(mine.astype(jnp.float32) + swap(theirs, 1).astype(jnp.float32))
            h0_half = (chip.astype(jnp.float32) + swap(chip, 2).astype(jnp.float32)) / sig0
            h0_other = swap(h0_half, 1)
            dx = jnp.where(core == 0, jnp.concatenate([h0_half, h0_other], axis=0), jnp.concatenate([h0_other, h0_half], axis=0))
            sums_own = jnp.stack([
                jnp.sum(e0 * y0),
                jnp.sum(e1[:, :o_blk] * y1[:, :o_blk]),
                jnp.sum(e2[:, :o_blk] * y2[:, :o_blk]),
                jnp.sum(e2[:, :o_blk] * e2[:, :o_blk]),
            ])
            chains.append((x2, e2h[:, :o_blk], e1f, e0h, dx, sums_own))
        corr = lax.psum(chains[0][5] + chains[1][5], "model")
        loss_val = corr[3] * (0.5 / n_rows)

        outer1 = t_dot(chains[0][2], x1s[0]) + t_dot(chains[1][2], x1s[1])
        out1 = []
        for place, bits in enumerate(ORDER):
            block = outer1[place * o_blk:(place + 1) * o_blk]
            out1.append(swap(half(block), bits).astype(jnp.float32) if bits else block)
        by_bits = jnp.stack([out1[ORDER.index(bits)] for bits in range(4)])
        full1 = jnp.concatenate([lax.dynamic_index_in_dim(by_bits, me ^ block_no, 0, keepdims=False) for block_no in range(4)], axis=1)
        dw1 = (full1 - corr[1] * u_news[1][:, None] * v_news[1][None, :]) / (n_rows * sig1)

        outer0 = t_dot(chains[0][3], x0s[0]) + t_dot(chains[1][3], x0s[1])
        dw0 = (outer0 - corr[0] * u_news[0][:, None] * v_news[0][None, :]) / (n_rows * sig0)

        outer2 = t_dot(chains[0][1], chains[0][0]) + t_dot(chains[1][1], chains[1][0])
        pieces = []
        for block_no in range(4):
            bits = me ^ block_no
            place = bits // 2 + 2 * (bits % 2)
            pieces.append(lax.dynamic_slice(outer2, (0, place * o_blk), (o_blk, o_blk)))
        full2 = jnp.concatenate(pieces, axis=1)
        dw2 = (full2 - corr[2] * u_news[2][:, None] * v_news[2][None, :]) / (n_rows * sig2)
        return (loss_val.reshape(1), chains[0][4], chains[1][4], dw0, dw1, dw2, u_news[0], u_news[1], u_news[2], v_news[0], v_news[1], v_news[2], sigmas)

    return jax.shard_map(local_step, mesh=mesh, in_specs=(rows_spec, rows_spec, weight_spec, weight_spec, weight_spec, left_spec, left_spec, left_spec, target_spec, target_spec), out_specs=(group_spec, rows_spec, rows_spec, weight_spec, weight_spec, weight_spec, left_spec, left_spec, left_spec, group_spec, group_spec, group_spec, group_spec), check_vma=False)
```

```python
import jax
import jax.numpy as jnp
from jax import lax
from jax.experimental import pallas as pl
from jax.experimental.pallas import tpu as pltpu
from jax.sharding import PartitionSpec as P

SLOPE = 0.2
EPSILON = 1e-12
MESH = pl.DeviceIdType.MESH
CHUNKS = 4
PIECES = 4
TILE = 256
BF16 = jnp.bfloat16
F32 = jnp.float32


def leaky_relu(values):
    return jnp.where(values > 0, values, SLOPE * values)


def leaky_slope(values):
    return jnp.where(values > 0, 1.0, SLOPE)


def dot_t(left, right):
    return lax.dot_general(left, right, (((1,), (1,)), ((), ())), preferred_element_type=F32)


def dot_n(left, right):
    return lax.dot_general(left, right, (((1,), (0,)), ((), ())), preferred_element_type=F32)


def t_dot(left, right):
    return lax.dot_general(left, right, (((0,), (0,)), ((), ())), preferred_element_type=F32)


def total(values):
    return jnp.sum(jnp.sum(values, axis=1, keepdims=True), axis=0, keepdims=True)


def chain_kernel(x_real, x_fake, w0_in, w1_in, w2_in, u0_in, u1_in, u2_in, t_real, t_fake,
                 x1_out, x2_out, e2_out, e1_out, e0_out, dx_out, v0_out, v1_out, v2_out, u0_out, u1_out, u2_out, sig_out, cor_out,
                 w0, w1, w1x, w2, x0, x1, x2, y0, y1, tt, e2, h2_own, h2_put, h2_got, e1, e0, h0_put, h0_got, dx,
                 p_buf, n_buf, c_buf,
                 load_sem, put_sem, w_send, w_recv, w1x_send, w1x_recv, fwd_send, fwd_recv, small_send, small_recv,
                 x1_send, x1_recv, x2_send, x2_recv, h2_send, h2_recv, e1_send, e1_recv, h0_send, h0_recv, out_send, out_recv, dx_sem, dx_send, dx_recv):
    me = lax.axis_index("model")
    chip = me // 2
    core = me % 2
    other = 1 - chip
    mate = me + 1 - 2 * core
    far = me + 2 - 4 * chip
    diag = mate + 2 - 4 * chip
    n_rows, n0 = x0.shape
    wide1 = w0.shape[0]
    rows1 = wide1 // 2
    wide2 = w2.shape[0]
    rows2 = wide2 // 2
    n1 = 2 * wide1
    step = n_rows // CHUNKS
    piece = rows2 // PIECES

    def send(src, dst, send_sem, recv_sem, device):
        return pltpu.make_async_remote_copy(src_ref=src, dst_ref=dst, send_sem=send_sem, recv_sem=recv_sem, device_id={"model": device}, device_id_type=MESH)

    def part(index, size):
        return pl.ds(pl.multiple_of(index * size, size), size)

    barrier = pltpu.get_barrier_semaphore()
    for device in (mate, far, diag):
        pl.semaphore_signal(barrier, inc=1, device_id={"model": device}, device_id_type=MESH)
    pl.semaphore_wait(barrier, 3)

    def w1x_copy(piece_no):
        return send(
            w1_in.at[pl.ds(piece_no * piece, piece), part(other, wide1)],
            w1x.at[pl.ds(pl.multiple_of(core * rows2 + piece_no * piece, piece), piece), :],
            w1x_send.at[piece_no], w1x_recv.at[piece_no], far)

    def w1x_forward(piece_no):
        rows = w1x.at[pl.ds(pl.multiple_of(core * rows2 + piece_no * piece, piece), piece), :]
        return send(rows, rows, fwd_send.at[piece_no], fwd_recv.at[piece_no], mate)

    own1, own2 = part(core, rows1), part(core, rows2)
    loads = [
        pltpu.make_async_copy(w0_in, w0.at[own1, :], load_sem.at[0]),
        pltpu.make_async_copy(w1_in, w1.at[own2, :], load_sem.at[1]),
        pltpu.make_async_copy(w2_in, w2.at[own2, :], load_sem.at[2]),
    ]
    gives = [
        send(w0_in, w0.at[own1, :], w_send.at[0], w_recv.at[0], mate),
        send(w1_in, w1.at[own2, :], w_send.at[1], w_recv.at[1], mate),
        send(w2_in, w2.at[own2, :], w_send.at[2], w_recv.at[2], mate),
    ]
    loads[0].start()
    w1x_copy(0).start()
    for copy in loads[1:]:
        copy.start()

    def mine(x_in, t_own, t_mate):
        return (
            pltpu.make_async_copy(x_in, x0, load_sem.at[3]),
            pltpu.make_async_copy(t_own, tt.at[core], load_sem.at[4]),
            send(t_mate, tt.at[core], w_send.at[3], w_recv.at[3], mate),
        )

    @pl.when(core == 0)
    def _():
        for copy in mine(x_real, t_real, t_fake):
            copy.start()

    @pl.when(core == 1)
    def _():
        for copy in mine(x_fake, t_fake, t_real):
            copy.start()

    for copy in gives:
        copy.start()

    def row(values):
        return jnp.broadcast_to(values.astype(BF16), (16, values.shape[1]))

    u_rows = [row(u0_in[...]), row(u1_in[...]), row(u2_in[...])]
    loads[0].wait()
    p_buf[me, :, pl.ds(0, n0)] = dot_n(u_rows[0], w0[own1, :])[0:1]
    loads[1].wait()

    def p1_tile(tile_no, carry):
        cols = part(tile_no, wide1 // 2)
        p_buf[me, :, pl.ds(pl.multiple_of(n0 + tile_no * (wide1 // 2), 128), wide1 // 2)] = dot_n(u_rows[1], w1[own2, cols])[0:1]
        return carry

    lax.fori_loop(0, 4, p1_tile, 0)
    loads[2].wait()
    p_buf[me, :, pl.ds(n0 + n1, wide2 * 2)] = dot_n(u_rows[2], w2[own2, :])[0:1]

    def spread(buf, first):
        return [send(buf.at[me], buf.at[me], small_send.at[first + which], small_recv.at[first + which], device) for which, device in enumerate((mate, far, diag))]

    p_copies = spread(p_buf, 0)
    for copy in p_copies:
        copy.start()
    w1x_copy(1).start()
    for copy in p_copies:
        copy.wait()
    p_all = p_buf[0] + p_buf[1] + p_buf[2] + p_buf[3]
    spans = ((0, n0, v0_out), (n0, n1, v1_out), (n0 + n1, 2 * wide2, v2_out))
    for first, size, v_out in spans:
        p_vec = p_all[:, first:first + size]
        v_out[...] = p_vec / jnp.maximum(jnp.sqrt(total(p_vec * p_vec)), EPSILON)
    u0_out[...] = dot_t(row(v0_out[...]), w0[own1, :])[0:1]
    u1_out[...] = dot_t(row(v1_out[...]), w1[own2, :])[0:1]
    u2_out[...] = dot_t(row(v2_out[...]), w2[own2, :])[0:1]
    lane = lax.broadcasted_iota(jnp.int32, (8, 128), 1)

    def pack(values):
        packed = jnp.zeros((8, 128), F32)
        for place, value in enumerate(values):
            packed = jnp.where(lane == place, value, packed)
        return packed

    n_buf[me] = pack([total(u_out[...] * u_out[...]) for u_out in (u0_out, u1_out, u2_out)])
    n_copies = spread(n_buf, 3)
    for copy in n_copies:
        copy.start()
    for piece_no in range(2, PIECES):
        w1x_copy(piece_no).start()
    for copy in n_copies:
        copy.wait()
    sigmas = jnp.sqrt(n_buf[0] + n_buf[1] + n_buf[2] + n_buf[3])
    sig_out[...] = sigmas
    sig0, sig1, sig2 = sigmas[0:1, 0:1], sigmas[0:1, 1:2], sigmas[0:1, 2:3]
    u0_out[...] = u0_out[...] / sig0
    u1_out[...] = u1_out[...] / sig1
    u2_out[...] = u2_out[...] / sig2

    pltpu.make_async_copy(x_real, x0, load_sem.at[3]).wait()
    gives[0].wait_recv()

    def y0_tile(tile_no, carry):
        cols = part(tile_no, TILE)
        y_tile = dot_t(x0[...], w0[cols, :]) / sig0
        y0[:, cols] = y_tile
        x1[chip, :, cols] = leaky_relu(y_tile).astype(BF16)
        return carry

    lax.fori_loop(0, wide1 // TILE, y0_tile, 0)

    def chunk_copy(buf, slot, chunk_no, send_sem, recv_sem):
        rows = buf.at[slot, part(chunk_no, step), :]
        return send(rows, rows, send_sem.at[chunk_no], recv_sem.at[chunk_no], far)

    for chunk_no in range(CHUNKS):
        chunk_copy(x1, chip, chunk_no, x1_send, x1_recv).start()

    batch = part(core, n_rows)

    def outputs(src, dst, which):
        return (
            pltpu.make_async_copy(src, dst, put_sem.at[which]),
            send(src, dst, out_send.at[which], out_recv.at[which], mate),
        )

    x1_near = outputs(x1.at[chip], x1_out.at[batch, part(chip, wide1)], 0)
    for copy in x1_near:
        copy.start()
    for piece_no in range(PIECES):
        w1x_copy(piece_no).wait_recv()
        w1x_forward(piece_no).start()

    gives[1].wait_recv()

    def layer1(chunk_no, carry):
        rows = part(chunk_no, step)
        chunk_copy(x1, other, chunk_no, x1_send, x1_recv).wait_recv()
        y_val = (dot_t(x1[0, rows, :], w1[:, pl.ds(0, wide1)]) + dot_t(x1[1, rows, :], w1[:, pl.ds(wide1, wide1)])) / sig1
        y1[rows, :] = y_val
        x2[chip, rows, :] = leaky_relu(y_val).astype(BF16)
        chunk_copy(x2, chip, chunk_no, x2_send, x2_recv).start()
        return carry

    lax.fori_loop(0, CHUNKS, layer1, 0)
    x1_far = outputs(x1.at[other], x1_out.at[batch, part(other, wide1)], 1)
    for copy in x1_far:
        copy.start()

    gives[2].wait_recv()
    pltpu.make_async_copy(t_real, tt.at[core], load_sem.at[4]).wait()
    send(t_real, tt.at[core], w_send.at[3], w_recv.at[3], mate).wait_recv()

    def layer2(chunk_no, carry):
        corr2, loss = carry
        rows = part(chunk_no, step)
        chunk_copy(x2, other, chunk_no, x2_send, x2_recv).wait_recv()
        y_val = (dot_t(x2[0, rows, :], w2[:, pl.ds(0, wide2)]) + dot_t(x2[1, rows, :], w2[:, pl.ds(wide2, wide2)])) / sig2
        target = jnp.concatenate([tt[0, rows, :].astype(F32), tt[1, rows, :].astype(F32)], axis=1)
        e_val = y_val - target
        corr2 = corr2 + total(e_val * y_val)
        loss = loss + total(e_val * e_val)
        e_half = e_val.astype(BF16)
        e2[rows, :] = e_half
        h2_put[rows, :] = dot_n(e_half, w2[:, part(other, wide2)]).astype(BF16)
        send(h2_put.at[rows, :], h2_got.at[rows, :], h2_send.at[chunk_no], h2_recv.at[chunk_no], far).start()
        h2_own[rows, :] = dot_n(e_half, w2[:, part(chip, wide2)])
        return corr2, loss

    zero = jnp.zeros((1, 1), F32)
    corr2, loss = lax.fori_loop(0, CHUNKS, layer2, (zero, zero))

    def back1(chunk_no, corr1):
        rows = part(chunk_no, step)
        send(h2_put.at[rows, :], h2_got.at[rows, :], h2_send.at[chunk_no], h2_recv.at[chunk_no], far).wait_recv()
        y_val = y1[rows, :]
        e_val = (h2_own[rows, :] + h2_got[rows, :].astype(F32)) / sig2 * leaky_slope(y_val)
        e1[chip, rows, :] = e_val.astype(BF16)
        chunk_copy(e1, chip, chunk_no, e1_send, e1_recv).start()
        return corr1 + total(e_val * y_val)

    corr1 = lax.fori_loop(0, CHUNKS, back1, zero)
    lesser = [
        outputs(x2.at[0], x2_out.at[batch, pl.ds(0, wide2)], 2),
        outputs(x2.at[1], x2_out.at[batch, pl.ds(wide2, wide2)], 3),
        outputs(e2, e2_out.at[batch, :], 4),
        outputs(e1.at[chip], e1_out.at[batch, :], 5),
    ]
    for pair in lesser:
        for copy in pair:
            copy.start()
    for piece_no in range(PIECES):
        w1x_forward(piece_no).wait_recv()

    def back0(chunk_no, corr0):
        rows = part(chunk_no, step)
        chunk_copy(e1, other, chunk_no, e1_send, e1_recv).wait_recv()

        def h1_tile(tile_no, corr):
            cols = part(tile_no, TILE)
            own_cols = pl.ds(pl.multiple_of(chip * wide1 + tile_no * TILE, TILE), TILE)
            h_val = (dot_n(e1[chip, rows, :], w1[:, own_cols]) + dot_n(e1[other, rows, :], w1x[:, cols])) / sig1
            y_val = y0[rows, cols]
            e_val = h_val * leaky_slope(y_val)
            e0[rows, cols] = e_val.astype(BF16)
            return corr + total(e_val * y_val)

        corr0 = lax.fori_loop(0, wide1 // TILE, h1_tile, corr0)
        h0_put[rows, :] = dot_n(e0[rows, :], w0[...]).astype(BF16)
        send(h0_put.at[rows, :], h0_got.at[rows, :], h0_send.at[chunk_no], h0_recv.at[chunk_no], far).start()
        return corr0

    corr0 = lax.fori_loop(0, CHUNKS, back0, zero)
    e0_near = pltpu.make_async_copy(e0.at[:, part(core, rows1)], e0_out.at[batch, :], put_sem.at[6])
    e0_mate = send(e0.at[:, part(1 - core, rows1)], e0_out.at[batch, :], out_send.at[6], out_recv.at[6], mate)
    e0_near.start()
    e0_mate.start()
    c_buf[me] = pack([corr0, corr1, corr2, loss])
    c_copies = spread(c_buf, 6)
    for copy in c_copies:
        copy.start()

    def dx_copies(chunk_no):
        rows = part(chunk_no, step)
        dst = dx_out.at[pl.ds(pl.multiple_of(core * n_rows + chunk_no * step, step), step), :]
        return (
            pltpu.make_async_copy(dx.at[rows, :], dst, dx_sem.at[chunk_no]),
            send(dx.at[rows, :], dst, dx_send.at[chunk_no], dx_recv.at[chunk_no], mate),
        )

    def finish(chunk_no, carry):
        rows = part(chunk_no, step)
        send(h0_put.at[rows, :], h0_got.at[rows, :], h0_send.at[chunk_no], h0_recv.at[chunk_no], far).wait_recv()
        dx[rows, :] = (h0_put[rows, :].astype(F32) + h0_got[rows, :].astype(F32)) / sig0
        for copy in dx_copies(chunk_no):
            copy.start()
        return carry

    lax.fori_loop(0, CHUNKS, finish, 0)
    for copy in c_copies:
        copy.wait()
    cor_out[...] = c_buf[0] + c_buf[1] + c_buf[2] + c_buf[3]

    for copy in gives:
        copy.wait_send()
    send(t_real, tt.at[core], w_send.at[3], w_recv.at[3], mate).wait_send()
    for piece_no in range(PIECES):
        w1x_copy(piece_no).wait_send()
        w1x_forward(piece_no).wait_send()
    for pair in (x1_near, x1_far, *lesser, (e0_near, e0_mate)):
        for copy in pair:
            copy.wait()

    def drain(chunk_no, carry):
        rows = part(chunk_no, step)
        chunk_copy(x1, chip, chunk_no, x1_send, x1_recv).wait_send()
        chunk_copy(x2, chip, chunk_no, x2_send, x2_recv).wait_send()
        send(h2_put.at[rows, :], h2_got.at[rows, :], h2_send.at[chunk_no], h2_recv.at[chunk_no], far).wait_send()
        chunk_copy(e1, chip, chunk_no, e1_send, e1_recv).wait_send()
        send(h0_put.at[rows, :], h0_got.at[rows, :], h0_send.at[chunk_no], h0_recv.at[chunk_no], far).wait_send()
        for copy in dx_copies(chunk_no):
            copy.wait()
        return carry

    lax.fori_loop(0, CHUNKS, drain, 0)


def run_chain(x_real, x_fake, weight0, weight1, weight2, u_left0, u_left1, u_left2, t_real, t_fake):
    n_rows, n0 = x_real.shape
    rows1 = weight0.shape[0]
    rows2, n1 = weight1.shape
    wide1, wide2 = 2 * rows1, 2 * rows2
    n2 = 2 * wide2
    hbm = pl.BlockSpec(memory_space=pl.ANY)
    vmem = pl.BlockSpec(memory_space=pltpu.VMEM)
    shape = jax.ShapeDtypeStruct
    dma = pltpu.SemaphoreType.DMA
    return pl.pallas_call(
        chain_kernel,
        out_shape=(
            shape((2 * n_rows, n1), BF16), shape((2 * n_rows, n2), BF16), shape((2 * n_rows, wide2), BF16), shape((2 * n_rows, wide2), BF16),
            shape((2 * n_rows, rows1), BF16), shape((2 * n_rows, n0), F32),
            shape((1, n0), F32), shape((1, n1), F32), shape((1, n2), F32),
            shape((1, rows1), F32), shape((1, rows2), F32), shape((1, rows2), F32),
            shape((8, 128), F32), shape((8, 128), F32),
        ),
        in_specs=[hbm] * 5 + [vmem] * 3 + [hbm] * 2,
        out_specs=[hbm] * 6 + [vmem] * 8,
        scratch_shapes=[
            pltpu.VMEM((wide1, n0), BF16), pltpu.VMEM((wide2, n1), BF16), pltpu.VMEM((wide2, wide1), BF16), pltpu.VMEM((wide2, n2), BF16),
            pltpu.VMEM((n_rows, n0), BF16), pltpu.VMEM((2, n_rows, wide1), BF16), pltpu.VMEM((2, n_rows, wide2), BF16),
            pltpu.VMEM((n_rows, wide1), F32), pltpu.VMEM((n_rows, wide2), F32), pltpu.VMEM((2, n_rows, rows2), BF16),
            pltpu.VMEM((n_rows, wide2), BF16), pltpu.VMEM((n_rows, wide2), F32), pltpu.VMEM((n_rows, wide2), BF16), pltpu.VMEM((n_rows, wide2), BF16),
            pltpu.VMEM((2, n_rows, wide2), BF16), pltpu.VMEM((n_rows, wide1), BF16),
            pltpu.VMEM((n_rows, n0), BF16), pltpu.VMEM((n_rows, n0), BF16), pltpu.VMEM((n_rows, n0), F32),
            pltpu.VMEM((4, 1, n0 + n1 + n2), F32), pltpu.VMEM((4, 8, 128), F32), pltpu.VMEM((4, 8, 128), F32),
            dma((5,)), dma((7,)), dma((4,)), dma((4,)), dma((PIECES,)), dma((PIECES,)), dma((PIECES,)), dma((PIECES,)), dma((9,)), dma((9,)),
            dma((CHUNKS,)), dma((CHUNKS,)), dma((CHUNKS,)), dma((CHUNKS,)), dma((CHUNKS,)), dma((CHUNKS,)),
            dma((CHUNKS,)), dma((CHUNKS,)), dma((CHUNKS,)), dma((CHUNKS,)), dma((7,)), dma((7,)), dma((CHUNKS,)), dma((CHUNKS,)), dma((CHUNKS,)),
        ],
        compiler_params=pltpu.CompilerParams(collective_id=0, has_side_effects=True, vmem_limit_bytes=60 * 1024 * 1024),
        name="chain",
    )(x_real, x_fake, weight0, weight1, weight2, u_left0[None, :], u_left1[None, :], u_left2[None, :], t_real, t_fake)


def solution(mesh):
    rows_spec = P("rep", None)
    weight_spec = P(("rep", "model"), None)
    left_spec = P(("rep", "model"))
    target_spec = P("rep", "model")
    group_spec = P("rep")

    def local_step(x_real, x_fake, weight0, weight1, weight2, u_left0, u_left1, u_left2, t_real, t_fake):
        core = lax.axis_index("model") % 2
        n_rows = x_real.shape[0]
        rows2 = weight1.shape[0]
        x1, x2, e2, e1, e0, dx, v0, v1, v2, u0, u1, u2, sig, cor = run_chain(x_real, x_fake, weight0, weight1, weight2, u_left0, u_left1, u_left2, t_real, t_fake)
        x0 = jnp.concatenate([x_real, x_fake], axis=0)
        e2_own = lax.dynamic_slice(e2, (0, core * rows2), (2 * n_rows, rows2))
        e1_own = lax.dynamic_slice(e1, (0, core * rows2), (2 * n_rows, rows2))

        def gradient(up_half, layer_in, layer_no, u_new, v_new):
            return (t_dot(up_half, layer_in) - cor[0, layer_no] * u_new[0][:, None] * v_new) / (n_rows * sig[0, layer_no])

        dw0 = gradient(e0, x0, 0, u0, v0)
        dw1 = gradient(e1_own, x1, 1, u1, v1)
        dw2 = gradient(e2_own, x2, 2, u2, v2)
        loss_val = cor[0, 3:4] * (0.5 / n_rows)
        return (loss_val, dx[:n_rows], dx[n_rows:], dw0, dw1, dw2, u0[0], u1[0], u2[0], v0[0], v1[0], v2[0], sig[0, :3])

    return jax.shard_map(local_step, mesh=mesh, in_specs=(rows_spec, rows_spec, weight_spec, weight_spec, weight_spec, left_spec, left_spec, left_spec, target_spec, target_spec), out_specs=(group_spec, rows_spec, rows_spec, weight_spec, weight_spec, weight_spec, left_spec, left_spec, left_spec, group_spec, group_spec, group_spec, group_spec), check_vma=False)
```

```python
import jax
import jax.numpy as jnp
from jax import lax
from jax.experimental import pallas as pl
from jax.experimental.pallas import tpu as pltpu
from jax.sharding import PartitionSpec as P

SLOPE = 0.2
EPSILON = 1e-12
MESH = pl.DeviceIdType.MESH
CHUNKS = 4
PIECES = 4
TILE = 256
BF16 = jnp.bfloat16
F32 = jnp.float32


def leaky_relu(values):
    return jnp.where(values > 0, values, SLOPE * values)


def leaky_slope(values):
    return jnp.where(values > 0, 1.0, SLOPE)


def dot_t(left, right):
    return lax.dot_general(left, right, (((1,), (1,)), ((), ())), preferred_element_type=F32)


def dot_n(left, right):
    return lax.dot_general(left, right, (((1,), (0,)), ((), ())), preferred_element_type=F32)


def t_dot(left, right):
    return lax.dot_general(left, right, (((0,), (0,)), ((), ())), preferred_element_type=F32)


def total(values):
    return jnp.sum(jnp.sum(values, axis=1, keepdims=True), axis=0, keepdims=True)


def chain_kernel(x_real, x_fake, w0_in, w1_in, w2_in, u0_in, u1_in, u2_in, t_real, t_fake,
                 x1_out, x2_out, e2_out, e1_out, e0_out, dx_out, v0_out, v1_out, v2_out, u0_out, u1_out, u2_out, sig_out, cor_out,
                 w0, w1, w1x, w2, x0, x1, x2, y0, y1, tt, e2_t, h2_own, h2_put, h2_got, e1, e1_t, e0, e0_t, h0_put, h0_got, dx,
                 p_buf, n_buf, c_buf,
                 eye, load_sem, put_sem, w_send, w_recv, w1x_send, w1x_recv, fwd_send, fwd_recv, small_send, small_recv,
                 x1_send, x1_recv, x2_send, x2_recv, h2_send, h2_recv, e1_send, e1_recv, h0_send, h0_recv, out_send, out_recv, dx_sem, dx_send, dx_recv):
    me = lax.axis_index("model")
    chip = me // 2
    core = me % 2
    other = 1 - chip
    mate = me + 1 - 2 * core
    far = me + 2 - 4 * chip
    diag = mate + 2 - 4 * chip
    n_rows, n0 = x0.shape
    wide1 = w0.shape[0]
    rows1 = wide1 // 2
    wide2 = w2.shape[0]
    rows2 = wide2 // 2
    n1 = 2 * wide1
    step = n_rows // CHUNKS
    piece = rows2 // PIECES

    def send(src, dst, send_sem, recv_sem, device):
        return pltpu.make_async_remote_copy(src_ref=src, dst_ref=dst, send_sem=send_sem, recv_sem=recv_sem, device_id={"model": device}, device_id_type=MESH)

    def part(index, size):
        return pl.ds(pl.multiple_of(index * size, size), size)

    barrier = pltpu.get_barrier_semaphore()
    for device in (mate, far, diag):
        pl.semaphore_signal(barrier, inc=1, device_id={"model": device}, device_id_type=MESH)
    pl.semaphore_wait(barrier, 3)

    def w1x_copy(piece_no):
        return send(
            w1_in.at[pl.ds(piece_no * piece, piece), part(other, wide1)],
            w1x.at[pl.ds(pl.multiple_of(core * rows2 + piece_no * piece, piece), piece), :],
            w1x_send.at[piece_no], w1x_recv.at[piece_no], far)

    def w1x_forward(piece_no):
        rows = w1x.at[pl.ds(pl.multiple_of(core * rows2 + piece_no * piece, piece), piece), :]
        return send(rows, rows, fwd_send.at[piece_no], fwd_recv.at[piece_no], mate)

    own1, own2 = part(core, rows1), part(core, rows2)
    loads = [
        pltpu.make_async_copy(w0_in, w0.at[own1, :], load_sem.at[0]),
        pltpu.make_async_copy(w1_in, w1.at[own2, :], load_sem.at[1]),
        pltpu.make_async_copy(w2_in, w2.at[own2, :], load_sem.at[2]),
    ]
    gives = [
        send(w0_in, w0.at[own1, :], w_send.at[0], w_recv.at[0], mate),
        send(w1_in, w1.at[own2, :], w_send.at[1], w_recv.at[1], mate),
        send(w2_in, w2.at[own2, :], w_send.at[2], w_recv.at[2], mate),
    ]
    loads[0].start()
    w1x_copy(0).start()
    for copy in loads[1:]:
        copy.start()

    def mine(x_in, t_own, t_mate):
        return (
            pltpu.make_async_copy(x_in, x0, load_sem.at[3]),
            pltpu.make_async_copy(t_own, tt.at[own2, :], load_sem.at[4]),
            send(t_mate, tt.at[own2, :], w_send.at[3], w_recv.at[3], mate),
        )

    @pl.when(core == 0)
    def _():
        for copy in mine(x_real, t_real, t_fake):
            copy.start()

    @pl.when(core == 1)
    def _():
        for copy in mine(x_fake, t_fake, t_real):
            copy.start()

    for copy in gives:
        copy.start()

    def row(values):
        return jnp.broadcast_to(values.reshape(1, values.size).astype(BF16), (16, values.size))

    lanes = lax.broadcasted_iota(jnp.int32, (128, 128), 1)
    eye[...] = jnp.where(lanes == lax.broadcasted_iota(jnp.int32, (128, 128), 0), 1.0, 0.0).astype(BF16)

    def store_transposed(dst, first, rows, values):
        for place in range(values.shape[1] // 128):
            block = dot_t(eye[...], values[:, place * 128:(place + 1) * 128])
            dst[pl.ds(pl.multiple_of(first + place * 128, 128), 128), rows] = block.astype(BF16)

    u_rows = [row(u0_in[...]), row(u1_in[...]), row(u2_in[...])]
    loads[0].wait()
    p_buf[me, :, pl.ds(0, n0)] = dot_n(u_rows[0], w0[own1, :])[0:1]
    loads[1].wait()

    def p1_tile(tile_no, carry):
        cols = part(tile_no, wide1 // 2)
        p_buf[me, :, pl.ds(pl.multiple_of(n0 + tile_no * (wide1 // 2), 128), wide1 // 2)] = dot_n(u_rows[1], w1[own2, cols])[0:1]
        return carry

    lax.fori_loop(0, 4, p1_tile, 0)
    loads[2].wait()
    p_buf[me, :, pl.ds(n0 + n1, wide2 * 2)] = dot_n(u_rows[2], w2[own2, :])[0:1]

    def spread(buf, first):
        return [send(buf.at[me], buf.at[me], small_send.at[first + which], small_recv.at[first + which], device) for which, device in enumerate((mate, far, diag))]

    p_copies = spread(p_buf, 0)
    for copy in p_copies:
        copy.start()
    w1x_copy(1).start()
    for copy in p_copies:
        copy.wait()
    p_all = p_buf[0] + p_buf[1] + p_buf[2] + p_buf[3]
    spans = ((0, n0, v0_out), (n0, n1, v1_out), (n0 + n1, 2 * wide2, v2_out))
    for first, size, v_out in spans:
        p_vec = p_all[:, first:first + size]
        v_out[...] = p_vec / jnp.maximum(jnp.sqrt(total(p_vec * p_vec)), EPSILON)
    u0_out[...] = dot_t(row(v0_out[...]), w0[own1, :])[0:1]
    u1_out[...] = dot_t(row(v1_out[...]), w1[own2, :])[0:1]
    u2_out[...] = dot_t(row(v2_out[...]), w2[own2, :])[0:1]
    lane = lax.broadcasted_iota(jnp.int32, (8, 128), 1)

    def pack(values):
        packed = jnp.zeros((8, 128), F32)
        for place, value in enumerate(values):
            packed = jnp.where(lane == place, value, packed)
        return packed

    n_buf[me] = pack([total(u_out[...] * u_out[...]) for u_out in (u0_out, u1_out, u2_out)])
    n_copies = spread(n_buf, 3)
    for copy in n_copies:
        copy.start()
    for piece_no in range(2, PIECES):
        w1x_copy(piece_no).start()
    for copy in n_copies:
        copy.wait()
    sigmas = jnp.sqrt(n_buf[0] + n_buf[1] + n_buf[2] + n_buf[3])
    sig_out[...] = sigmas
    sig0, sig1, sig2 = sigmas[0:1, 0:1], sigmas[0:1, 1:2], sigmas[0:1, 2:3]
    u0_out[...] = u0_out[...] / sig0
    u1_out[...] = u1_out[...] / sig1
    u2_out[...] = u2_out[...] / sig2

    pltpu.make_async_copy(x_real, x0, load_sem.at[3]).wait()
    gives[0].wait_recv()

    def y0_tile(tile_no, carry):
        cols = part(tile_no, TILE)
        y_tile = dot_t(x0[...], w0[cols, :]) / sig0
        y0[:, cols] = y_tile
        x1[chip, :, cols] = leaky_relu(y_tile).astype(BF16)
        return carry

    lax.fori_loop(0, wide1 // TILE, y0_tile, 0)

    def chunk_copy(buf, slot, chunk_no, send_sem, recv_sem):
        rows = buf.at[slot, part(chunk_no, step), :]
        return send(rows, rows, send_sem.at[chunk_no], recv_sem.at[chunk_no], far)

    for chunk_no in range(CHUNKS):
        chunk_copy(x1, chip, chunk_no, x1_send, x1_recv).start()

    batch = part(core, n_rows)

    def outputs(src, dst, which):
        return (
            pltpu.make_async_copy(src, dst, put_sem.at[which]),
            send(src, dst, out_send.at[which], out_recv.at[which], mate),
        )

    def halves(src, dst, size, which):
        return (
            pltpu.make_async_copy(src.at[part(core, size), :], dst.at[:, batch], put_sem.at[which]),
            send(src.at[part(1 - core, size), :], dst.at[:, batch], out_send.at[which], out_recv.at[which], mate),
        )

    x1_near = outputs(x1.at[chip], x1_out.at[batch, part(chip, wide1)], 0)
    for copy in x1_near:
        copy.start()
    for piece_no in range(PIECES):
        w1x_copy(piece_no).wait_recv()
        w1x_forward(piece_no).start()

    gives[1].wait_recv()

    def layer1(chunk_no, carry):
        rows = part(chunk_no, step)
        chunk_copy(x1, other, chunk_no, x1_send, x1_recv).wait_recv()
        y_val = (dot_t(x1[0, rows, :], w1[:, pl.ds(0, wide1)]) + dot_t(x1[1, rows, :], w1[:, pl.ds(wide1, wide1)])) / sig1
        y1[rows, :] = y_val
        x2[chip, rows, :] = leaky_relu(y_val).astype(BF16)
        chunk_copy(x2, chip, chunk_no, x2_send, x2_recv).start()
        return carry

    lax.fori_loop(0, CHUNKS, layer1, 0)
    x1_far = outputs(x1.at[other], x1_out.at[batch, part(other, wide1)], 1)
    for copy in x1_far:
        copy.start()

    gives[2].wait_recv()
    pltpu.make_async_copy(t_real, tt.at[own2, :], load_sem.at[4]).wait()
    t_give = send(t_real, tt.at[own2, :], w_send.at[3], w_recv.at[3], mate)
    t_give.wait_recv()

    def layer2(chunk_no, carry):
        corr2, loss = carry
        rows = part(chunk_no, step)
        chunk_copy(x2, other, chunk_no, x2_send, x2_recv).wait_recv()
        y_val = (dot_t(x2[0, rows, :], w2[:, pl.ds(0, wide2)]) + dot_t(x2[1, rows, :], w2[:, pl.ds(wide2, wide2)])) / sig2
        e_val = y_val - dot_t(eye[...], tt[:, rows])
        corr2 = corr2 + total(e_val * y_val)
        loss = loss + total(e_val * e_val)
        e_half = e_val.astype(BF16)
        h2_put[rows, :] = dot_n(e_half, w2[:, part(other, wide2)]).astype(BF16)
        send(h2_put.at[rows, :], h2_got.at[rows, :], h2_send.at[chunk_no], h2_recv.at[chunk_no], far).start()
        h2_own[rows, :] = dot_n(e_half, w2[:, part(chip, wide2)])
        store_transposed(e2_t, 0, rows, e_half)
        return corr2, loss

    zero = jnp.zeros((1, 1), F32)
    corr2, loss = lax.fori_loop(0, CHUNKS, layer2, (zero, zero))

    def back1(chunk_no, corr1):
        rows = part(chunk_no, step)
        send(h2_put.at[rows, :], h2_got.at[rows, :], h2_send.at[chunk_no], h2_recv.at[chunk_no], far).wait_recv()
        y_val = y1[rows, :]
        e_val = (h2_own[rows, :] + h2_got[rows, :].astype(F32)) / sig2 * leaky_slope(y_val)
        e_half = e_val.astype(BF16)
        e1[chip, rows, :] = e_half
        chunk_copy(e1, chip, chunk_no, e1_send, e1_recv).start()
        store_transposed(e1_t, 0, rows, e_half)
        return corr1 + total(e_val * y_val)

    corr1 = lax.fori_loop(0, CHUNKS, back1, zero)
    lesser = [
        outputs(x2.at[0], x2_out.at[batch, pl.ds(0, wide2)], 2),
        outputs(x2.at[1], x2_out.at[batch, pl.ds(wide2, wide2)], 3),
        halves(e2_t, e2_out, rows2, 4),
        halves(e1_t, e1_out, rows2, 5),
    ]
    for pair in lesser:
        for copy in pair:
            copy.start()
    for piece_no in range(PIECES):
        w1x_forward(piece_no).wait_recv()

    def back0(chunk_no, corr0):
        rows = part(chunk_no, step)
        chunk_copy(e1, other, chunk_no, e1_send, e1_recv).wait_recv()

        def h1_tile(tile_no, corr):
            cols = part(tile_no, TILE)
            own_cols = pl.ds(pl.multiple_of(chip * wide1 + tile_no * TILE, TILE), TILE)
            h_val = (dot_n(e1[chip, rows, :], w1[:, own_cols]) + dot_n(e1[other, rows, :], w1x[:, cols])) / sig1
            y_val = y0[rows, cols]
            e_val = h_val * leaky_slope(y_val)
            e_half = e_val.astype(BF16)
            e0[:, cols] = e_half
            store_transposed(e0_t, tile_no * TILE, rows, e_half)
            return corr + total(e_val * y_val)

        corr0 = lax.fori_loop(0, wide1 // TILE, h1_tile, corr0)
        h0_put[rows, :] = dot_n(e0[...], w0[...]).astype(BF16)
        send(h0_put.at[rows, :], h0_got.at[rows, :], h0_send.at[chunk_no], h0_recv.at[chunk_no], far).start()
        return corr0

    corr0 = lax.fori_loop(0, CHUNKS, back0, zero)
    e0_pair = halves(e0_t, e0_out, rows1, 6)
    for copy in e0_pair:
        copy.start()
    c_buf[me] = pack([corr0, corr1, corr2, loss])
    c_copies = spread(c_buf, 6)
    for copy in c_copies:
        copy.start()

    def dx_copies(chunk_no):
        rows = part(chunk_no, step)
        dst = dx_out.at[pl.ds(pl.multiple_of(core * n_rows + chunk_no * step, step), step), :]
        return (
            pltpu.make_async_copy(dx.at[rows, :], dst, dx_sem.at[chunk_no]),
            send(dx.at[rows, :], dst, dx_send.at[chunk_no], dx_recv.at[chunk_no], mate),
        )

    def finish(chunk_no, carry):
        rows = part(chunk_no, step)
        send(h0_put.at[rows, :], h0_got.at[rows, :], h0_send.at[chunk_no], h0_recv.at[chunk_no], far).wait_recv()
        dx[rows, :] = (h0_put[rows, :].astype(F32) + h0_got[rows, :].astype(F32)) / sig0
        for copy in dx_copies(chunk_no):
            copy.start()
        return carry

    lax.fori_loop(0, CHUNKS, finish, 0)
    for copy in c_copies:
        copy.wait()
    cor_out[...] = c_buf[0] + c_buf[1] + c_buf[2] + c_buf[3]

    for copy in gives:
        copy.wait_send()
    t_give.wait_send()
    for piece_no in range(PIECES):
        w1x_copy(piece_no).wait_send()
        w1x_forward(piece_no).wait_send()
    for pair in (x1_near, x1_far, *lesser, e0_pair):
        for copy in pair:
            copy.wait()

    def drain(chunk_no, carry):
        rows = part(chunk_no, step)
        chunk_copy(x1, chip, chunk_no, x1_send, x1_recv).wait_send()
        chunk_copy(x2, chip, chunk_no, x2_send, x2_recv).wait_send()
        send(h2_put.at[rows, :], h2_got.at[rows, :], h2_send.at[chunk_no], h2_recv.at[chunk_no], far).wait_send()
        chunk_copy(e1, chip, chunk_no, e1_send, e1_recv).wait_send()
        send(h0_put.at[rows, :], h0_got.at[rows, :], h0_send.at[chunk_no], h0_recv.at[chunk_no], far).wait_send()
        for copy in dx_copies(chunk_no):
            copy.wait()
        return carry

    lax.fori_loop(0, CHUNKS, drain, 0)


def run_chain(x_real, x_fake, weight0, weight1, weight2, u_left0, u_left1, u_left2, t_real, t_fake):
    n_rows, n0 = x_real.shape
    rows1 = weight0.shape[0]
    rows2, n1 = weight1.shape
    wide1, wide2 = 2 * rows1, 2 * rows2
    n2 = 2 * wide2
    hbm = pl.BlockSpec(memory_space=pl.ANY)
    vmem = pl.BlockSpec(memory_space=pltpu.VMEM)
    shape = jax.ShapeDtypeStruct
    dma = pltpu.SemaphoreType.DMA
    return pl.pallas_call(
        chain_kernel,
        out_shape=(
            shape((2 * n_rows, n1), BF16), shape((2 * n_rows, n2), BF16), shape((rows2, 2 * n_rows), BF16), shape((rows2, 2 * n_rows), BF16),
            shape((rows1, 2 * n_rows), BF16), shape((2 * n_rows, n0), F32),
            shape((1, n0), F32), shape((1, n1), F32), shape((1, n2), F32),
            shape((1, rows1), F32), shape((1, rows2), F32), shape((1, rows2), F32),
            shape((8, 128), F32), shape((8, 128), F32),
        ),
        in_specs=[hbm] * 5 + [vmem] * 3 + [hbm] * 2,
        out_specs=[hbm] * 6 + [vmem] * 8,
        scratch_shapes=[
            pltpu.VMEM((wide1, n0), BF16), pltpu.VMEM((wide2, n1), BF16), pltpu.VMEM((wide2, wide1), BF16), pltpu.VMEM((wide2, n2), BF16),
            pltpu.VMEM((n_rows, n0), BF16), pltpu.VMEM((2, n_rows, wide1), BF16), pltpu.VMEM((2, n_rows, wide2), BF16),
            pltpu.VMEM((n_rows, wide1), F32), pltpu.VMEM((n_rows, wide2), F32), pltpu.VMEM((wide2, n_rows), BF16),
            pltpu.VMEM((wide2, n_rows), BF16), pltpu.VMEM((n_rows, wide2), F32), pltpu.VMEM((n_rows, wide2), BF16), pltpu.VMEM((n_rows, wide2), BF16),
            pltpu.VMEM((2, n_rows, wide2), BF16), pltpu.VMEM((wide2, n_rows), BF16), pltpu.VMEM((n_rows // CHUNKS, wide1), BF16), pltpu.VMEM((wide1, n_rows), BF16),
            pltpu.VMEM((n_rows, n0), BF16), pltpu.VMEM((n_rows, n0), BF16), pltpu.VMEM((n_rows, n0), F32),
            pltpu.VMEM((4, 1, n0 + n1 + n2), F32), pltpu.VMEM((4, 8, 128), F32), pltpu.VMEM((4, 8, 128), F32), pltpu.VMEM((128, 128), BF16),
            dma((5,)), dma((7,)), dma((4,)), dma((4,)), dma((PIECES,)), dma((PIECES,)), dma((PIECES,)), dma((PIECES,)), dma((9,)), dma((9,)),
            dma((CHUNKS,)), dma((CHUNKS,)), dma((CHUNKS,)), dma((CHUNKS,)), dma((CHUNKS,)), dma((CHUNKS,)),
            dma((CHUNKS,)), dma((CHUNKS,)), dma((CHUNKS,)), dma((CHUNKS,)), dma((7,)), dma((7,)), dma((CHUNKS,)), dma((CHUNKS,)), dma((CHUNKS,)),
        ],
        compiler_params=pltpu.CompilerParams(collective_id=0, has_side_effects=True, vmem_limit_bytes=60 * 1024 * 1024),
        name="chain",
    )(x_real, x_fake, weight0, weight1, weight2, u_left0, u_left1, u_left2, t_real.T, t_fake.T)


def grad_kernel(x1, e1, x2, e2, x_real, x_fake, e0, dx_a, dx_b, u0, u1, u2, v0, v1, v2, sig, cor,
                dw0, dw1, dw2, dx_real, dx_fake, u0_out, u1_out, u2_out, v0_out, v1_out, v2_out, sig_out, loss_out, col0, col1, col2):
    step = pl.program_id(0)
    n_rows = x_real.shape[0]
    dx_real[...] = dx_a[...]
    dx_fake[...] = dx_b[...]

    def scale(layer_no):
        return 1.0 / (n_rows * sig[0:1, layer_no:layer_no + 1])

    @pl.when(step == 0)
    def _():
        for src, dst in ((u0, u0_out), (u1, u1_out), (u2, u2_out), (v0, v0_out), (v1, v1_out), (v2, v2_out)):
            dst[...] = src[...].reshape(dst.shape)
        sig_out[...] = sig[...]
        loss_out[...] = cor[0:1, 3:4] * (0.5 / n_rows)
        for layer_no, (src, dst) in enumerate(((u0, col0), (u1, col1), (u2, col2))):
            spread = jnp.broadcast_to(src[...] * cor[0:1, layer_no:layer_no + 1], (128, src.shape[1]))
            dst[...] = spread.T

    @pl.when(step < 8)
    def _():
        cols = pl.ds(pl.multiple_of(step * dw1.shape[1], 128), dw1.shape[1])
        dw1[...] = (dot_n(e1[...], x1[...]) - col1[:, 0:1] * v1[:, cols]) * scale(1)

    @pl.when((step >= 8) & (step < 10))
    def _():
        cols = pl.ds(pl.multiple_of((step - 8) * dw2.shape[1], 128), dw2.shape[1])
        dw2[...] = (dot_n(e2[...], x2[...]) - col2[:, 0:1] * v2[:, cols]) * scale(2)

    @pl.when((step >= 10) & (step < 15))
    def _():
        rows = pl.ds(pl.multiple_of((step - 10) * dw0.shape[0], 128), dw0.shape[0])
        outer = dot_n(e0[:, 0:n_rows], x_real[...]) + dot_n(e0[:, n_rows:], x_fake[...])
        dw0[...] = (outer - col0[rows, 0:1] * v0[...]) * scale(0)


def run_grads(x1, e1, x2, e2, x_real, x_fake, e0, dx, u0, u1, u2, v0, v1, v2, sig, cor):
    both, n1 = x1.shape
    n_rows, n0 = x_real.shape
    n2 = x2.shape[1]
    rows2 = e1.shape[0]
    rows1 = e0.shape[0]
    steps = 16
    dx_rows = n_rows // steps
    shape = jax.ShapeDtypeStruct
    vmem = pl.BlockSpec(memory_space=pltpu.VMEM)

    def whole(array):
        return pl.BlockSpec(array.shape, lambda step: (0, 0))

    def at1(step):
        return (0, jnp.minimum(step, 7))

    def at2(step):
        return (0, jnp.clip(step - 8, 0, 1))

    def at0(step):
        return (jnp.clip(step - 10, 0, 4), 0)

    flops = 2 * both * (rows2 * (n1 + n2) + rows1 * n0)
    return pl.pallas_call(
        grad_kernel,
        grid=(steps,),
        out_shape=(
            shape((rows1, n0), F32), shape((rows2, n1), F32), shape((rows2, n2), F32), shape((n_rows, n0), F32), shape((n_rows, n0), F32),
            shape((rows1,), F32), shape((rows2,), F32), shape((rows2,), F32), shape((n0,), F32), shape((n1,), F32), shape((n2,), F32),
            shape((8, 128), F32), shape((1, 1), F32),
        ),
        in_specs=[
            pl.BlockSpec((both, n1 // 8), at1), whole(e1), pl.BlockSpec((both, n2 // 2), at2), whole(e2),
            whole(x_real), whole(x_fake), pl.BlockSpec((rows1 // 5, both), at0),
            pl.BlockSpec((dx_rows, n0), lambda step: (step, 0)), pl.BlockSpec((dx_rows, n0), lambda step: (step + steps, 0)),
            whole(u0), whole(u1), whole(u2), whole(v0), whole(v1), whole(v2), whole(sig), whole(cor),
        ],
        out_specs=[
            pl.BlockSpec((rows1 // 5, n0), at0), pl.BlockSpec((rows2, n1 // 8), at1), pl.BlockSpec((rows2, n2 // 2), at2),
            pl.BlockSpec((dx_rows, n0), lambda step: (step, 0)), pl.BlockSpec((dx_rows, n0), lambda step: (step, 0)),
            *[pl.BlockSpec((size,), lambda step: (0,)) for size in (rows1, rows2, rows2, n0, n1, n2)],
            pl.BlockSpec((8, 128), lambda step: (0, 0)), pl.BlockSpec((1, 1), lambda step: (0, 0)),
        ],
        scratch_shapes=[pltpu.VMEM((rows1, 128), F32), pltpu.VMEM((rows2, 128), F32), pltpu.VMEM((rows2, 128), F32)],
        compiler_params=pltpu.CompilerParams(dimension_semantics=("arbitrary",), vmem_limit_bytes=48 * 1024 * 1024),
        cost_estimate=pl.CostEstimate(flops=flops, bytes_accessed=45 * 1024 * 1024, transcendentals=0),
        name="grads",
    )(x1, e1, x2, e2, x_real, x_fake, e0, dx, dx, u0, u1, u2, v0, v1, v2, sig, cor)


def solution(mesh):
    rows_spec = P("rep", None)
    weight_spec = P(("rep", "model"), None)
    left_spec = P(("rep", "model"))
    target_spec = P("rep", "model")
    group_spec = P("rep")

    def local_step(x_real, x_fake, weight0, weight1, weight2, u_left0, u_left1, u_left2, t_real, t_fake):
        x1, x2, e2, e1, e0, dx, v0, v1, v2, u0, u1, u2, sig, cor = run_chain(x_real, x_fake, weight0, weight1, weight2, u_left0, u_left1, u_left2, t_real, t_fake)
        dw0, dw1, dw2, dx_real, dx_fake, u0, u1, u2, v0, v1, v2, sig, loss = run_grads(x1, e1, x2, e2, x_real, x_fake, e0, dx, u0, u1, u2, v0, v1, v2, sig, cor)
        return (loss[0], dx_real, dx_fake, dw0, dw1, dw2, u0, u1, u2, v0, v1, v2, sig[0, :3])

    return jax.shard_map(local_step, mesh=mesh, in_specs=(rows_spec, rows_spec, weight_spec, weight_spec, weight_spec, left_spec, left_spec, left_spec, target_spec, target_spec), out_specs=(group_spec, rows_spec, rows_spec, weight_spec, weight_spec, weight_spec, left_spec, left_spec, left_spec, group_spec, group_spec, group_spec, group_spec), check_vma=False)
```

```python
import jax
import jax.numpy as jnp
from jax import lax
from jax.experimental import pallas as pl
from jax.experimental.pallas import tpu as pltpu
from jax.sharding import PartitionSpec as P

SLOPE = 0.2
EPSILON = 1e-12
MESH = pl.DeviceIdType.MESH
CHUNKS = 4
PIECES = 4
TILE = 256
BF16 = jnp.bfloat16
F32 = jnp.float32


def leaky_relu(values):
    return jnp.where(values > 0, values, SLOPE * values)


def leaky_slope(values):
    return jnp.where(values > 0, 1.0, SLOPE)


def dot_t(left, right):
    return lax.dot_general(left, right, (((1,), (1,)), ((), ())), preferred_element_type=F32)


def dot_n(left, right):
    return lax.dot_general(left, right, (((1,), (0,)), ((), ())), preferred_element_type=F32)


def t_dot(left, right):
    return lax.dot_general(left, right, (((0,), (0,)), ((), ())), preferred_element_type=F32)


def total(values):
    return jnp.sum(jnp.sum(values, axis=1, keepdims=True), axis=0, keepdims=True)


def chain_kernel(x_real, x_fake, w0_in, w1_in, w2_in, u0_in, u1_in, u2_in, t_real, t_fake,
                 x1_out, x2_out, e2_out, e1_out, e0_out, dx_out, v0_out, v1_out, v2_out, u0_out, u1_out, u2_out, sig_out, cor_out,
                 w0, w1, w1x, w2, x0, x1, x2, y0, y1, tt, e2_t, h2_own, h2_put, h2_got, e1, e1_t, e0, e0_t, h0_put, h0_got, dx,
                 p_buf, n_buf, c_buf,
                 eye, load_sem, put_sem, w_send, w_recv, w1x_send, w1x_recv, fwd_send, fwd_recv, small_send, small_recv,
                 x1_send, x1_recv, x2_send, x2_recv, h2_send, h2_recv, e1_send, e1_recv, h0_send, h0_recv, out_send, out_recv, dx_sem, dx_send, dx_recv):
    me = lax.axis_index("model")
    chip = me // 2
    core = me % 2
    other = 1 - chip
    mate = me + 1 - 2 * core
    far = me + 2 - 4 * chip
    diag = mate + 2 - 4 * chip
    n_rows, n0 = x0.shape
    wide1 = w0.shape[0]
    rows1 = wide1 // 2
    wide2 = w2.shape[0]
    rows2 = wide2 // 2
    n1 = 2 * wide1
    step = n_rows // CHUNKS
    piece = rows2 // PIECES

    def send(src, dst, send_sem, recv_sem, device):
        return pltpu.make_async_remote_copy(src_ref=src, dst_ref=dst, send_sem=send_sem, recv_sem=recv_sem, device_id={"model": device}, device_id_type=MESH)

    def part(index, size):
        return pl.ds(pl.multiple_of(index * size, size), size)

    barrier = pltpu.get_barrier_semaphore()
    for device in (mate, far, diag):
        pl.semaphore_signal(barrier, inc=1, device_id={"model": device}, device_id_type=MESH)
    pl.semaphore_wait(barrier, 3)

    def w1x_copy(piece_no):
        return send(
            w1_in.at[pl.ds(piece_no * piece, piece), part(other, wide1)],
            w1x.at[pl.ds(pl.multiple_of(core * rows2 + piece_no * piece, piece), piece), :],
            w1x_send.at[piece_no], w1x_recv.at[piece_no], far)

    def w1x_forward(piece_no):
        rows = w1x.at[pl.ds(pl.multiple_of(core * rows2 + piece_no * piece, piece), piece), :]
        return send(rows, rows, fwd_send.at[piece_no], fwd_recv.at[piece_no], mate)

    own1, own2 = part(core, rows1), part(core, rows2)
    loads = [
        pltpu.make_async_copy(w0_in, w0.at[own1, :], load_sem.at[0]),
        pltpu.make_async_copy(w1_in, w1.at[own2, :], load_sem.at[1]),
        pltpu.make_async_copy(w2_in, w2.at[own2, :], load_sem.at[2]),
    ]
    gives = [
        send(w0_in, w0.at[own1, :], w_send.at[0], w_recv.at[0], mate),
        send(w1_in, w1.at[own2, :], w_send.at[1], w_recv.at[1], mate),
        send(w2_in, w2.at[own2, :], w_send.at[2], w_recv.at[2], mate),
    ]
    loads[0].start()
    w1x_copy(0).start()
    for copy in loads[1:]:
        copy.start()

    def mine(x_in, t_own, t_mate):
        return (
            pltpu.make_async_copy(x_in, x0, load_sem.at[3]),
            pltpu.make_async_copy(t_own, tt.at[own2, :], load_sem.at[4]),
            send(t_mate, tt.at[own2, :], w_send.at[3], w_recv.at[3], mate),
        )

    @pl.when(core == 0)
    def _():
        for copy in mine(x_real, t_real, t_fake):
            copy.start()

    @pl.when(core == 1)
    def _():
        for copy in mine(x_fake, t_fake, t_real):
            copy.start()

    for copy in gives:
        copy.start()

    def row(values):
        return jnp.broadcast_to(values.reshape(1, values.size).astype(BF16), (16, values.size))

    lanes = lax.broadcasted_iota(jnp.int32, (128, 128), 1)
    eye[...] = jnp.where(lanes == lax.broadcasted_iota(jnp.int32, (128, 128), 0), 1.0, 0.0).astype(BF16)

    def store_transposed(dst, first, rows, values):
        for place in range(values.shape[1] // 128):
            block = dot_t(eye[...], values[:, place * 128:(place + 1) * 128])
            dst[pl.ds(pl.multiple_of(first + place * 128, 128), 128), rows] = block.astype(BF16)

    u_rows = [row(u0_in[...]), row(u1_in[...]), row(u2_in[...])]
    loads[0].wait()
    p_buf[me, :, pl.ds(0, n0)] = dot_n(u_rows[0], w0[own1, :])[0:1]
    loads[1].wait()

    def p1_tile(tile_no, carry):
        cols = part(tile_no, wide1 // 2)
        p_buf[me, :, pl.ds(pl.multiple_of(n0 + tile_no * (wide1 // 2), 128), wide1 // 2)] = dot_n(u_rows[1], w1[own2, cols])[0:1]
        return carry

    lax.fori_loop(0, 4, p1_tile, 0)
    loads[2].wait()
    p_buf[me, :, pl.ds(n0 + n1, wide2 * 2)] = dot_n(u_rows[2], w2[own2, :])[0:1]

    def spread(buf, first):
        return [send(buf.at[me], buf.at[me], small_send.at[first + which], small_recv.at[first + which], device) for which, device in enumerate((mate, far, diag))]

    p_copies = spread(p_buf, 0)
    for copy in p_copies:
        copy.start()
    w1x_copy(1).start()
    for copy in p_copies:
        copy.wait()
    p_all = p_buf[0] + p_buf[1] + p_buf[2] + p_buf[3]
    spans = ((0, n0, v0_out), (n0, n1, v1_out), (n0 + n1, 2 * wide2, v2_out))
    for first, size, v_out in spans:
        p_vec = p_all[:, first:first + size]
        v_out[...] = p_vec / jnp.maximum(jnp.sqrt(total(p_vec * p_vec)), EPSILON)
    u0_out[...] = dot_t(row(v0_out[...]), w0[own1, :])[0:1]
    u1_out[...] = dot_t(row(v1_out[...]), w1[own2, :])[0:1]
    u2_out[...] = dot_t(row(v2_out[...]), w2[own2, :])[0:1]
    lane = lax.broadcasted_iota(jnp.int32, (8, 128), 1)

    def pack(values):
        packed = jnp.zeros((8, 128), F32)
        for place, value in enumerate(values):
            packed = jnp.where(lane == place, value, packed)
        return packed

    n_buf[me] = pack([total(u_out[...] * u_out[...]) for u_out in (u0_out, u1_out, u2_out)])
    n_copies = spread(n_buf, 3)
    for copy in n_copies:
        copy.start()
    for piece_no in range(2, PIECES):
        w1x_copy(piece_no).start()
    for copy in n_copies:
        copy.wait()
    sigmas = jnp.sqrt(n_buf[0] + n_buf[1] + n_buf[2] + n_buf[3])
    sig_out[...] = sigmas
    sig0, sig1, sig2 = sigmas[0:1, 0:1], sigmas[0:1, 1:2], sigmas[0:1, 2:3]
    u0_out[...] = u0_out[...] / sig0
    u1_out[...] = u1_out[...] / sig1
    u2_out[...] = u2_out[...] / sig2

    pltpu.make_async_copy(x_real, x0, load_sem.at[3]).wait()
    gives[0].wait_recv()

    def y0_tile(tile_no, carry):
        cols = part(tile_no, TILE)
        y_tile = dot_t(x0[...], w0[cols, :]) / sig0
        y0[:, cols] = y_tile
        x1[chip, :, cols] = leaky_relu(y_tile).astype(BF16)
        return carry

    lax.fori_loop(0, wide1 // TILE, y0_tile, 0)

    def chunk_copy(buf, slot, chunk_no, send_sem, recv_sem):
        rows = buf.at[slot, part(chunk_no, step), :]
        return send(rows, rows, send_sem.at[chunk_no], recv_sem.at[chunk_no], far)

    for chunk_no in range(CHUNKS):
        chunk_copy(x1, chip, chunk_no, x1_send, x1_recv).start()

    batch = part(core, n_rows)

    def outputs(src, dst, which):
        return (
            pltpu.make_async_copy(src, dst, put_sem.at[which]),
            send(src, dst, out_send.at[which], out_recv.at[which], mate),
        )

    def halves(src, dst, size, which):
        return (
            pltpu.make_async_copy(src.at[part(core, size), :], dst.at[:, batch], put_sem.at[which]),
            send(src.at[part(1 - core, size), :], dst.at[:, batch], out_send.at[which], out_recv.at[which], mate),
        )

    x1_near = outputs(x1.at[chip], x1_out.at[batch, part(chip, wide1)], 0)
    for copy in x1_near:
        copy.start()
    for piece_no in range(PIECES):
        w1x_copy(piece_no).wait_recv()
        w1x_forward(piece_no).start()

    gives[1].wait_recv()

    def layer1(chunk_no, carry):
        rows = part(chunk_no, step)
        chunk_copy(x1, other, chunk_no, x1_send, x1_recv).wait_recv()
        y_val = (dot_t(x1[0, rows, :], w1[:, pl.ds(0, wide1)]) + dot_t(x1[1, rows, :], w1[:, pl.ds(wide1, wide1)])) / sig1
        y1[rows, :] = y_val
        x2[chip, rows, :] = leaky_relu(y_val).astype(BF16)
        chunk_copy(x2, chip, chunk_no, x2_send, x2_recv).start()
        return carry

    lax.fori_loop(0, CHUNKS, layer1, 0)
    x1_far = outputs(x1.at[other], x1_out.at[batch, part(other, wide1)], 1)
    for copy in x1_far:
        copy.start()

    gives[2].wait_recv()
    pltpu.make_async_copy(t_real, tt.at[own2, :], load_sem.at[4]).wait()
    t_give = send(t_real, tt.at[own2, :], w_send.at[3], w_recv.at[3], mate)
    t_give.wait_recv()

    def layer2(chunk_no, carry):
        corr2, loss = carry
        rows = part(chunk_no, step)
        chunk_copy(x2, other, chunk_no, x2_send, x2_recv).wait_recv()
        y_val = (dot_t(x2[0, rows, :], w2[:, pl.ds(0, wide2)]) + dot_t(x2[1, rows, :], w2[:, pl.ds(wide2, wide2)])) / sig2
        e_val = y_val - dot_t(eye[...], tt[:, rows])
        corr2 = corr2 + total(e_val * y_val)
        loss = loss + total(e_val * e_val)
        e_half = e_val.astype(BF16)
        h2_put[rows, :] = dot_n(e_half, w2[:, part(other, wide2)]).astype(BF16)
        send(h2_put.at[rows, :], h2_got.at[rows, :], h2_send.at[chunk_no], h2_recv.at[chunk_no], far).start()
        h2_own[rows, :] = dot_n(e_half, w2[:, part(chip, wide2)])
        store_transposed(e2_t, 0, rows, e_half)
        return corr2, loss

    zero = jnp.zeros((1, 1), F32)
    corr2, loss = lax.fori_loop(0, CHUNKS, layer2, (zero, zero))

    def back1(chunk_no, corr1):
        rows = part(chunk_no, step)
        send(h2_put.at[rows, :], h2_got.at[rows, :], h2_send.at[chunk_no], h2_recv.at[chunk_no], far).wait_recv()
        y_val = y1[rows, :]
        e_val = (h2_own[rows, :] + h2_got[rows, :].astype(F32)) / sig2 * leaky_slope(y_val)
        e_half = e_val.astype(BF16)
        e1[chip, rows, :] = e_half
        chunk_copy(e1, chip, chunk_no, e1_send, e1_recv).start()
        store_transposed(e1_t, 0, rows, e_half)
        return corr1 + total(e_val * y_val)

    corr1 = lax.fori_loop(0, CHUNKS, back1, zero)
    lesser = [
        outputs(x2.at[0], x2_out.at[batch, pl.ds(0, wide2)], 2),
        outputs(x2.at[1], x2_out.at[batch, pl.ds(wide2, wide2)], 3),
        halves(e2_t, e2_out, rows2, 4),
        halves(e1_t, e1_out, rows2, 5),
    ]
    for pair in lesser:
        for copy in pair:
            copy.start()
    for piece_no in range(PIECES):
        w1x_forward(piece_no).wait_recv()

    def back0(chunk_no, corr0):
        rows = part(chunk_no, step)
        chunk_copy(e1, other, chunk_no, e1_send, e1_recv).wait_recv()

        def h1_tile(tile_no, corr):
            cols = part(tile_no, TILE)
            own_cols = pl.ds(pl.multiple_of(chip * wide1 + tile_no * TILE, TILE), TILE)
            h_val = (dot_n(e1[chip, rows, :], w1[:, own_cols]) + dot_n(e1[other, rows, :], w1x[:, cols])) / sig1
            y_val = y0[rows, cols]
            e_val = h_val * leaky_slope(y_val)
            e_half = e_val.astype(BF16)
            e0[:, cols] = e_half
            store_transposed(e0_t, tile_no * TILE, rows, e_half)
            return corr + total(e_val * y_val)

        corr0 = lax.fori_loop(0, wide1 // TILE, h1_tile, corr0)
        h0_put[rows, :] = dot_n(e0[...], w0[...]).astype(BF16)
        send(h0_put.at[rows, :], h0_got.at[rows, :], h0_send.at[chunk_no], h0_recv.at[chunk_no], far).start()
        return corr0

    corr0 = lax.fori_loop(0, CHUNKS, back0, zero)
    e0_pair = halves(e0_t, e0_out, rows1, 6)
    for copy in e0_pair:
        copy.start()
    c_buf[me] = pack([corr0, corr1, corr2, loss])
    c_copies = spread(c_buf, 6)
    for copy in c_copies:
        copy.start()

    def dx_copies(chunk_no):
        rows = part(chunk_no, step)
        dst = dx_out.at[pl.ds(pl.multiple_of(core * n_rows + chunk_no * step, step), step), :]
        return (
            pltpu.make_async_copy(dx.at[rows, :], dst, dx_sem.at[chunk_no]),
            send(dx.at[rows, :], dst, dx_send.at[chunk_no], dx_recv.at[chunk_no], mate),
        )

    def finish(chunk_no, carry):
        rows = part(chunk_no, step)
        send(h0_put.at[rows, :], h0_got.at[rows, :], h0_send.at[chunk_no], h0_recv.at[chunk_no], far).wait_recv()
        dx[rows, :] = (h0_put[rows, :].astype(F32) + h0_got[rows, :].astype(F32)) / sig0
        for copy in dx_copies(chunk_no):
            copy.start()
        return carry

    lax.fori_loop(0, CHUNKS, finish, 0)
    for copy in c_copies:
        copy.wait()
    cor_out[...] = c_buf[0] + c_buf[1] + c_buf[2] + c_buf[3]

    for copy in gives:
        copy.wait_send()
    t_give.wait_send()
    for piece_no in range(PIECES):
        w1x_copy(piece_no).wait_send()
        w1x_forward(piece_no).wait_send()
    for pair in (x1_near, x1_far, *lesser, e0_pair):
        for copy in pair:
            copy.wait()

    def drain(chunk_no, carry):
        rows = part(chunk_no, step)
        chunk_copy(x1, chip, chunk_no, x1_send, x1_recv).wait_send()
        chunk_copy(x2, chip, chunk_no, x2_send, x2_recv).wait_send()
        send(h2_put.at[rows, :], h2_got.at[rows, :], h2_send.at[chunk_no], h2_recv.at[chunk_no], far).wait_send()
        chunk_copy(e1, chip, chunk_no, e1_send, e1_recv).wait_send()
        send(h0_put.at[rows, :], h0_got.at[rows, :], h0_send.at[chunk_no], h0_recv.at[chunk_no], far).wait_send()
        for copy in dx_copies(chunk_no):
            copy.wait()
        return carry

    lax.fori_loop(0, CHUNKS, drain, 0)


def run_chain(x_real, x_fake, weight0, weight1, weight2, u_left0, u_left1, u_left2, t_real, t_fake):
    n_rows, n0 = x_real.shape
    rows1 = weight0.shape[0]
    rows2, n1 = weight1.shape
    wide1, wide2 = 2 * rows1, 2 * rows2
    n2 = 2 * wide2
    hbm = pl.BlockSpec(memory_space=pl.ANY)
    vmem = pl.BlockSpec(memory_space=pltpu.VMEM)
    shape = jax.ShapeDtypeStruct
    dma = pltpu.SemaphoreType.DMA
    return pl.pallas_call(
        chain_kernel,
        out_shape=(
            shape((2 * n_rows, n1), BF16), shape((2 * n_rows, n2), BF16), shape((rows2, 2 * n_rows), BF16), shape((rows2, 2 * n_rows), BF16),
            shape((rows1, 2 * n_rows), BF16), shape((2 * n_rows, n0), F32),
            shape((1, n0), F32), shape((1, n1), F32), shape((1, n2), F32),
            shape((1, rows1), F32), shape((1, rows2), F32), shape((1, rows2), F32),
            shape((8, 128), F32), shape((8, 128), F32),
        ),
        in_specs=[hbm] * 5 + [vmem] * 3 + [hbm] * 2,
        out_specs=[hbm] * 6 + [vmem] * 8,
        scratch_shapes=[
            pltpu.VMEM((wide1, n0), BF16), pltpu.VMEM((wide2, n1), BF16), pltpu.VMEM((wide2, wide1), BF16), pltpu.VMEM((wide2, n2), BF16),
            pltpu.VMEM((n_rows, n0), BF16), pltpu.VMEM((2, n_rows, wide1), BF16), pltpu.VMEM((2, n_rows, wide2), BF16),
            pltpu.VMEM((n_rows, wide1), F32), pltpu.VMEM((n_rows, wide2), F32), pltpu.VMEM((wide2, n_rows), BF16),
            pltpu.VMEM((wide2, n_rows), BF16), pltpu.VMEM((n_rows, wide2), F32), pltpu.VMEM((n_rows, wide2), BF16), pltpu.VMEM((n_rows, wide2), BF16),
            pltpu.VMEM((2, n_rows, wide2), BF16), pltpu.VMEM((wide2, n_rows), BF16), pltpu.VMEM((n_rows // CHUNKS, wide1), BF16), pltpu.VMEM((wide1, n_rows), BF16),
            pltpu.VMEM((n_rows, n0), BF16), pltpu.VMEM((n_rows, n0), BF16), pltpu.VMEM((n_rows, n0), F32),
            pltpu.VMEM((4, 1, n0 + n1 + n2), F32), pltpu.VMEM((4, 8, 128), F32), pltpu.VMEM((4, 8, 128), F32), pltpu.VMEM((128, 128), BF16),
            dma((5,)), dma((7,)), dma((4,)), dma((4,)), dma((PIECES,)), dma((PIECES,)), dma((PIECES,)), dma((PIECES,)), dma((9,)), dma((9,)),
            dma((CHUNKS,)), dma((CHUNKS,)), dma((CHUNKS,)), dma((CHUNKS,)), dma((CHUNKS,)), dma((CHUNKS,)),
            dma((CHUNKS,)), dma((CHUNKS,)), dma((CHUNKS,)), dma((CHUNKS,)), dma((7,)), dma((7,)), dma((CHUNKS,)), dma((CHUNKS,)), dma((CHUNKS,)),
        ],
        compiler_params=pltpu.CompilerParams(collective_id=0, has_side_effects=True, vmem_limit_bytes=67043328),
        name="chain",
    )(x_real, x_fake, weight0, weight1, weight2, u_left0, u_left1, u_left2, t_real.T, t_fake.T)


def grad_kernel(x1_in, e1_in, x2_in, e2_in, x_real, x_fake, e0_in, dx_in, u0_in, u1_in, u2_in, v0_in, v1_in, v2_in, sig_in, cor_in,
                dw0_out, dw1_out, dw2_out, dx_real, dx_fake, u0_out, u1_out, u2_out, v0_out, v1_out, v2_out, sig_out, loss_out,
                x1, e1, x2, e2, x0, e0, dx, dw0, dw1, dw2, u0, u1, u2, v0, v1, v2, sig, cor, in_sem, x1_sem, out_sem, dw1_sem, dw0_sem):
    n_rows = x_real.shape[0]
    tiles1 = x1_sem.shape[0]
    tiles0 = dw0_sem.shape[0]
    wide1 = x1.shape[1] // tiles1
    wide0 = x0.shape[1] // tiles0

    def pull(src, dst, which):
        copy = pltpu.make_async_copy(src, dst, in_sem.at[which])
        copy.start()
        return copy

    small = [pull(src, dst, place) for place, (src, dst) in enumerate((
        (u0_in, u0), (u1_in, u1), (u2_in, u2), (v0_in, v0), (v1_in, v1), (v2_in, v2), (sig_in, sig), (cor_in, cor)))]
    got_e0 = pull(e0_in, e0, 8)
    got_x0 = [pull(x_real, x0.at[pl.ds(0, n_rows), :], 9), pull(x_fake, x0.at[pl.ds(n_rows, n_rows), :], 10)]
    got_e1 = pull(e1_in, e1, 11)

    def x1_copy(tile_no):
        cols = pl.ds(pl.multiple_of(tile_no * wide1, 128), wide1)
        return pltpu.make_async_copy(x1_in.at[:, cols], x1.at[:, cols], x1_sem.at[tile_no])

    for tile_no in range(tiles1):
        x1_copy(tile_no).start()
    got_dx = pull(dx_in, dx, 12)
    got_2 = [pull(e2_in, e2, 13), pull(x2_in, x2, 14)]

    for copy in small:
        copy.wait()
    for src, dst in ((u0, u0_out), (u1, u1_out), (u2, u2_out), (v0, v0_out), (v1, v1_out), (v2, v2_out)):
        dst[...] = src[...].reshape(dst.shape)
    sig_out[...] = sig[...]
    loss_out[...] = cor[0:1, 3:4] * (0.5 / n_rows)

    def column(u_new, layer_no):
        return jnp.broadcast_to(u_new[...] * cor[0:1, layer_no:layer_no + 1], (128, u_new.shape[1])).T[:, 0:1]

    def scale(layer_no):
        return 1.0 / (n_rows * sig[0:1, layer_no:layer_no + 1])

    got_e0.wait()
    for copy in got_x0:
        copy.wait()
    col0, scale0 = column(u0, 0), scale(0)

    def dw0_copy(tile_no):
        cols = pl.ds(pl.multiple_of(tile_no * wide0, 128), wide0)
        return pltpu.make_async_copy(dw0.at[:, cols], dw0_out.at[:, cols], dw0_sem.at[tile_no])

    def dw0_tile(tile_no, carry):
        cols = pl.ds(pl.multiple_of(tile_no * wide0, 128), wide0)
        dw0[:, cols] = (dot_n(e0[...], x0[:, cols]) - col0 * v0[:, cols]) * scale0
        dw0_copy(tile_no).start()
        return carry

    lax.fori_loop(0, tiles0, dw0_tile, 0)
    got_e1.wait()
    col1, scale1 = column(u1, 1), scale(1)

    def dw1_copy(tile_no):
        cols = pl.ds(pl.multiple_of(tile_no * wide1, 128), wide1)
        return pltpu.make_async_copy(dw1.at[:, cols], dw1_out.at[:, cols], dw1_sem.at[tile_no])

    def dw1_tile(tile_no, carry):
        cols = pl.ds(pl.multiple_of(tile_no * wide1, 128), wide1)
        x1_copy(tile_no).wait()
        dw1[:, cols] = (dot_n(e1[...], x1[:, cols]) - col1 * v1[:, cols]) * scale1
        dw1_copy(tile_no).start()
        return carry

    lax.fori_loop(0, tiles1, dw1_tile, 0)
    got_dx.wait()
    pushes = [
        pltpu.make_async_copy(dx.at[pl.ds(0, n_rows), :], dx_real, out_sem.at[0]),
        pltpu.make_async_copy(dx.at[pl.ds(n_rows, n_rows), :], dx_fake, out_sem.at[1]),
    ]
    for copy in pushes:
        copy.start()
    for copy in got_2:
        copy.wait()
    dw2[...] = (dot_n(e2[...], x2[...]) - column(u2, 2) * v2[...]) * scale(2)
    last = pltpu.make_async_copy(dw2, dw2_out, out_sem.at[2])
    last.start()

    def drain0(tile_no, carry):
        dw0_copy(tile_no).wait()
        return carry

    def drain1(tile_no, carry):
        dw1_copy(tile_no).wait()
        return carry

    lax.fori_loop(0, tiles0, drain0, 0)
    lax.fori_loop(0, tiles1, drain1, 0)
    for copy in (*pushes, last):
        copy.wait()


def run_grads(x1, e1, x2, e2, x_real, x_fake, e0, dx, u0, u1, u2, v0, v1, v2, sig, cor):
    both, n1 = x1.shape
    n_rows, n0 = x_real.shape
    n2 = x2.shape[1]
    rows2 = e1.shape[0]
    rows1 = e0.shape[0]
    tiles1, tiles0 = 8, 5
    shape = jax.ShapeDtypeStruct
    hbm = pl.BlockSpec(memory_space=pl.ANY)
    vmem = pl.BlockSpec(memory_space=pltpu.VMEM)
    dma = pltpu.SemaphoreType.DMA
    flops = 2 * both * (rows2 * (n1 + n2) + rows1 * n0)
    inputs = (x1, e1, x2, e2, x_real, x_fake, e0, dx, u0, u1, u2, v0, v1, v2, sig, cor)
    return pl.pallas_call(
        grad_kernel,
        out_shape=(
            shape((rows1, n0), F32), shape((rows2, n1), F32), shape((rows2, n2), F32), shape((n_rows, n0), F32), shape((n_rows, n0), F32),
            shape((rows1,), F32), shape((rows2,), F32), shape((rows2,), F32), shape((n0,), F32), shape((n1,), F32), shape((n2,), F32),
            shape((8, 128), F32), shape((1, 1), F32),
        ),
        in_specs=[hbm] * len(inputs),
        out_specs=[hbm] * 5 + [vmem] * 8,
        scratch_shapes=[
            pltpu.VMEM((both, n1), BF16), pltpu.VMEM((rows2, both), BF16), pltpu.VMEM((both, n2), BF16), pltpu.VMEM((rows2, both), BF16),
            pltpu.VMEM((both, n0), BF16), pltpu.VMEM((rows1, both), BF16), pltpu.VMEM((both, n0), F32),
            pltpu.VMEM((rows1, n0), F32), pltpu.VMEM((rows2, n1), F32), pltpu.VMEM((rows2, n2), F32),
            *[pltpu.VMEM(array.shape, F32) for array in (u0, u1, u2, v0, v1, v2, sig, cor)],
            dma((15,)), dma((tiles1,)), dma((3,)), dma((tiles1,)), dma((tiles0,)),
        ],
        compiler_params=pltpu.CompilerParams(vmem_limit_bytes=67043328),
        cost_estimate=pl.CostEstimate(flops=flops, bytes_accessed=45 * 1024 * 1024, transcendentals=0),
        name="grads",
    )(*inputs)


def solution(mesh):
    rows_spec = P("rep", None)
    weight_spec = P(("rep", "model"), None)
    left_spec = P(("rep", "model"))
    target_spec = P("rep", "model")
    group_spec = P("rep")

    def local_step(x_real, x_fake, weight0, weight1, weight2, u_left0, u_left1, u_left2, t_real, t_fake):
        x1, x2, e2, e1, e0, dx, v0, v1, v2, u0, u1, u2, sig, cor = run_chain(x_real, x_fake, weight0, weight1, weight2, u_left0, u_left1, u_left2, t_real, t_fake)
        dw0, dw1, dw2, dx_real, dx_fake, u0, u1, u2, v0, v1, v2, sig, loss = run_grads(x1, e1, x2, e2, x_real, x_fake, e0, dx, u0, u1, u2, v0, v1, v2, sig, cor)
        return (loss[0], dx_real, dx_fake, dw0, dw1, dw2, u0, u1, u2, v0, v1, v2, sig[0, :3])

    return jax.shard_map(local_step, mesh=mesh, in_specs=(rows_spec, rows_spec, weight_spec, weight_spec, weight_spec, left_spec, left_spec, left_spec, target_spec, target_spec), out_specs=(group_spec, rows_spec, rows_spec, weight_spec, weight_spec, weight_spec, left_spec, left_spec, left_spec, group_spec, group_spec, group_spec, group_spec), check_vma=False)
```

```python
import jax
import jax.numpy as jnp
from jax import lax
from jax.experimental import pallas as pl
from jax.experimental.pallas import tpu as pltpu
from jax.sharding import PartitionSpec as P

SLOPE = 0.2
EPSILON = 1e-12
MESH = pl.DeviceIdType.MESH
CHUNKS = 4
EARLY = 1
PIECES = 4
TILE = 256
BF16 = jnp.bfloat16
F32 = jnp.float32


def leaky_relu(values):
    return jnp.where(values > 0, values, SLOPE * values)


def leaky_slope(values):
    return jnp.where(values > 0, 1.0, SLOPE)


def dot_t(left, right):
    return lax.dot_general(left, right, (((1,), (1,)), ((), ())), preferred_element_type=F32)


def dot_n(left, right):
    return lax.dot_general(left, right, (((1,), (0,)), ((), ())), preferred_element_type=F32)


def t_dot(left, right):
    return lax.dot_general(left, right, (((0,), (0,)), ((), ())), preferred_element_type=F32)


def total(values):
    return jnp.sum(jnp.sum(values, axis=1, keepdims=True), axis=0, keepdims=True)


def chain_kernel(x_real, x_fake, w0_in, w1_in, w2_in, u0_in, u1_in, u2_in, t_real, t_fake,
                 x1_out, x2_out, e2_out, e1_out, e0_out, dx_out, sum_out, both_out, v0_out, v1_out, v2_out, u0_out, u1_out, u2_out, sig_out, cor_out,
                 w0, w1, w1x, w2, x0, x1, x2, y0, y1, tt, e2_t, h2_own, h2_put, h2_got, e1, e1_t, e0, e0_t, h0_put, h0_got, dx,
                 p_buf, n_buf, c_buf,
                 eye, load_sem, put_sem, w_send, w_recv, w1x_send, w1x_recv, fwd_send, fwd_recv, small_send, small_recv,
                 x1_send, x1_recv, x2_send, x2_recv, h2_send, h2_recv, e1_send, e1_recv, h0_send, h0_recv, out_send, out_recv, dx_sem, dx_send, dx_recv, sum_sem, both_sem, both_send, both_recv):
    me = lax.axis_index("model")
    chip = me // 2
    core = me % 2
    other = 1 - chip
    mate = me + 1 - 2 * core
    far = me + 2 - 4 * chip
    diag = mate + 2 - 4 * chip
    n_rows, n0 = x0.shape
    wide1 = w0.shape[0]
    rows1 = wide1 // 2
    wide2 = w2.shape[0]
    rows2 = wide2 // 2
    n1 = 2 * wide1
    step = n_rows // CHUNKS
    piece = rows2 // PIECES

    def send(src, dst, send_sem, recv_sem, device):
        return pltpu.make_async_remote_copy(src_ref=src, dst_ref=dst, send_sem=send_sem, recv_sem=recv_sem, device_id={"model": device}, device_id_type=MESH)

    def part(index, size):
        return pl.ds(pl.multiple_of(index * size, size), size)

    barrier = pltpu.get_barrier_semaphore()
    for device in (mate, far, diag):
        pl.semaphore_signal(barrier, inc=1, device_id={"model": device}, device_id_type=MESH)
    pl.semaphore_wait(barrier, 3)

    def w1x_copy(piece_no):
        return send(
            w1_in.at[pl.ds(piece_no * piece, piece), part(other, wide1)],
            w1x.at[pl.ds(pl.multiple_of(core * rows2 + piece_no * piece, piece), piece), :],
            w1x_send.at[piece_no], w1x_recv.at[piece_no], far)

    def w1x_forward(piece_no):
        rows = w1x.at[pl.ds(pl.multiple_of(core * rows2 + piece_no * piece, piece), piece), :]
        return send(rows, rows, fwd_send.at[piece_no], fwd_recv.at[piece_no], mate)

    own1, own2 = part(core, rows1), part(core, rows2)
    loads = [
        pltpu.make_async_copy(w0_in, w0.at[own1, :], load_sem.at[0]),
        pltpu.make_async_copy(w1_in, w1.at[own2, :], load_sem.at[1]),
        pltpu.make_async_copy(w2_in, w2.at[own2, :], load_sem.at[2]),
    ]
    gives = [
        send(w0_in, w0.at[own1, :], w_send.at[0], w_recv.at[0], mate),
        send(w1_in, w1.at[own2, :], w_send.at[1], w_recv.at[1], mate),
        send(w2_in, w2.at[own2, :], w_send.at[2], w_recv.at[2], mate),
    ]
    loads[0].start()
    w1x_copy(0).start()
    for copy in loads[1:]:
        copy.start()

    def mine(x_in, t_own, t_mate):
        return (
            pltpu.make_async_copy(x_in, x0, load_sem.at[3]),
            pltpu.make_async_copy(t_own, tt.at[own2, :], load_sem.at[4]),
            send(t_mate, tt.at[own2, :], w_send.at[3], w_recv.at[3], mate),
        )

    @pl.when(core == 0)
    def _():
        for copy in mine(x_real, t_real, t_fake):
            copy.start()

    @pl.when(core == 1)
    def _():
        for copy in mine(x_fake, t_fake, t_real):
            copy.start()

    for copy in gives:
        copy.start()

    def row(values):
        return jnp.broadcast_to(values.reshape(1, values.size).astype(BF16), (16, values.size))

    lanes = lax.broadcasted_iota(jnp.int32, (128, 128), 1)
    eye[...] = jnp.where(lanes == lax.broadcasted_iota(jnp.int32, (128, 128), 0), 1.0, 0.0).astype(BF16)

    def store_transposed(dst, first, rows, values):
        for place in range(values.shape[1] // 128):
            block = dot_t(eye[...], values[:, place * 128:(place + 1) * 128])
            dst[pl.ds(pl.multiple_of(first + place * 128, 128), 128), rows] = block.astype(BF16)

    u_rows = [row(u0_in[...]), row(u1_in[...]), row(u2_in[...])]
    loads[0].wait()
    p_buf[me, :, pl.ds(0, n0)] = dot_n(u_rows[0], w0[own1, :])[0:1]
    loads[1].wait()

    def p1_tile(tile_no, carry):
        cols = part(tile_no, wide1 // 2)
        p_buf[me, :, pl.ds(pl.multiple_of(n0 + tile_no * (wide1 // 2), 128), wide1 // 2)] = dot_n(u_rows[1], w1[own2, cols])[0:1]
        return carry

    lax.fori_loop(0, 4, p1_tile, 0)
    loads[2].wait()
    p_buf[me, :, pl.ds(n0 + n1, wide2 * 2)] = dot_n(u_rows[2], w2[own2, :])[0:1]

    def spread(buf, first):
        return [send(buf.at[me], buf.at[me], small_send.at[first + which], small_recv.at[first + which], device) for which, device in enumerate((mate, far, diag))]

    p_copies = spread(p_buf, 0)
    for copy in p_copies:
        copy.start()
    w1x_copy(1).start()
    for copy in p_copies:
        copy.wait()
    p_all = p_buf[0] + p_buf[1] + p_buf[2] + p_buf[3]
    spans = ((0, n0, v0_out), (n0, n1, v1_out), (n0 + n1, 2 * wide2, v2_out))
    for first, size, v_out in spans:
        p_vec = p_all[:, first:first + size]
        v_out[...] = p_vec / jnp.maximum(jnp.sqrt(total(p_vec * p_vec)), EPSILON)
    u0_out[...] = dot_t(row(v0_out[...]), w0[own1, :])[0:1]
    u1_out[...] = dot_t(row(v1_out[...]), w1[own2, :])[0:1]
    u2_out[...] = dot_t(row(v2_out[...]), w2[own2, :])[0:1]
    lane = lax.broadcasted_iota(jnp.int32, (8, 128), 1)

    def pack(values):
        packed = jnp.zeros((8, 128), F32)
        for place, value in enumerate(values):
            packed = jnp.where(lane == place, value, packed)
        return packed

    n_buf[me] = pack([total(u_out[...] * u_out[...]) for u_out in (u0_out, u1_out, u2_out)])
    n_copies = spread(n_buf, 3)
    for copy in n_copies:
        copy.start()
    for piece_no in range(2, PIECES):
        w1x_copy(piece_no).start()
    for copy in n_copies:
        copy.wait()
    sigmas = jnp.sqrt(n_buf[0] + n_buf[1] + n_buf[2] + n_buf[3])
    sig_out[...] = sigmas
    sig0, sig1, sig2 = sigmas[0:1, 0:1], sigmas[0:1, 1:2], sigmas[0:1, 2:3]
    u0_out[...] = u0_out[...] / sig0
    u1_out[...] = u1_out[...] / sig1
    u2_out[...] = u2_out[...] / sig2

    pltpu.make_async_copy(x_real, x0, load_sem.at[3]).wait()
    gives[0].wait_recv()

    def y0_tile(tile_no, carry):
        cols = part(tile_no, TILE)
        y_tile = dot_t(x0[...], w0[cols, :]) / sig0
        y0[:, cols] = y_tile
        x1[chip, :, cols] = leaky_relu(y_tile).astype(BF16)
        return carry

    lax.fori_loop(0, wide1 // TILE, y0_tile, 0)

    def chunk_copy(buf, slot, chunk_no, send_sem, recv_sem):
        rows = buf.at[slot, part(chunk_no, step), :]
        return send(rows, rows, send_sem.at[chunk_no], recv_sem.at[chunk_no], far)

    for chunk_no in range(CHUNKS):
        chunk_copy(x1, chip, chunk_no, x1_send, x1_recv).start()

    batch = part(core, n_rows)

    def outputs(src, dst, which):
        return (
            pltpu.make_async_copy(src, dst, put_sem.at[which]),
            send(src, dst, out_send.at[which], out_recv.at[which], mate),
        )

    def halves(src, dst, size, which):
        return (
            pltpu.make_async_copy(src.at[part(core, size), :], dst.at[:, batch], put_sem.at[which]),
            send(src.at[part(1 - core, size), :], dst.at[:, batch], out_send.at[which], out_recv.at[which], mate),
        )

    x1_near = outputs(x1.at[chip], x1_out.at[batch, part(chip, wide1)], 0)
    for copy in x1_near:
        copy.start()
    for piece_no in range(PIECES):
        w1x_copy(piece_no).wait_recv()
        w1x_forward(piece_no).start()

    gives[1].wait_recv()

    def layer1(chunk_no, carry):
        rows = part(chunk_no, step)
        chunk_copy(x1, other, chunk_no, x1_send, x1_recv).wait_recv()
        y_val = (dot_t(x1[0, rows, :], w1[:, pl.ds(0, wide1)]) + dot_t(x1[1, rows, :], w1[:, pl.ds(wide1, wide1)])) / sig1
        y1[rows, :] = y_val
        x2[chip, rows, :] = leaky_relu(y_val).astype(BF16)
        chunk_copy(x2, chip, chunk_no, x2_send, x2_recv).start()
        return carry

    lax.fori_loop(0, CHUNKS, layer1, 0)
    x1_far = outputs(x1.at[other], x1_out.at[batch, part(other, wide1)], 1)
    for copy in x1_far:
        copy.start()

    gives[2].wait_recv()
    pltpu.make_async_copy(t_real, tt.at[own2, :], load_sem.at[4]).wait()
    t_give = send(t_real, tt.at[own2, :], w_send.at[3], w_recv.at[3], mate)
    t_give.wait_recv()

    def layer2(chunk_no, carry):
        corr2, loss = carry
        rows = part(chunk_no, step)
        chunk_copy(x2, other, chunk_no, x2_send, x2_recv).wait_recv()
        y_val = (dot_t(x2[0, rows, :], w2[:, pl.ds(0, wide2)]) + dot_t(x2[1, rows, :], w2[:, pl.ds(wide2, wide2)])) / sig2
        e_val = y_val - dot_t(eye[...], tt[:, rows])
        corr2 = corr2 + total(e_val * y_val)
        loss = loss + total(e_val * e_val)
        e_half = e_val.astype(BF16)
        h2_put[rows, :] = dot_n(e_half, w2[:, part(other, wide2)]).astype(BF16)
        send(h2_put.at[rows, :], h2_got.at[rows, :], h2_send.at[chunk_no], h2_recv.at[chunk_no], far).start()
        h2_own[rows, :] = dot_n(e_half, w2[:, part(chip, wide2)])
        store_transposed(e2_t, 0, rows, e_half)
        return corr2, loss

    zero = jnp.zeros((1, 1), F32)
    corr2, loss = lax.fori_loop(0, CHUNKS, layer2, (zero, zero))

    def back1(chunk_no, corr1):
        rows = part(chunk_no, step)
        send(h2_put.at[rows, :], h2_got.at[rows, :], h2_send.at[chunk_no], h2_recv.at[chunk_no], far).wait_recv()
        y_val = y1[rows, :]
        e_val = (h2_own[rows, :] + h2_got[rows, :].astype(F32)) / sig2 * leaky_slope(y_val)
        e_half = e_val.astype(BF16)
        e1[chip, rows, :] = e_half
        chunk_copy(e1, chip, chunk_no, e1_send, e1_recv).start()
        store_transposed(e1_t, 0, rows, e_half)
        return corr1 + total(e_val * y_val)

    corr1 = lax.fori_loop(0, CHUNKS, back1, zero)
    lesser = [
        outputs(x2.at[0], x2_out.at[batch, pl.ds(0, wide2)], 2),
        outputs(x2.at[1], x2_out.at[batch, pl.ds(wide2, wide2)], 3),
        halves(e2_t, e2_out, rows2, 4),
        halves(e1_t, e1_out, rows2, 5),
    ]
    for pair in lesser:
        for copy in pair:
            copy.start()
    for piece_no in range(PIECES):
        w1x_forward(piece_no).wait_recv()

    late = n_rows - EARLY * step

    def h0_copy(chunk_no):
        rows = part(chunk_no, step)
        return send(h0_put.at[rows, :], h0_got.at[rows, :], h0_send.at[chunk_no], h0_recv.at[chunk_no], far)

    def late_copies(chunk_no):
        src = h0_put.at[part(chunk_no, step), :]
        place = chunk_no - EARLY
        dst = both_out.at[pl.ds(pl.multiple_of(core * late + place * step, step), step), :]
        return (
            pltpu.make_async_copy(src, sum_out.at[part(place, step), :], sum_sem.at[place]),
            pltpu.make_async_copy(src, dst, both_sem.at[place]),
            send(src, dst, both_send.at[place], both_recv.at[place], mate),
        )

    def back0(chunk_no, corr0):
        rows = part(chunk_no, step)
        chunk_copy(e1, other, chunk_no, e1_send, e1_recv).wait_recv()

        def h1_tile(tile_no, corr):
            cols = part(tile_no, TILE)
            own_cols = pl.ds(pl.multiple_of(chip * wide1 + tile_no * TILE, TILE), TILE)
            h_val = (dot_n(e1[chip, rows, :], w1[:, own_cols]) + dot_n(e1[other, rows, :], w1x[:, cols])) / sig1
            y_val = y0[rows, cols]
            e_val = h_val * leaky_slope(y_val)
            e_half = e_val.astype(BF16)
            e0[:, cols] = e_half
            store_transposed(e0_t, tile_no * TILE, rows, e_half)
            return corr + total(e_val * y_val)

        corr0 = lax.fori_loop(0, wide1 // TILE, h1_tile, corr0)
        h0_put[rows, :] = dot_n(e0[...], w0[...]).astype(BF16)
        return corr0

    def back0_early(chunk_no, corr0):
        corr0 = back0(chunk_no, corr0)
        h0_copy(chunk_no).start()
        return corr0

    def back0_late(chunk_no, corr0):
        corr0 = back0(chunk_no, corr0)
        for copy in late_copies(chunk_no):
            copy.start()
        return corr0

    corr0 = lax.fori_loop(0, EARLY, back0_early, zero)
    corr0 = lax.fori_loop(EARLY, CHUNKS, back0_late, corr0)
    e0_pair = halves(e0_t, e0_out, rows1, 6)
    for copy in e0_pair:
        copy.start()
    c_buf[me] = pack([corr0, corr1, corr2, loss])
    c_copies = spread(c_buf, 6)
    for copy in c_copies:
        copy.start()

    def dx_copies(chunk_no):
        rows = part(chunk_no, step)
        dst = dx_out.at[pl.ds(pl.multiple_of((core * EARLY + chunk_no) * step, step), step), :]
        return (
            pltpu.make_async_copy(dx.at[rows, :], dst, dx_sem.at[chunk_no]),
            send(dx.at[rows, :], dst, dx_send.at[chunk_no], dx_recv.at[chunk_no], mate),
        )

    def finish(chunk_no, carry):
        rows = part(chunk_no, step)
        h0_copy(chunk_no).wait_recv()
        dx[rows, :] = (h0_put[rows, :].astype(F32) + h0_got[rows, :].astype(F32)) / sig0
        for copy in dx_copies(chunk_no):
            copy.start()
        return carry

    lax.fori_loop(0, EARLY, finish, 0)
    for copy in c_copies:
        copy.wait()
    cor_out[...] = c_buf[0] + c_buf[1] + c_buf[2] + c_buf[3]

    for copy in gives:
        copy.wait_send()
    t_give.wait_send()
    for piece_no in range(PIECES):
        w1x_copy(piece_no).wait_send()
        w1x_forward(piece_no).wait_send()
    for pair in (x1_near, x1_far, *lesser, e0_pair):
        for copy in pair:
            copy.wait()

    def drain(chunk_no, carry):
        rows = part(chunk_no, step)
        chunk_copy(x1, chip, chunk_no, x1_send, x1_recv).wait_send()
        chunk_copy(x2, chip, chunk_no, x2_send, x2_recv).wait_send()
        send(h2_put.at[rows, :], h2_got.at[rows, :], h2_send.at[chunk_no], h2_recv.at[chunk_no], far).wait_send()
        chunk_copy(e1, chip, chunk_no, e1_send, e1_recv).wait_send()
        return carry

    lax.fori_loop(0, CHUNKS, drain, 0)

    def drain_early(chunk_no, carry):
        h0_copy(chunk_no).wait_send()
        for copy in dx_copies(chunk_no):
            copy.wait()
        return carry

    lax.fori_loop(0, EARLY, drain_early, 0)

    def drain_late(chunk_no, carry):
        for copy in late_copies(chunk_no):
            copy.wait()
        return carry

    lax.fori_loop(EARLY, CHUNKS, drain_late, 0)


def run_chain(x_real, x_fake, weight0, weight1, weight2, u_left0, u_left1, u_left2, t_real, t_fake):
    n_rows, n0 = x_real.shape
    rows1 = weight0.shape[0]
    rows2, n1 = weight1.shape
    wide1, wide2 = 2 * rows1, 2 * rows2
    n2 = 2 * wide2
    early = n_rows // CHUNKS * EARLY
    late = n_rows - early
    hbm = pl.BlockSpec(memory_space=pl.ANY)
    vmem = pl.BlockSpec(memory_space=pltpu.VMEM)
    shape = jax.ShapeDtypeStruct
    dma = pltpu.SemaphoreType.DMA
    return pl.pallas_call(
        chain_kernel,
        out_shape=(
            shape((2 * n_rows, n1), BF16), shape((2 * n_rows, n2), BF16), shape((rows2, 2 * n_rows), BF16), shape((rows2, 2 * n_rows), BF16),
            shape((rows1, 2 * n_rows), BF16), shape((2 * early, n0), F32), shape((late, n0), BF16), shape((2 * late, n0), BF16),
            shape((1, n0), F32), shape((1, n1), F32), shape((1, n2), F32),
            shape((1, rows1), F32), shape((1, rows2), F32), shape((1, rows2), F32),
            shape((8, 128), F32), shape((8, 128), F32),
        ),
        in_specs=[hbm] * 5 + [vmem] * 3 + [hbm] * 2,
        out_specs=[hbm] * 8 + [vmem] * 8,
        scratch_shapes=[
            pltpu.VMEM((wide1, n0), BF16), pltpu.VMEM((wide2, n1), BF16), pltpu.VMEM((wide2, wide1), BF16), pltpu.VMEM((wide2, n2), BF16),
            pltpu.VMEM((n_rows, n0), BF16), pltpu.VMEM((2, n_rows, wide1), BF16), pltpu.VMEM((2, n_rows, wide2), BF16),
            pltpu.VMEM((n_rows, wide1), F32), pltpu.VMEM((n_rows, wide2), F32), pltpu.VMEM((wide2, n_rows), BF16),
            pltpu.VMEM((wide2, n_rows), BF16), pltpu.VMEM((n_rows, wide2), F32), pltpu.VMEM((n_rows, wide2), BF16), pltpu.VMEM((n_rows, wide2), BF16),
            pltpu.VMEM((2, n_rows, wide2), BF16), pltpu.VMEM((wide2, n_rows), BF16), pltpu.VMEM((n_rows // CHUNKS, wide1), BF16), pltpu.VMEM((wide1, n_rows), BF16),
            pltpu.VMEM((n_rows, n0), BF16), pltpu.VMEM((early, n0), BF16), pltpu.VMEM((early, n0), F32),
            pltpu.VMEM((4, 1, n0 + n1 + n2), F32), pltpu.VMEM((4, 8, 128), F32), pltpu.VMEM((4, 8, 128), F32), pltpu.VMEM((128, 128), BF16),
            dma((5,)), dma((7,)), dma((4,)), dma((4,)), dma((PIECES,)), dma((PIECES,)), dma((PIECES,)), dma((PIECES,)), dma((9,)), dma((9,)),
            dma((CHUNKS,)), dma((CHUNKS,)), dma((CHUNKS,)), dma((CHUNKS,)), dma((CHUNKS,)), dma((CHUNKS,)),
            dma((CHUNKS,)), dma((CHUNKS,)), dma((EARLY,)), dma((EARLY,)), dma((7,)), dma((7,)), dma((EARLY,)), dma((EARLY,)), dma((EARLY,)),
            dma((CHUNKS - EARLY,)), dma((CHUNKS - EARLY,)), dma((CHUNKS - EARLY,)), dma((CHUNKS - EARLY,)),
        ],
        compiler_params=pltpu.CompilerParams(collective_id=0, has_side_effects=True, vmem_limit_bytes=67043328),
        name="chain",
    )(x_real, x_fake, weight0, weight1, weight2, u_left0, u_left1, u_left2, t_real.T, t_fake.T)


def grad_kernel(x1_in, e1_in, x2_in, e2_in, x_real, x_fake, e0_in, dx_in, u0_in, u1_in, u2_in, v0_in, v1_in, v2_in, sig_in, cor_in,
                dw0_out, dw1_out, dw2_out, dx_real, dx_fake, u0_out, u1_out, u2_out, v0_out, v1_out, v2_out, sig_out, loss_out,
                x1, e1, x2, e2, x0, e0, dx, dw0, dw1, dw2, u0, u1, u2, v0, v1, v2, sig, cor, in_sem, x1_sem, out_sem, dw1_sem, dw0_sem):
    n_rows = x_real.shape[0]
    early = dx.shape[0] // 2
    tiles1 = x1_sem.shape[0]
    tiles0 = dw0_sem.shape[0]
    wide1 = x1.shape[1] // tiles1
    wide0 = x0.shape[1] // tiles0

    def pull(src, dst, which):
        copy = pltpu.make_async_copy(src, dst, in_sem.at[which])
        copy.start()
        return copy

    small = [pull(src, dst, place) for place, (src, dst) in enumerate((
        (u0_in, u0), (u1_in, u1), (u2_in, u2), (v0_in, v0), (v1_in, v1), (v2_in, v2), (sig_in, sig), (cor_in, cor)))]
    got_e0 = pull(e0_in, e0, 8)
    got_x0 = [pull(x_real, x0.at[pl.ds(0, n_rows), :], 9), pull(x_fake, x0.at[pl.ds(n_rows, n_rows), :], 10)]
    got_e1 = pull(e1_in, e1, 11)

    def x1_copy(tile_no):
        cols = pl.ds(pl.multiple_of(tile_no * wide1, 128), wide1)
        return pltpu.make_async_copy(x1_in.at[:, cols], x1.at[:, cols], x1_sem.at[tile_no])

    for tile_no in range(tiles1):
        x1_copy(tile_no).start()
    got_dx = pull(dx_in, dx, 12)
    got_2 = [pull(e2_in, e2, 13), pull(x2_in, x2, 14)]

    for copy in small:
        copy.wait()
    for src, dst in ((u0, u0_out), (u1, u1_out), (u2, u2_out), (v0, v0_out), (v1, v1_out), (v2, v2_out)):
        dst[...] = src[...].reshape(dst.shape)
    sig_out[...] = sig[0:1, 0:3].reshape(3)
    loss_out[...] = cor[0:1, 3:4] * (0.5 / n_rows)

    def column(u_new, layer_no):
        return jnp.broadcast_to(u_new[...] * cor[0:1, layer_no:layer_no + 1], (128, u_new.shape[1])).T[:, 0:1]

    def scale(layer_no):
        return 1.0 / (n_rows * sig[0:1, layer_no:layer_no + 1])

    got_e0.wait()
    for copy in got_x0:
        copy.wait()
    col0, scale0 = column(u0, 0), scale(0)

    def dw0_copy(tile_no):
        cols = pl.ds(pl.multiple_of(tile_no * wide0, 128), wide0)
        return pltpu.make_async_copy(dw0.at[:, cols], dw0_out.at[:, cols], dw0_sem.at[tile_no])

    def dw0_tile(tile_no, carry):
        cols = pl.ds(pl.multiple_of(tile_no * wide0, 128), wide0)
        dw0[:, cols] = (dot_n(e0[...], x0[:, cols]) - col0 * v0[:, cols]) * scale0
        dw0_copy(tile_no).start()
        return carry

    lax.fori_loop(0, tiles0, dw0_tile, 0)
    got_e1.wait()
    col1, scale1 = column(u1, 1), scale(1)

    def dw1_copy(tile_no):
        cols = pl.ds(pl.multiple_of(tile_no * wide1, 128), wide1)
        return pltpu.make_async_copy(dw1.at[:, cols], dw1_out.at[:, cols], dw1_sem.at[tile_no])

    def dw1_tile(tile_no, carry):
        cols = pl.ds(pl.multiple_of(tile_no * wide1, 128), wide1)
        x1_copy(tile_no).wait()
        dw1[:, cols] = (dot_n(e1[...], x1[:, cols]) - col1 * v1[:, cols]) * scale1
        dw1_copy(tile_no).start()
        return carry

    lax.fori_loop(0, tiles1, dw1_tile, 0)
    got_dx.wait()
    pushes = [
        pltpu.make_async_copy(dx.at[pl.ds(0, early), :], dx_real.at[pl.ds(0, early), :], out_sem.at[0]),
        pltpu.make_async_copy(dx.at[pl.ds(early, early), :], dx_fake.at[pl.ds(0, early), :], out_sem.at[1]),
    ]
    for copy in pushes:
        copy.start()
    for copy in got_2:
        copy.wait()
    dw2[...] = (dot_n(e2[...], x2[...]) - column(u2, 2) * v2[...]) * scale(2)
    last = pltpu.make_async_copy(dw2, dw2_out, out_sem.at[2])
    last.start()

    def drain0(tile_no, carry):
        dw0_copy(tile_no).wait()
        return carry

    def drain1(tile_no, carry):
        dw1_copy(tile_no).wait()
        return carry

    lax.fori_loop(0, tiles0, drain0, 0)
    lax.fori_loop(0, tiles1, drain1, 0)
    for copy in (*pushes, last):
        copy.wait()


def run_grads(x1, e1, x2, e2, x_real, x_fake, e0, dx, u0, u1, u2, v0, v1, v2, sig, cor):
    both, n1 = x1.shape
    n_rows, n0 = x_real.shape
    n2 = x2.shape[1]
    rows2 = e1.shape[0]
    rows1 = e0.shape[0]
    tiles1, tiles0 = 8, 5
    shape = jax.ShapeDtypeStruct
    hbm = pl.BlockSpec(memory_space=pl.ANY)
    vmem = pl.BlockSpec(memory_space=pltpu.VMEM)
    dma = pltpu.SemaphoreType.DMA
    flops = 2 * both * (rows2 * (n1 + n2) + rows1 * n0)
    inputs = (x1, e1, x2, e2, x_real, x_fake, e0, dx, u0, u1, u2, v0, v1, v2, sig, cor)
    return pl.pallas_call(
        grad_kernel,
        out_shape=(
            shape((rows1, n0), F32), shape((rows2, n1), F32), shape((rows2, n2), F32), shape((n_rows, n0), F32), shape((n_rows, n0), F32),
            shape((rows1,), F32), shape((rows2,), F32), shape((rows2,), F32), shape((n0,), F32), shape((n1,), F32), shape((n2,), F32),
            shape((3,), F32), shape((1, 1), F32),
        ),
        in_specs=[hbm] * len(inputs),
        out_specs=[hbm] * 5 + [vmem] * 8,
        scratch_shapes=[
            pltpu.VMEM((both, n1), BF16), pltpu.VMEM((rows2, both), BF16), pltpu.VMEM((both, n2), BF16), pltpu.VMEM((rows2, both), BF16),
            pltpu.VMEM((both, n0), BF16), pltpu.VMEM((rows1, both), BF16), pltpu.VMEM(dx.shape, F32),
            pltpu.VMEM((rows1, n0), F32), pltpu.VMEM((rows2, n1), F32), pltpu.VMEM((rows2, n2), F32),
            *[pltpu.VMEM(array.shape, F32) for array in (u0, u1, u2, v0, v1, v2, sig, cor)],
            dma((15,)), dma((tiles1,)), dma((3,)), dma((tiles1,)), dma((tiles0,)),
        ],
        compiler_params=pltpu.CompilerParams(vmem_limit_bytes=67043328),
        cost_estimate=pl.CostEstimate(flops=flops, bytes_accessed=45 * 1024 * 1024, transcendentals=0),
        name="grads",
    )(*inputs)


def swap(values, bits):
    return lax.ppermute(values, "model", [(dev, dev ^ bits) for dev in range(4)])


def solution(mesh):
    rows_spec = P("rep", None)
    weight_spec = P(("rep", "model"), None)
    left_spec = P(("rep", "model"))
    target_spec = P("rep", "model")
    group_spec = P("rep")

    def local_step(x_real, x_fake, weight0, weight1, weight2, u_left0, u_left1, u_left2, t_real, t_fake):
        core = lax.axis_index("model") % 2
        x1, x2, e2, e1, e0, dx, sums, both, v0, v1, v2, u0, u1, u2, sig, cor = run_chain(x_real, x_fake, weight0, weight1, weight2, u_left0, u_left1, u_left2, t_real, t_fake)
        came = swap(sums, 2)
        dw0, dw1, dw2, dx_real, dx_fake, u0, u1, u2, v0, v1, v2, sigmas, loss = run_grads(x1, e1, x2, e2, x_real, x_fake, e0, dx, u0, u1, u2, v0, v1, v2, sig, cor)
        came, sigmas = lax.optimization_barrier((came, sigmas))
        came_mate = swap(came, 1)
        late = sums.shape[0]
        first = x_real.shape[0] - late

        def finish(dx_batch, batch_no):
            got = jnp.where(core == batch_no, came, came_mate)
            own = both[batch_no * late:(batch_no + 1) * late]
            dx_late = (own.astype(F32) + got.astype(F32)) / sigmas[0]
            return lax.dynamic_update_slice(dx_batch, dx_late, (first, 0))

        return (loss[0], finish(dx_real, 0), finish(dx_fake, 1), dw0, dw1, dw2, u0, u1, u2, v0, v1, v2, sigmas)

    return jax.shard_map(local_step, mesh=mesh, in_specs=(rows_spec, rows_spec, weight_spec, weight_spec, weight_spec, left_spec, left_spec, left_spec, target_spec, target_spec), out_specs=(group_spec, rows_spec, rows_spec, weight_spec, weight_spec, weight_spec, left_spec, left_spec, left_spec, group_spec, group_spec, group_spec, group_spec), check_vma=False)
```

```python
import functools

import jax
import jax.numpy as jnp
from jax import lax
from jax.experimental import pallas as pl
from jax.experimental.pallas import tpu as pltpu
from jax.sharding import PartitionSpec as P

SLOPE = 0.2
EPSILON = 1e-12
MESH = pl.DeviceIdType.MESH
CHUNKS = 4
EARLY = 2
PIECES = 4
TILE = 256
BF16 = jnp.bfloat16
F32 = jnp.float32


def leaky_relu(values):
    return jnp.where(values > 0, values, SLOPE * values)


def leaky_slope(values):
    return jnp.where(values > 0, 1.0, SLOPE)


def dot_t(left, right):
    return lax.dot_general(left, right, (((1,), (1,)), ((), ())), preferred_element_type=F32)


def dot_n(left, right):
    return lax.dot_general(left, right, (((1,), (0,)), ((), ())), preferred_element_type=F32)


def t_dot(left, right):
    return lax.dot_general(left, right, (((0,), (0,)), ((), ())), preferred_element_type=F32)


def fold(values):
    rows, cols = values.shape
    return jnp.sum(values.reshape(rows // 8, 8, cols), axis=0)


def total(values):
    return jnp.sum(jnp.sum(values, axis=1, keepdims=True), axis=0, keepdims=True)


def chain_kernel(x_real, x_fake, w0_in, w1_in, w2_in, u0_in, u1_in, u2_in, t_real, t_fake,
                 x1_out, x2_out, e2_out, e1_out, e0_out, dx_out, sum_out, both_out, v0_out, v1_out, v2_out, u0_out, u1_out, u2_out, sig_out, cor_out,
                 w0, w1, w1x, w2, x0, x1, x2, y0, y1, tt, e2_t, h2_own, h2_put, h2_got, e1, e1_t, e0, e0_t, h0_put, h0_got, dx,
                 p_buf, n_buf, c_buf,
                 eye, load_sem, put_sem, w_send, w_recv, w1x_send, w1x_recv, fwd_send, fwd_recv, small_send, small_recv,
                 x1_send, x1_recv, x2_send, x2_recv, h2_send, h2_recv, e1_send, e1_recv, h0_send, h0_recv, out_send, out_recv, dx_sem, dx_send, dx_recv, sum_sem, both_sem, both_send, both_recv):
    me = lax.axis_index("model")
    chip = me // 2
    core = me % 2
    other = 1 - chip
    mate = me + 1 - 2 * core
    far = me + 2 - 4 * chip
    diag = mate + 2 - 4 * chip
    n_rows, n0 = x0.shape
    wide1 = w0.shape[0]
    rows1 = wide1 // 2
    wide2 = w2.shape[0]
    rows2 = wide2 // 2
    n1 = 2 * wide1
    step = n_rows // CHUNKS
    piece = rows2 // PIECES

    def send(src, dst, send_sem, recv_sem, device):
        return pltpu.make_async_remote_copy(src_ref=src, dst_ref=dst, send_sem=send_sem, recv_sem=recv_sem, device_id={"model": device}, device_id_type=MESH)

    def part(index, size):
        return pl.ds(pl.multiple_of(index * size, size), size)

    barrier = pltpu.get_barrier_semaphore()
    for device in (mate, far, diag):
        pl.semaphore_signal(barrier, inc=1, device_id={"model": device}, device_id_type=MESH)
    pl.semaphore_wait(barrier, 3)

    def w1x_copy(piece_no):
        return send(
            w1_in.at[pl.ds(piece_no * piece, piece), part(other, wide1)],
            w1x.at[pl.ds(pl.multiple_of(core * rows2 + piece_no * piece, piece), piece), :],
            w1x_send.at[piece_no], w1x_recv.at[piece_no], far)

    def w1x_forward(piece_no):
        rows = w1x.at[pl.ds(pl.multiple_of(core * rows2 + piece_no * piece, piece), piece), :]
        return send(rows, rows, fwd_send.at[piece_no], fwd_recv.at[piece_no], mate)

    own1, own2 = part(core, rows1), part(core, rows2)
    loads = [
        pltpu.make_async_copy(w0_in, w0.at[own1, :], load_sem.at[0]),
        pltpu.make_async_copy(w1_in, w1.at[own2, :], load_sem.at[1]),
        pltpu.make_async_copy(w2_in, w2.at[own2, :], load_sem.at[2]),
    ]
    gives = [
        send(w0_in, w0.at[own1, :], w_send.at[0], w_recv.at[0], mate),
        send(w1_in, w1.at[own2, :], w_send.at[1], w_recv.at[1], mate),
        send(w2_in, w2.at[own2, :], w_send.at[2], w_recv.at[2], mate),
    ]
    loads[0].start()
    w1x_copy(0).start()
    for copy in loads[1:]:
        copy.start()

    def mine(x_in, t_own, t_mate):
        return (
            pltpu.make_async_copy(x_in, x0, load_sem.at[3]),
            pltpu.make_async_copy(t_own, tt.at[own2, :], load_sem.at[4]),
            send(t_mate, tt.at[own2, :], w_send.at[3], w_recv.at[3], mate),
        )

    @pl.when(core == 0)
    def _():
        for copy in mine(x_real, t_real, t_fake):
            copy.start()

    @pl.when(core == 1)
    def _():
        for copy in mine(x_fake, t_fake, t_real):
            copy.start()

    for copy in gives:
        copy.start()

    def row(values):
        return jnp.broadcast_to(values.reshape(1, values.size).astype(BF16), (16, values.size))

    lanes = lax.broadcasted_iota(jnp.int32, eye.shape, 1)
    eye[...] = jnp.where(lanes == lax.broadcasted_iota(jnp.int32, eye.shape, 0), 1.0, 0.0).astype(BF16)

    def store_transposed(dst, first, rows, values):
        for begin in range(0, values.shape[1], eye.shape[0]):
            size = min(eye.shape[0], values.shape[1] - begin)
            block = dot_t(eye[0:size, 0:size], values[:, begin:begin + size])
            dst[pl.ds(pl.multiple_of(first + begin, 128), size), rows] = block.astype(BF16)

    u_rows = [row(u0_in[...]), row(u1_in[...]), row(u2_in[...])]
    loads[0].wait()
    p_buf[me, :, pl.ds(0, n0)] = dot_n(u_rows[0], w0[own1, :])[0:1]
    loads[1].wait()

    def p1_tile(tile_no, carry):
        cols = part(tile_no, wide1 // 2)
        p_buf[me, :, pl.ds(pl.multiple_of(n0 + tile_no * (wide1 // 2), 128), wide1 // 2)] = dot_n(u_rows[1], w1[own2, cols])[0:1]
        return carry

    lax.fori_loop(0, 4, p1_tile, 0)
    loads[2].wait()
    p_buf[me, :, pl.ds(n0 + n1, wide2 * 2)] = dot_n(u_rows[2], w2[own2, :])[0:1]

    def spread(buf, first):
        return [send(buf.at[me], buf.at[me], small_send.at[first + which], small_recv.at[first + which], device) for which, device in enumerate((mate, far, diag))]

    p_copies = spread(p_buf, 0)
    for copy in p_copies:
        copy.start()
    w1x_copy(1).start()
    for copy in p_copies:
        copy.wait()
    p_all = p_buf[0] + p_buf[1] + p_buf[2] + p_buf[3]
    spans = ((0, n0, v0_out), (n0, n1, v1_out), (n0 + n1, 2 * wide2, v2_out))
    for first, size, v_out in spans:
        p_vec = p_all[:, first:first + size]
        v_out[...] = p_vec / jnp.maximum(jnp.sqrt(total(p_vec * p_vec)), EPSILON)
    u0_out[...] = dot_t(row(v0_out[...]), w0[own1, :])[0:1]
    u1_out[...] = dot_t(row(v1_out[...]), w1[own2, :])[0:1]
    u2_out[...] = dot_t(row(v2_out[...]), w2[own2, :])[0:1]
    lane = lax.broadcasted_iota(jnp.int32, (8, 128), 1)

    def pack(values):
        packed = jnp.zeros((8, 128), F32)
        for place, value in enumerate(values):
            packed = jnp.where(lane == place, value, packed)
        return packed

    n_buf[me] = pack([total(u_out[...] * u_out[...]) for u_out in (u0_out, u1_out, u2_out)])
    n_copies = spread(n_buf, 3)
    for copy in n_copies:
        copy.start()
    for piece_no in range(2, PIECES):
        w1x_copy(piece_no).start()
    for copy in n_copies:
        copy.wait()
    sigmas = jnp.sqrt(n_buf[0] + n_buf[1] + n_buf[2] + n_buf[3])
    sig_out[...] = sigmas
    sig0, sig1, sig2 = sigmas[0:1, 0:1], sigmas[0:1, 1:2], sigmas[0:1, 2:3]
    inv0, inv1, inv2 = 1.0 / sig0, 1.0 / sig1, 1.0 / sig2
    u0_out[...] = u0_out[...] / sig0
    u1_out[...] = u1_out[...] / sig1
    u2_out[...] = u2_out[...] / sig2

    pltpu.make_async_copy(x_real, x0, load_sem.at[3]).wait()
    gives[0].wait_recv()

    def y0_tile(tile_no, carry):
        cols = part(tile_no, TILE)
        y_tile = dot_t(x0[...], w0[cols, :]) * inv0
        y0[:, cols] = y_tile
        x1[chip, :, cols] = leaky_relu(y_tile).astype(BF16)
        return carry

    lax.fori_loop(0, wide1 // TILE, y0_tile, 0)

    def chunk_copy(buf, slot, chunk_no, send_sem, recv_sem):
        rows = buf.at[slot, part(chunk_no, step), :]
        return send(rows, rows, send_sem.at[chunk_no], recv_sem.at[chunk_no], far)

    for chunk_no in range(CHUNKS):
        chunk_copy(x1, chip, chunk_no, x1_send, x1_recv).start()

    batch = part(core, n_rows)

    def outputs(src, dst, which):
        return (
            pltpu.make_async_copy(src, dst, put_sem.at[which]),
            send(src, dst, out_send.at[which], out_recv.at[which], mate),
        )

    def halves(src, dst, size, which):
        return (
            pltpu.make_async_copy(src.at[part(core, size), :], dst.at[:, batch], put_sem.at[which]),
            send(src.at[part(1 - core, size), :], dst.at[:, batch], out_send.at[which], out_recv.at[which], mate),
        )

    x1_near = outputs(x1.at[chip], x1_out.at[batch, part(chip, wide1)], 0)
    for copy in x1_near:
        copy.start()
    for piece_no in range(PIECES):
        w1x_copy(piece_no).wait_recv()
        w1x_forward(piece_no).start()

    gives[1].wait_recv()

    def layer1(chunk_no, carry):
        rows = part(chunk_no, step)
        chunk_copy(x1, other, chunk_no, x1_send, x1_recv).wait_recv()
        y_val = (dot_t(x1[0, rows, :], w1[:, pl.ds(0, wide1)]) + dot_t(x1[1, rows, :], w1[:, pl.ds(wide1, wide1)])) * inv1
        y1[rows, :] = y_val
        x2[chip, rows, :] = leaky_relu(y_val).astype(BF16)
        chunk_copy(x2, chip, chunk_no, x2_send, x2_recv).start()
        return carry

    lax.fori_loop(0, CHUNKS, layer1, 0)
    x1_far = outputs(x1.at[other], x1_out.at[batch, part(other, wide1)], 1)
    for copy in x1_far:
        copy.start()

    gives[2].wait_recv()
    pltpu.make_async_copy(t_real, tt.at[own2, :], load_sem.at[4]).wait()
    t_give = send(t_real, tt.at[own2, :], w_send.at[3], w_recv.at[3], mate)
    t_give.wait_recv()

    def layer2(chunk_no, carry):
        corr2, loss = carry
        rows = part(chunk_no, step)
        chunk_copy(x2, other, chunk_no, x2_send, x2_recv).wait_recv()
        y_val = (dot_t(x2[0, rows, :], w2[:, pl.ds(0, wide2)]) + dot_t(x2[1, rows, :], w2[:, pl.ds(wide2, wide2)])) * inv2
        e_val = y_val - dot_t(eye[0:step, 0:step], tt[:, rows])
        corr2 = corr2 + fold(e_val * y_val)
        loss = loss + fold(e_val * e_val)
        e_half = e_val.astype(BF16)
        h2_put[rows, :] = dot_n(e_half, w2[:, part(other, wide2)]).astype(BF16)
        send(h2_put.at[rows, :], h2_got.at[rows, :], h2_send.at[chunk_no], h2_recv.at[chunk_no], far).start()
        h2_own[rows, :] = dot_n(e_half, w2[:, part(chip, wide2)])
        store_transposed(e2_t, 0, rows, e_half)
        return corr2, loss

    zero = jnp.zeros((8, wide2), F32)
    corr2, loss = lax.fori_loop(0, CHUNKS, layer2, (zero, zero))

    def back1(chunk_no, corr1):
        rows = part(chunk_no, step)
        send(h2_put.at[rows, :], h2_got.at[rows, :], h2_send.at[chunk_no], h2_recv.at[chunk_no], far).wait_recv()
        y_val = y1[rows, :]
        e_val = (h2_own[rows, :] + h2_got[rows, :].astype(F32)) * (inv2 * leaky_slope(y_val))
        e_half = e_val.astype(BF16)
        e1[chip, rows, :] = e_half
        chunk_copy(e1, chip, chunk_no, e1_send, e1_recv).start()
        store_transposed(e1_t, 0, rows, e_half)
        return corr1 + fold(e_val * y_val)

    corr1 = lax.fori_loop(0, CHUNKS, back1, zero)
    lesser = [
        outputs(x2.at[0], x2_out.at[batch, pl.ds(0, wide2)], 2),
        outputs(x2.at[1], x2_out.at[batch, pl.ds(wide2, wide2)], 3),
        halves(e2_t, e2_out, rows2, 4),
        halves(e1_t, e1_out, rows2, 5),
    ]
    for pair in lesser:
        for copy in pair:
            copy.start()
    for piece_no in range(PIECES):
        w1x_forward(piece_no).wait_recv()

    late = n_rows - EARLY * step

    def h0_copy(chunk_no):
        rows = part(chunk_no, step)
        return send(h0_put.at[rows, :], h0_got.at[rows, :], h0_send.at[chunk_no], h0_recv.at[chunk_no], far)

    def late_copies(chunk_no):
        src = h0_put.at[part(chunk_no, step), :]
        place = chunk_no - EARLY
        dst = both_out.at[pl.ds(pl.multiple_of(core * late + place * step, step), step), :]
        return (
            pltpu.make_async_copy(src, sum_out.at[part(place, step), :], sum_sem.at[place]),
            pltpu.make_async_copy(src, dst, both_sem.at[place]),
            send(src, dst, both_send.at[place], both_recv.at[place], mate),
        )

    def back0(chunk_no, corr0):
        rows = part(chunk_no, step)
        chunk_copy(e1, other, chunk_no, e1_send, e1_recv).wait_recv()

        def h1_tile(tile_no, corr):
            cols = part(tile_no, wide2)
            own_cols = pl.ds(pl.multiple_of(chip * wide1 + tile_no * wide2, 128), wide2)
            h_val = dot_n(e1[chip, rows, :], w1[:, own_cols]) + dot_n(e1[other, rows, :], w1x[:, cols])
            y_val = y0[rows, cols]
            e_val = h_val * (inv1 * leaky_slope(y_val))
            e0[:, cols] = e_val.astype(BF16)
            return corr + fold(e_val * y_val)

        corr0 = lax.fori_loop(0, wide1 // wide2, h1_tile, corr0)
        h0_put[rows, :] = dot_n(e0[...], w0[...]).astype(BF16)
        return corr0

    def transpose0(chunk_no):
        rows = part(chunk_no, step)

        def tile(tile_no, carry):
            store_transposed(e0_t, tile_no * wide2, rows, e0[:, part(tile_no, wide2)])
            return carry

        lax.fori_loop(0, wide1 // wide2, tile, 0)

    def back0_early(chunk_no, corr0):
        corr0 = back0(chunk_no, corr0)
        h0_copy(chunk_no).start()
        transpose0(chunk_no)
        return corr0

    def back0_late(chunk_no, corr0):
        corr0 = back0(chunk_no, corr0)
        for copy in late_copies(chunk_no):
            copy.start()
        transpose0(chunk_no)
        return corr0

    corr0 = lax.fori_loop(0, EARLY, back0_early, zero)
    corr0 = lax.fori_loop(EARLY, CHUNKS, back0_late, corr0)
    e0_pair = halves(e0_t, e0_out, rows1, 6)
    for copy in e0_pair:
        copy.start()
    c_buf[me] = pack([total(corr) for corr in (corr0, corr1, corr2, loss)])
    c_copies = spread(c_buf, 6)
    for copy in c_copies:
        copy.start()

    def dx_copies(chunk_no):
        rows = part(chunk_no, step)
        dst = dx_out.at[pl.ds(pl.multiple_of((core * EARLY + chunk_no) * step, step), step), :]
        return (
            pltpu.make_async_copy(dx.at[rows, :], dst, dx_sem.at[chunk_no]),
            send(dx.at[rows, :], dst, dx_send.at[chunk_no], dx_recv.at[chunk_no], mate),
        )

    def finish(chunk_no, carry):
        rows = part(chunk_no, step)
        h0_copy(chunk_no).wait_recv()
        dx[rows, :] = (h0_put[rows, :].astype(F32) + h0_got[rows, :].astype(F32)) * inv0
        for copy in dx_copies(chunk_no):
            copy.start()
        return carry

    lax.fori_loop(0, EARLY, finish, 0)
    for copy in c_copies:
        copy.wait()
    cor_out[...] = c_buf[0] + c_buf[1] + c_buf[2] + c_buf[3]

    for copy in gives:
        copy.wait_send()
    t_give.wait_send()
    for piece_no in range(PIECES):
        w1x_copy(piece_no).wait_send()
        w1x_forward(piece_no).wait_send()
    for pair in (x1_near, x1_far, *lesser, e0_pair):
        for copy in pair:
            copy.wait()

    def drain(chunk_no, carry):
        rows = part(chunk_no, step)
        chunk_copy(x1, chip, chunk_no, x1_send, x1_recv).wait_send()
        chunk_copy(x2, chip, chunk_no, x2_send, x2_recv).wait_send()
        send(h2_put.at[rows, :], h2_got.at[rows, :], h2_send.at[chunk_no], h2_recv.at[chunk_no], far).wait_send()
        chunk_copy(e1, chip, chunk_no, e1_send, e1_recv).wait_send()
        return carry

    lax.fori_loop(0, CHUNKS, drain, 0)

    def drain_early(chunk_no, carry):
        h0_copy(chunk_no).wait_send()
        for copy in dx_copies(chunk_no):
            copy.wait()
        return carry

    lax.fori_loop(0, EARLY, drain_early, 0)

    def drain_late(chunk_no, carry):
        for copy in late_copies(chunk_no):
            copy.wait()
        return carry

    lax.fori_loop(EARLY, CHUNKS, drain_late, 0)


def run_chain(x_real, x_fake, weight0, weight1, weight2, u_left0, u_left1, u_left2, t_real, t_fake):
    n_rows, n0 = x_real.shape
    rows1 = weight0.shape[0]
    rows2, n1 = weight1.shape
    wide1, wide2 = 2 * rows1, 2 * rows2
    n2 = 2 * wide2
    early = n_rows // CHUNKS * EARLY
    late = n_rows - early
    hbm = pl.BlockSpec(memory_space=pl.ANY)
    vmem = pl.BlockSpec(memory_space=pltpu.VMEM)
    shape = jax.ShapeDtypeStruct
    dma = pltpu.SemaphoreType.DMA
    return pl.pallas_call(
        chain_kernel,
        out_shape=(
            shape((2 * n_rows, n1), BF16), shape((2 * n_rows, n2), BF16), shape((rows2, 2 * n_rows), BF16), shape((rows2, 2 * n_rows), BF16),
            shape((rows1, 2 * n_rows), BF16), shape((2 * early, n0), F32), shape((late, n0), BF16), shape((2 * late, n0), BF16),
            shape((1, n0), F32), shape((1, n1), F32), shape((1, n2), F32),
            shape((1, rows1), F32), shape((1, rows2), F32), shape((1, rows2), F32),
            shape((8, 128), F32), shape((8, 128), F32),
        ),
        in_specs=[hbm] * 5 + [vmem] * 3 + [hbm] * 2,
        out_specs=[hbm] * 8 + [vmem] * 8,
        scratch_shapes=[
            pltpu.VMEM((wide1, n0), BF16), pltpu.VMEM((wide2, n1), BF16), pltpu.VMEM((wide2, wide1), BF16), pltpu.VMEM((wide2, n2), BF16),
            pltpu.VMEM((n_rows, n0), BF16), pltpu.VMEM((2, n_rows, wide1), BF16), pltpu.VMEM((2, n_rows, wide2), BF16),
            pltpu.VMEM((n_rows, wide1), F32), pltpu.VMEM((n_rows, wide2), F32), pltpu.VMEM((wide2, n_rows), BF16),
            pltpu.VMEM((wide2, n_rows), BF16), pltpu.VMEM((n_rows, wide2), F32), pltpu.VMEM((n_rows, wide2), BF16), pltpu.VMEM((n_rows, wide2), BF16),
            pltpu.VMEM((2, n_rows, wide2), BF16), pltpu.VMEM((wide2, n_rows), BF16), pltpu.VMEM((n_rows // CHUNKS, wide1), BF16), pltpu.VMEM((wide1, n_rows), BF16),
            pltpu.VMEM((n_rows, n0), BF16), pltpu.VMEM((early, n0), BF16), pltpu.VMEM((early, n0), F32),
            pltpu.VMEM((4, 1, n0 + n1 + n2), F32), pltpu.VMEM((4, 8, 128), F32), pltpu.VMEM((4, 8, 128), F32), pltpu.VMEM((256, 256), BF16),
            dma((5,)), dma((7,)), dma((4,)), dma((4,)), dma((PIECES,)), dma((PIECES,)), dma((PIECES,)), dma((PIECES,)), dma((9,)), dma((9,)),
            dma((CHUNKS,)), dma((CHUNKS,)), dma((CHUNKS,)), dma((CHUNKS,)), dma((CHUNKS,)), dma((CHUNKS,)),
            dma((CHUNKS,)), dma((CHUNKS,)), dma((EARLY,)), dma((EARLY,)), dma((7,)), dma((7,)), dma((EARLY,)), dma((EARLY,)), dma((EARLY,)),
            dma((CHUNKS - EARLY,)), dma((CHUNKS - EARLY,)), dma((CHUNKS - EARLY,)), dma((CHUNKS - EARLY,)),
        ],
        compiler_params=pltpu.CompilerParams(collective_id=0, has_side_effects=True, vmem_limit_bytes=67043328),
        name="chain",
    )(x_real, x_fake, weight0, weight1, weight2, u_left0, u_left1, u_left2, t_real.T, t_fake.T)


def grad_kernel(x1_in, e1_in, x2_in, e2_in, x_real, x_fake, e0_in, dx_in, u0_in, u1_in, u2_in, v0_in, v1_in, v2_in, sig_in, cor_in,
                dw0_out, dw1_out, dw2_out, dx_real, dx_fake, u0_out, u1_out, u2_out, v0_out, v1_out, v2_out, sig_out, loss_out,
                x1, e1, x2, e2, x0, e0, dx, dw0, dw1, dw2, u0, u1, u2, v0, v1, v2, sig, cor, in_sem, x1_sem, out_sem, dw1_sem, dw0_sem):
    n_rows = x_real.shape[0]
    early = dx.shape[0] // 2
    tiles1 = x1_sem.shape[0]
    tiles0 = dw0_sem.shape[0]
    wide1 = x1.shape[1] // tiles1
    wide0 = x0.shape[1] // tiles0

    def pull(src, dst, which):
        copy = pltpu.make_async_copy(src, dst, in_sem.at[which])
        copy.start()
        return copy

    small = [pull(src, dst, place) for place, (src, dst) in enumerate((
        (u0_in, u0), (u1_in, u1), (u2_in, u2), (v0_in, v0), (v1_in, v1), (v2_in, v2), (sig_in, sig), (cor_in, cor)))]
    got_e0 = pull(e0_in, e0, 8)
    got_x0 = [pull(x_real, x0.at[pl.ds(0, n_rows), :], 9), pull(x_fake, x0.at[pl.ds(n_rows, n_rows), :], 10)]
    got_e1 = pull(e1_in, e1, 11)

    def x1_copy(tile_no):
        cols = pl.ds(pl.multiple_of(tile_no * wide1, 128), wide1)
        return pltpu.make_async_copy(x1_in.at[:, cols], x1.at[:, cols], x1_sem.at[tile_no])

    for tile_no in range(tiles1):
        x1_copy(tile_no).start()
    got_dx = pull(dx_in, dx, 12)
    got_2 = [pull(e2_in, e2, 13), pull(x2_in, x2, 14)]

    for copy in small:
        copy.wait()
    for src, dst in ((u0, u0_out), (u1, u1_out), (u2, u2_out), (v0, v0_out), (v1, v1_out), (v2, v2_out)):
        dst[...] = src[...].reshape(dst.shape)
    sig_out[...] = sig[0:1, 0:3].reshape(3)
    loss_out[...] = cor[0:1, 3:4] * (0.5 / n_rows)

    def column(u_new, layer_no):
        return jnp.broadcast_to(u_new[...] * cor[0:1, layer_no:layer_no + 1], (128, u_new.shape[1])).T[:, 0:1]

    def scale(layer_no):
        return 1.0 / (n_rows * sig[0:1, layer_no:layer_no + 1])

    got_e0.wait()
    for copy in got_x0:
        copy.wait()
    col0, scale0 = column(u0, 0), scale(0)

    def dw0_copy(tile_no):
        cols = pl.ds(pl.multiple_of(tile_no * wide0, 128), wide0)
        return pltpu.make_async_copy(dw0.at[:, cols], dw0_out.at[:, cols], dw0_sem.at[tile_no])

    def dw0_tile(tile_no, carry):
        cols = pl.ds(pl.multiple_of(tile_no * wide0, 128), wide0)
        dw0[:, cols] = (dot_n(e0[...], x0[:, cols]) - col0 * v0[:, cols]) * scale0
        dw0_copy(tile_no).start()
        return carry

    lax.fori_loop(0, tiles0, dw0_tile, 0)
    got_e1.wait()
    col1, scale1 = column(u1, 1), scale(1)

    def dw1_copy(tile_no):
        cols = pl.ds(pl.multiple_of(tile_no * wide1, 128), wide1)
        return pltpu.make_async_copy(dw1.at[:, cols], dw1_out.at[:, cols], dw1_sem.at[tile_no])

    def dw1_tile(tile_no, carry):
        cols = pl.ds(pl.multiple_of(tile_no * wide1, 128), wide1)
        x1_copy(tile_no).wait()
        dw1[:, cols] = (dot_n(e1[...], x1[:, cols]) - col1 * v1[:, cols]) * scale1
        dw1_copy(tile_no).start()
        return carry

    lax.fori_loop(0, tiles1, dw1_tile, 0)
    got_dx.wait()
    pushes = [
        pltpu.make_async_copy(dx.at[pl.ds(0, early), :], dx_real.at[pl.ds(0, early), :], out_sem.at[0]),
        pltpu.make_async_copy(dx.at[pl.ds(early, early), :], dx_fake.at[pl.ds(0, early), :], out_sem.at[1]),
    ]
    for copy in pushes:
        copy.start()
    for copy in got_2:
        copy.wait()
    dw2[...] = (dot_n(e2[...], x2[...]) - column(u2, 2) * v2[...]) * scale(2)
    last = pltpu.make_async_copy(dw2, dw2_out, out_sem.at[2])
    last.start()

    def drain0(tile_no, carry):
        dw0_copy(tile_no).wait()
        return carry

    def drain1(tile_no, carry):
        dw1_copy(tile_no).wait()
        return carry

    lax.fori_loop(0, tiles0, drain0, 0)
    lax.fori_loop(0, tiles1, drain1, 0)
    for copy in (*pushes, last):
        copy.wait()


def run_grads(x1, e1, x2, e2, x_real, x_fake, e0, dx, u0, u1, u2, v0, v1, v2, sig, cor):
    both, n1 = x1.shape
    n_rows, n0 = x_real.shape
    n2 = x2.shape[1]
    rows2 = e1.shape[0]
    rows1 = e0.shape[0]
    tiles1, tiles0 = 8, 5
    shape = jax.ShapeDtypeStruct
    hbm = pl.BlockSpec(memory_space=pl.ANY)
    vmem = pl.BlockSpec(memory_space=pltpu.VMEM)
    dma = pltpu.SemaphoreType.DMA
    flops = 2 * both * (rows2 * (n1 + n2) + rows1 * n0)
    inputs = (x1, e1, x2, e2, x_real, x_fake, e0, dx, u0, u1, u2, v0, v1, v2, sig, cor)
    return pl.pallas_call(
        grad_kernel,
        out_shape=(
            shape((rows1, n0), F32), shape((rows2, n1), F32), shape((rows2, n2), F32), shape((n_rows, n0), F32), shape((n_rows, n0), F32),
            shape((rows1,), F32), shape((rows2,), F32), shape((rows2,), F32), shape((n0,), F32), shape((n1,), F32), shape((n2,), F32),
            shape((3,), F32), shape((1, 1), F32),
        ),
        in_specs=[hbm] * len(inputs),
        out_specs=[hbm] * 5 + [vmem] * 8,
        scratch_shapes=[
            pltpu.VMEM((both, n1), BF16), pltpu.VMEM((rows2, both), BF16), pltpu.VMEM((both, n2), BF16), pltpu.VMEM((rows2, both), BF16),
            pltpu.VMEM((both, n0), BF16), pltpu.VMEM((rows1, both), BF16), pltpu.VMEM(dx.shape, F32),
            pltpu.VMEM((rows1, n0), F32), pltpu.VMEM((rows2, n1), F32), pltpu.VMEM((rows2, n2), F32),
            *[pltpu.VMEM(array.shape, F32) for array in (u0, u1, u2, v0, v1, v2, sig, cor)],
            dma((15,)), dma((tiles1,)), dma((3,)), dma((tiles1,)), dma((tiles0,)),
        ],
        compiler_params=pltpu.CompilerParams(vmem_limit_bytes=67043328),
        cost_estimate=pl.CostEstimate(flops=flops, bytes_accessed=45 * 1024 * 1024, transcendentals=0),
        name="grads",
    )(*inputs)


def finish_kernel(flip, real_in, fake_in, both_in, came_in, sig_in, real_out, fake_out, both, came, sig, dx, in_sem, out_sem):
    me = lax.axis_index("model")
    batch = me % 2
    if flip:
        batch = 1 - batch
    pieces = out_sem.shape[0]
    late = both.shape[0]
    size = late // pieces
    first = real_out.shape[0] - late
    scale_copy = pltpu.make_async_copy(sig_in, sig, in_sem.at[2 * pieces])
    scale_copy.start()

    def pulls(piece):
        rows = pl.ds(piece * size, size)
        return (
            pltpu.make_async_copy(both_in.at[pl.ds(pl.multiple_of(batch * late + piece * size, size), size), :], both.at[rows, :], in_sem.at[2 * piece]),
            pltpu.make_async_copy(came_in.at[rows, :], came.at[rows, :], in_sem.at[2 * piece + 1]),
        )

    def push(dst, piece):
        return pltpu.make_async_copy(dx.at[pl.ds(piece * size, size), :], dst.at[pl.ds(first + piece * size, size), :], out_sem.at[piece])

    for piece in range(pieces):
        for copy in pulls(piece):
            copy.start()
    scale_copy.wait()
    inv0 = 1.0 / sig[0:1, 0:1]
    for piece in range(pieces):
        for copy in pulls(piece):
            copy.wait()
        rows = pl.ds(piece * size, size)
        dx[rows, :] = (both[rows, :].astype(F32) + came[rows, :].astype(F32)) * inv0

        @pl.when(batch == 0)
        def _():
            push(real_out, piece).start()

        @pl.when(batch == 1)
        def _():
            push(fake_out, piece).start()

    for piece in range(pieces):
        push(real_out, piece).wait()


def run_finish(flip, dx_real, dx_fake, both, came, sig):
    late, n0 = came.shape
    pieces = 4
    hbm = pl.BlockSpec(memory_space=pl.ANY)
    dma = pltpu.SemaphoreType.DMA
    shape = jax.ShapeDtypeStruct(dx_real.shape, F32)
    return pl.pallas_call(
        functools.partial(finish_kernel, flip),
        out_shape=(shape, shape),
        in_specs=[hbm] * 5,
        out_specs=[hbm] * 2,
        scratch_shapes=[
            pltpu.VMEM((late, n0), BF16), pltpu.VMEM((late, n0), BF16), pltpu.VMEM((8, 128), F32), pltpu.VMEM((late, n0), F32),
            dma((2 * pieces + 1,)), dma((pieces,)),
        ],
        input_output_aliases={0: 0, 1: 1},
        compiler_params=pltpu.CompilerParams(vmem_limit_bytes=67043328),
        cost_estimate=pl.CostEstimate(flops=4 * late * n0, bytes_accessed=8 * late * n0, transcendentals=0),
        name="finish",
    )(dx_real, dx_fake, both, came, sig)


def swap(values, bits):
    return lax.ppermute(values, "model", [(dev, dev ^ bits) for dev in range(4)])


def solution(mesh):
    rows_spec = P("rep", None)
    weight_spec = P(("rep", "model"), None)
    left_spec = P(("rep", "model"))
    target_spec = P("rep", "model")
    group_spec = P("rep")

    def local_step(x_real, x_fake, weight0, weight1, weight2, u_left0, u_left1, u_left2, t_real, t_fake):
        x1, x2, e2, e1, e0, dx, sums, both, v0, v1, v2, u0, u1, u2, sig, cor = run_chain(x_real, x_fake, weight0, weight1, weight2, u_left0, u_left1, u_left2, t_real, t_fake)
        came = swap(sums, 2)
        dw0, dw1, dw2, dx_real, dx_fake, u0, u1, u2, v0, v1, v2, sigmas, loss = run_grads(x1, e1, x2, e2, x_real, x_fake, e0, dx, u0, u1, u2, v0, v1, v2, sig, cor)
        came, sigmas = lax.optimization_barrier((came, sigmas))
        came_mate = swap(came, 1)
        dx_real, dx_fake = run_finish(False, dx_real, dx_fake, both, came, sig)
        dx_real, dx_fake = run_finish(True, dx_real, dx_fake, both, came_mate, sig)
        return (loss[0], dx_real, dx_fake, dw0, dw1, dw2, u0, u1, u2, v0, v1, v2, sigmas)

    return jax.shard_map(local_step, mesh=mesh, in_specs=(rows_spec, rows_spec, weight_spec, weight_spec, weight_spec, left_spec, left_spec, left_spec, target_spec, target_spec), out_specs=(group_spec, rows_spec, rows_spec, weight_spec, weight_spec, weight_spec, left_spec, left_spec, left_spec, group_spec, group_spec, group_spec, group_spec), check_vma=False)
```

```python
import functools

import jax
import jax.numpy as jnp
from jax import lax
from jax.experimental import pallas as pl
from jax.experimental.pallas import tpu as pltpu
from jax.sharding import PartitionSpec as P

SLOPE = 0.2
EPSILON = 1e-12
MESH = pl.DeviceIdType.MESH
CHUNKS = 4
EARLY = 2
PIECES = 4
TILE = 256
BF16 = jnp.bfloat16
F32 = jnp.float32


def leaky_relu(values):
    return jnp.where(values > 0, values, SLOPE * values)


def leaky_slope(values):
    return jnp.where(values > 0, 1.0, SLOPE)


def dot_t(left, right):
    return lax.dot_general(left, right, (((1,), (1,)), ((), ())), preferred_element_type=F32)


def dot_n(left, right):
    return lax.dot_general(left, right, (((1,), (0,)), ((), ())), preferred_element_type=F32)


def t_dot(left, right):
    return lax.dot_general(left, right, (((0,), (0,)), ((), ())), preferred_element_type=F32)


def fold(values):
    rows, cols = values.shape
    return jnp.sum(values.reshape(rows // 8, 8, cols), axis=0)


def total(values):
    return jnp.sum(jnp.sum(values, axis=1, keepdims=True), axis=0, keepdims=True)


def chain_kernel(x_real, x_fake, w0_in, w1_in, w2_in, u0_in, u1_in, u2_in, t_real, t_fake,
                 x1_out, x2_out, e2_out, e1_out, e0_out, dx_out, sum_out, both_out, v0_out, v1_out, v2_out, u0_out, u1_out, u2_out, sig_out, cor_out,
                 w0, w1, w1x, w2, x0, x1, x2, y0, y1, tt, e2_t, h2_own, h2_put, h2_got, e1, e1_t, e0, e0_t, h0_put, h0_got, dx,
                 p_buf, p_sum, n_buf, c_buf,
                 eye, load_sem, put_sem, w_send, w_recv, w1x_send, w1x_recv, fwd_send, fwd_recv, small_send, small_recv,
                 x1_send, x1_recv, x2_send, x2_recv, h2_send, h2_recv, e1_send, e1_recv, h0_send, h0_recv, out_send, out_recv, dx_sem, dx_send, dx_recv, sum_sem, both_sem, both_send, both_recv):
    me = lax.axis_index("model")
    chip = me // 2
    core = me % 2
    other = 1 - chip
    mate = me + 1 - 2 * core
    far = me + 2 - 4 * chip
    diag = mate + 2 - 4 * chip
    n_rows, n0 = x0.shape
    wide1 = w0.shape[0]
    rows1 = wide1 // 2
    wide2 = w2.shape[0]
    rows2 = wide2 // 2
    n1 = 2 * wide1
    step = n_rows // CHUNKS
    piece = rows2 // PIECES

    def send(src, dst, send_sem, recv_sem, device):
        return pltpu.make_async_remote_copy(src_ref=src, dst_ref=dst, send_sem=send_sem, recv_sem=recv_sem, device_id={"model": device}, device_id_type=MESH)

    def part(index, size):
        return pl.ds(pl.multiple_of(index * size, size), size)

    barrier = pltpu.get_barrier_semaphore()
    for device in (mate, far, diag):
        pl.semaphore_signal(barrier, inc=1, device_id={"model": device}, device_id_type=MESH)
    pl.semaphore_wait(barrier, 3)

    def w1x_copy(piece_no):
        return send(
            w1_in.at[pl.ds(piece_no * piece, piece), part(other, wide1)],
            w1x.at[pl.ds(pl.multiple_of(core * rows2 + piece_no * piece, piece), piece), :],
            w1x_send.at[piece_no], w1x_recv.at[piece_no], far)

    def w1x_forward(piece_no):
        rows = w1x.at[pl.ds(pl.multiple_of(core * rows2 + piece_no * piece, piece), piece), :]
        return send(rows, rows, fwd_send.at[piece_no], fwd_recv.at[piece_no], mate)

    own1, own2 = part(core, rows1), part(core, rows2)
    loads = [
        pltpu.make_async_copy(w0_in, w0.at[own1, :], load_sem.at[0]),
        pltpu.make_async_copy(w1_in, w1.at[own2, :], load_sem.at[1]),
        pltpu.make_async_copy(w2_in, w2.at[own2, :], load_sem.at[2]),
    ]
    gives = [
        send(w0_in, w0.at[own1, :], w_send.at[0], w_recv.at[0], mate),
        send(w1_in, w1.at[own2, :], w_send.at[1], w_recv.at[1], mate),
        send(w2_in, w2.at[own2, :], w_send.at[2], w_recv.at[2], mate),
    ]
    loads[0].start()
    w1x_copy(0).start()
    for copy in loads[1:]:
        copy.start()

    def mine(x_in, t_own, t_mate):
        return (
            pltpu.make_async_copy(x_in, x0, load_sem.at[3]),
            pltpu.make_async_copy(t_own, tt.at[own2, :], load_sem.at[4]),
            send(t_mate, tt.at[own2, :], w_send.at[3], w_recv.at[3], mate),
        )

    @pl.when(core == 0)
    def _():
        for copy in mine(x_real, t_real, t_fake):
            copy.start()

    @pl.when(core == 1)
    def _():
        for copy in mine(x_fake, t_fake, t_real):
            copy.start()

    for copy in gives:
        copy.start()

    def row(values):
        return jnp.broadcast_to(values.reshape(1, values.size).astype(BF16), (16, values.size))

    lanes = lax.broadcasted_iota(jnp.int32, eye.shape, 1)
    eye[...] = jnp.where(lanes == lax.broadcasted_iota(jnp.int32, eye.shape, 0), 1.0, 0.0).astype(BF16)

    def store_transposed(dst, first, rows, values):
        for begin in range(0, values.shape[1], eye.shape[0]):
            size = min(eye.shape[0], values.shape[1] - begin)
            block = dot_t(eye[0:size, 0:size], values[:, begin:begin + size])
            dst[pl.ds(pl.multiple_of(first + begin, 128), size), rows] = block.astype(BF16)

    u_rows = [row(u0_in[...]), row(u1_in[...]), row(u2_in[...])]
    loads[0].wait()
    p_buf[me, :, pl.ds(0, n0)] = dot_n(u_rows[0], w0[own1, :])[0:1]
    loads[1].wait()

    def p1_tile(tile_no, carry):
        cols = part(tile_no, wide1 // 2)
        p_buf[me, :, pl.ds(pl.multiple_of(n0 + tile_no * (wide1 // 2), 128), wide1 // 2)] = dot_n(u_rows[1], w1[own2, cols])[0:1]
        return carry

    lax.fori_loop(0, 4, p1_tile, 0)
    loads[2].wait()
    p_buf[me, :, pl.ds(n0 + n1, wide2 * 2)] = dot_n(u_rows[2], w2[own2, :])[0:1]

    def spread(buf, first):
        return [send(buf.at[me], buf.at[me], small_send.at[first + which], small_recv.at[first + which], device) for which, device in enumerate((mate, far, diag))]

    p_near = send(p_buf.at[me], p_buf.at[me], small_send.at[0], small_recv.at[0], mate)
    p_near.start()
    p_near.wait()
    p_sum[chip] = p_buf[2 * chip] + p_buf[2 * chip + 1]
    p_far = send(p_sum.at[chip], p_sum.at[chip], small_send.at[1], small_recv.at[1], far)
    p_far.start()
    w1x_copy(1).start()
    p_far.wait()
    p_all = p_sum[0] + p_sum[1]
    spans = ((0, n0, v0_out), (n0, n1, v1_out), (n0 + n1, 2 * wide2, v2_out))
    for first, size, v_out in spans:
        p_vec = p_all[:, first:first + size]
        v_out[...] = p_vec / jnp.maximum(jnp.sqrt(total(p_vec * p_vec)), EPSILON)
    u0_out[...] = dot_t(row(v0_out[...]), w0[own1, :])[0:1]
    u1_out[...] = dot_t(row(v1_out[...]), w1[own2, :])[0:1]
    u2_out[...] = dot_t(row(v2_out[...]), w2[own2, :])[0:1]
    lane = lax.broadcasted_iota(jnp.int32, (8, 128), 1)

    def pack(values):
        packed = jnp.zeros((8, 128), F32)
        for place, value in enumerate(values):
            packed = jnp.where(lane == place, value, packed)
        return packed

    n_buf[me] = pack([total(u_out[...] * u_out[...]) for u_out in (u0_out, u1_out, u2_out)])
    n_copies = spread(n_buf, 3)
    for copy in n_copies:
        copy.start()
    for piece_no in range(2, PIECES):
        w1x_copy(piece_no).start()
    for copy in n_copies:
        copy.wait()
    sigmas = jnp.sqrt(n_buf[0] + n_buf[1] + n_buf[2] + n_buf[3])
    sig_out[...] = sigmas
    sig0, sig1, sig2 = sigmas[0:1, 0:1], sigmas[0:1, 1:2], sigmas[0:1, 2:3]
    inv0, inv1, inv2 = 1.0 / sig0, 1.0 / sig1, 1.0 / sig2
    u0_out[...] = u0_out[...] / sig0
    u1_out[...] = u1_out[...] / sig1
    u2_out[...] = u2_out[...] / sig2

    pltpu.make_async_copy(x_real, x0, load_sem.at[3]).wait()
    gives[0].wait_recv()

    def y0_tile(tile_no, carry):
        cols = part(tile_no, TILE)
        y_tile = dot_t(x0[...], w0[cols, :]) * inv0
        y0[:, cols] = y_tile
        x1[chip, :, cols] = leaky_relu(y_tile).astype(BF16)
        return carry

    lax.fori_loop(0, wide1 // TILE, y0_tile, 0)

    def chunk_copy(buf, slot, chunk_no, send_sem, recv_sem):
        rows = buf.at[slot, part(chunk_no, step), :]
        return send(rows, rows, send_sem.at[chunk_no], recv_sem.at[chunk_no], far)

    for chunk_no in range(CHUNKS):
        chunk_copy(x1, chip, chunk_no, x1_send, x1_recv).start()

    batch = part(core, n_rows)

    def outputs(src, dst, which):
        return (
            pltpu.make_async_copy(src, dst, put_sem.at[which]),
            send(src, dst, out_send.at[which], out_recv.at[which], mate),
        )

    def halves(src, dst, size, which):
        return (
            pltpu.make_async_copy(src.at[part(core, size), :], dst.at[:, batch], put_sem.at[which]),
            send(src.at[part(1 - core, size), :], dst.at[:, batch], out_send.at[which], out_recv.at[which], mate),
        )

    x1_near = outputs(x1.at[chip], x1_out.at[batch, part(chip, wide1)], 0)
    for copy in x1_near:
        copy.start()
    for piece_no in range(PIECES):
        w1x_copy(piece_no).wait_recv()
        w1x_forward(piece_no).start()

    gives[1].wait_recv()

    def layer1(chunk_no, carry):
        rows = part(chunk_no, step)
        chunk_copy(x1, other, chunk_no, x1_send, x1_recv).wait_recv()
        y_val = (dot_t(x1[0, rows, :], w1[:, pl.ds(0, wide1)]) + dot_t(x1[1, rows, :], w1[:, pl.ds(wide1, wide1)])) * inv1
        y1[rows, :] = y_val
        x2[chip, rows, :] = leaky_relu(y_val).astype(BF16)
        chunk_copy(x2, chip, chunk_no, x2_send, x2_recv).start()
        return carry

    lax.fori_loop(0, CHUNKS, layer1, 0)
    x1_far = outputs(x1.at[other], x1_out.at[batch, part(other, wide1)], 1)
    for copy in x1_far:
        copy.start()

    gives[2].wait_recv()
    pltpu.make_async_copy(t_real, tt.at[own2, :], load_sem.at[4]).wait()
    t_give = send(t_real, tt.at[own2, :], w_send.at[3], w_recv.at[3], mate)
    t_give.wait_recv()

    def layer2(chunk_no, carry):
        corr2, loss = carry
        rows = part(chunk_no, step)
        chunk_copy(x2, other, chunk_no, x2_send, x2_recv).wait_recv()
        y_val = (dot_t(x2[0, rows, :], w2[:, pl.ds(0, wide2)]) + dot_t(x2[1, rows, :], w2[:, pl.ds(wide2, wide2)])) * inv2
        e_val = y_val - dot_t(eye[0:step, 0:step], tt[:, rows])
        corr2 = corr2 + fold(e_val * y_val)
        loss = loss + fold(e_val * e_val)
        e_half = e_val.astype(BF16)
        h2_put[rows, :] = dot_n(e_half, w2[:, part(other, wide2)]).astype(BF16)
        send(h2_put.at[rows, :], h2_got.at[rows, :], h2_send.at[chunk_no], h2_recv.at[chunk_no], far).start()
        h2_own[rows, :] = dot_n(e_half, w2[:, part(chip, wide2)])
        store_transposed(e2_t, 0, rows, e_half)
        return corr2, loss

    zero = jnp.zeros((8, wide2), F32)
    corr2, loss = lax.fori_loop(0, CHUNKS, layer2, (zero, zero))

    def back1(chunk_no, corr1):
        rows = part(chunk_no, step)
        send(h2_put.at[rows, :], h2_got.at[rows, :], h2_send.at[chunk_no], h2_recv.at[chunk_no], far).wait_recv()
        y_val = y1[rows, :]
        e_val = (h2_own[rows, :] + h2_got[rows, :].astype(F32)) * (inv2 * leaky_slope(y_val))
        e_half = e_val.astype(BF16)
        e1[chip, rows, :] = e_half
        chunk_copy(e1, chip, chunk_no, e1_send, e1_recv).start()
        store_transposed(e1_t, 0, rows, e_half)
        return corr1 + fold(e_val * y_val)

    corr1 = lax.fori_loop(0, CHUNKS, back1, zero)
    lesser = [
        outputs(x2.at[0], x2_out.at[batch, pl.ds(0, wide2)], 2),
        outputs(x2.at[1], x2_out.at[batch, pl.ds(wide2, wide2)], 3),
        halves(e2_t, e2_out, rows2, 4),
        halves(e1_t, e1_out, rows2, 5),
    ]
    for pair in lesser:
        for copy in pair:
            copy.start()
    for piece_no in range(PIECES):
        w1x_forward(piece_no).wait_recv()

    late = n_rows - EARLY * step

    def h0_copy(chunk_no):
        rows = part(chunk_no, step)
        return send(h0_put.at[rows, :], h0_got.at[rows, :], h0_send.at[chunk_no], h0_recv.at[chunk_no], far)

    def late_copies(chunk_no):
        src = h0_put.at[part(chunk_no, step), :]
        place = chunk_no - EARLY
        dst = both_out.at[pl.ds(pl.multiple_of(core * late + place * step, step), step), :]
        return (
            pltpu.make_async_copy(src, sum_out.at[part(place, step), :], sum_sem.at[place]),
            pltpu.make_async_copy(src, dst, both_sem.at[place]),
            send(src, dst, both_send.at[place], both_recv.at[place], mate),
        )

    def back0(chunk_no, corr0):
        rows = part(chunk_no, step)
        chunk_copy(e1, other, chunk_no, e1_send, e1_recv).wait_recv()

        def h1_tile(tile_no, corr):
            cols = part(tile_no, wide2)
            own_cols = pl.ds(pl.multiple_of(chip * wide1 + tile_no * wide2, 128), wide2)
            h_val = dot_n(e1[chip, rows, :], w1[:, own_cols]) + dot_n(e1[other, rows, :], w1x[:, cols])
            y_val = y0[rows, cols]
            e_val = h_val * (inv1 * leaky_slope(y_val))
            e0[:, cols] = e_val.astype(BF16)
            return corr + fold(e_val * y_val)

        corr0 = lax.fori_loop(0, wide1 // wide2, h1_tile, corr0)
        h0_put[rows, :] = dot_n(e0[...], w0[...]).astype(BF16)
        return corr0

    def transpose0(chunk_no):
        rows = part(chunk_no, step)

        def tile(tile_no, carry):
            store_transposed(e0_t, tile_no * wide2, rows, e0[:, part(tile_no, wide2)])
            return carry

        lax.fori_loop(0, wide1 // wide2, tile, 0)

    def back0_early(chunk_no, corr0):
        corr0 = back0(chunk_no, corr0)
        h0_copy(chunk_no).start()
        transpose0(chunk_no)
        return corr0

    def back0_late(chunk_no, corr0):
        corr0 = back0(chunk_no, corr0)
        for copy in late_copies(chunk_no):
            copy.start()
        transpose0(chunk_no)
        return corr0

    corr0 = lax.fori_loop(0, EARLY, back0_early, zero)
    corr0 = lax.fori_loop(EARLY, CHUNKS, back0_late, corr0)
    e0_pair = halves(e0_t, e0_out, rows1, 6)
    for copy in e0_pair:
        copy.start()
    c_buf[me] = pack([total(corr) for corr in (corr0, corr1, corr2, loss)])
    c_copies = spread(c_buf, 6)
    for copy in c_copies:
        copy.start()

    def dx_copies(chunk_no):
        rows = part(chunk_no, step)
        dst = dx_out.at[pl.ds(pl.multiple_of((core * EARLY + chunk_no) * step, step), step), :]
        return (
            pltpu.make_async_copy(dx.at[rows, :], dst, dx_sem.at[chunk_no]),
            send(dx.at[rows, :], dst, dx_send.at[chunk_no], dx_recv.at[chunk_no], mate),
        )

    def finish(chunk_no, carry):
        rows = part(chunk_no, step)
        h0_copy(chunk_no).wait_recv()
        dx[rows, :] = (h0_put[rows, :].astype(F32) + h0_got[rows, :].astype(F32)) * inv0
        for copy in dx_copies(chunk_no):
            copy.start()
        return carry

    lax.fori_loop(0, EARLY, finish, 0)
    for copy in c_copies:
        copy.wait()
    cor_out[...] = c_buf[0] + c_buf[1] + c_buf[2] + c_buf[3]

    for copy in gives:
        copy.wait_send()
    t_give.wait_send()
    for piece_no in range(PIECES):
        w1x_copy(piece_no).wait_send()
        w1x_forward(piece_no).wait_send()
    for pair in (x1_near, x1_far, *lesser, e0_pair):
        for copy in pair:
            copy.wait()

    def drain(chunk_no, carry):
        rows = part(chunk_no, step)
        chunk_copy(x1, chip, chunk_no, x1_send, x1_recv).wait_send()
        chunk_copy(x2, chip, chunk_no, x2_send, x2_recv).wait_send()
        send(h2_put.at[rows, :], h2_got.at[rows, :], h2_send.at[chunk_no], h2_recv.at[chunk_no], far).wait_send()
        chunk_copy(e1, chip, chunk_no, e1_send, e1_recv).wait_send()
        return carry

    lax.fori_loop(0, CHUNKS, drain, 0)

    def drain_early(chunk_no, carry):
        h0_copy(chunk_no).wait_send()
        for copy in dx_copies(chunk_no):
            copy.wait()
        return carry

    lax.fori_loop(0, EARLY, drain_early, 0)

    def drain_late(chunk_no, carry):
        for copy in late_copies(chunk_no):
            copy.wait()
        return carry

    lax.fori_loop(EARLY, CHUNKS, drain_late, 0)


def run_chain(x_real, x_fake, weight0, weight1, weight2, u_left0, u_left1, u_left2, t_real, t_fake):
    n_rows, n0 = x_real.shape
    rows1 = weight0.shape[0]
    rows2, n1 = weight1.shape
    wide1, wide2 = 2 * rows1, 2 * rows2
    n2 = 2 * wide2
    early = n_rows // CHUNKS * EARLY
    late = n_rows - early
    hbm = pl.BlockSpec(memory_space=pl.ANY)
    vmem = pl.BlockSpec(memory_space=pltpu.VMEM)
    shape = jax.ShapeDtypeStruct
    dma = pltpu.SemaphoreType.DMA
    return pl.pallas_call(
        chain_kernel,
        out_shape=(
            shape((2 * n_rows, n1), BF16), shape((2 * n_rows, n2), BF16), shape((rows2, 2 * n_rows), BF16), shape((rows2, 2 * n_rows), BF16),
            shape((rows1, 2 * n_rows), BF16), shape((2 * early, n0), F32), shape((late, n0), BF16), shape((2 * late, n0), BF16),
            shape((1, n0), F32), shape((1, n1), F32), shape((1, n2), F32),
            shape((1, rows1), F32), shape((1, rows2), F32), shape((1, rows2), F32),
            shape((8, 128), F32), shape((8, 128), F32),
        ),
        in_specs=[hbm] * 5 + [vmem] * 3 + [hbm] * 2,
        out_specs=[hbm] * 8 + [vmem] * 8,
        scratch_shapes=[
            pltpu.VMEM((wide1, n0), BF16), pltpu.VMEM((wide2, n1), BF16), pltpu.VMEM((wide2, wide1), BF16), pltpu.VMEM((wide2, n2), BF16),
            pltpu.VMEM((n_rows, n0), BF16), pltpu.VMEM((2, n_rows, wide1), BF16), pltpu.VMEM((2, n_rows, wide2), BF16),
            pltpu.VMEM((n_rows, wide1), F32), pltpu.VMEM((n_rows, wide2), F32), pltpu.VMEM((wide2, n_rows), BF16),
            pltpu.VMEM((wide2, n_rows), BF16), pltpu.VMEM((n_rows, wide2), F32), pltpu.VMEM((n_rows, wide2), BF16), pltpu.VMEM((n_rows, wide2), BF16),
            pltpu.VMEM((2, n_rows, wide2), BF16), pltpu.VMEM((wide2, n_rows), BF16), pltpu.VMEM((n_rows // CHUNKS, wide1), BF16), pltpu.VMEM((wide1, n_rows), BF16),
            pltpu.VMEM((n_rows, n0), BF16), pltpu.VMEM((early, n0), BF16), pltpu.VMEM((early, n0), F32),
            pltpu.VMEM((4, 1, n0 + n1 + n2), F32), pltpu.VMEM((2, 1, n0 + n1 + n2), F32), pltpu.VMEM((4, 8, 128), F32), pltpu.VMEM((4, 8, 128), F32), pltpu.VMEM((256, 256), BF16),
            dma((5,)), dma((7,)), dma((4,)), dma((4,)), dma((PIECES,)), dma((PIECES,)), dma((PIECES,)), dma((PIECES,)), dma((9,)), dma((9,)),
            dma((CHUNKS,)), dma((CHUNKS,)), dma((CHUNKS,)), dma((CHUNKS,)), dma((CHUNKS,)), dma((CHUNKS,)),
            dma((CHUNKS,)), dma((CHUNKS,)), dma((EARLY,)), dma((EARLY,)), dma((7,)), dma((7,)), dma((EARLY,)), dma((EARLY,)), dma((EARLY,)),
            dma((CHUNKS - EARLY,)), dma((CHUNKS - EARLY,)), dma((CHUNKS - EARLY,)), dma((CHUNKS - EARLY,)),
        ],
        compiler_params=pltpu.CompilerParams(collective_id=0, has_side_effects=True, vmem_limit_bytes=67043328),
        name="chain",
    )(x_real, x_fake, weight0, weight1, weight2, u_left0, u_left1, u_left2, t_real.T, t_fake.T)


def grad_kernel(x1_in, e1_in, x2_in, e2_in, x_real, x_fake, e0_in, dx_in, u0_in, u1_in, u2_in, v0_in, v1_in, v2_in, sig_in, cor_in,
                dw0_out, dw1_out, dw2_out, dx_real, dx_fake, u0_out, u1_out, u2_out, v0_out, v1_out, v2_out, sig_out, loss_out,
                x1, e1, x2, e2, x0, e0, dx, dw0, dw1, dw2, u0, u1, u2, v0, v1, v2, sig, cor, in_sem, x1_sem, out_sem, dw1_sem, dw0_sem):
    n_rows = x_real.shape[0]
    early = dx.shape[0] // 2
    tiles1 = x1_sem.shape[0]
    tiles0 = dw0_sem.shape[0]

    def pull(src, dst, which):
        copy = pltpu.make_async_copy(src, dst, in_sem.at[which])
        copy.start()
        return copy

    small = [pull(src, dst, place) for place, (src, dst) in enumerate((
        (u0_in, u0), (u1_in, u1), (u2_in, u2), (v0_in, v0), (v1_in, v1), (v2_in, v2), (sig_in, sig), (cor_in, cor)))]
    def tile_of(size, tiles, tile_no):
        return pl.ds(tile_no * (size // tiles), size // tiles)

    got_e1 = pull(e1_in, e1, 11)
    got_x1 = []
    for tile_no in range(tiles1):
        cols = tile_of(x1.shape[1], tiles1, tile_no)
        copy = pltpu.make_async_copy(x1_in.at[:, cols], x1.at[:, cols], x1_sem.at[tile_no])
        copy.start()
        got_x1.append(copy)
    got_e0 = pull(e0_in, e0, 8)
    got_x0 = [pull(x_real, x0.at[pl.ds(0, n_rows), :], 9), pull(x_fake, x0.at[pl.ds(n_rows, n_rows), :], 10)]
    got_dx = pull(dx_in, dx, 12)
    got_2 = [pull(e2_in, e2, 13), pull(x2_in, x2, 14)]

    for copy in small:
        copy.wait()
    for src, dst in ((u0, u0_out), (u1, u1_out), (u2, u2_out), (v0, v0_out), (v1, v1_out), (v2, v2_out)):
        dst[...] = src[...].reshape(dst.shape)
    sig_out[...] = sig[0:1, 0:3].reshape(3)
    loss_out[...] = cor[0:1, 3:4] * (0.5 / n_rows)

    def column(u_new, layer_no):
        return jnp.broadcast_to(u_new[...] * cor[0:1, layer_no:layer_no + 1], (128, u_new.shape[1])).T[:, 0:1]

    def scale(layer_no):
        return 1.0 / (n_rows * sig[0:1, layer_no:layer_no + 1])

    pushes = []

    def gradient(errors, layer_in, cols, col, v_new, rate, dst, out, sem):
        dst[:, cols] = (dot_n(errors[...], layer_in[:, cols]) - col * v_new[:, cols]) * rate
        copy = pltpu.make_async_copy(dst.at[:, cols], out.at[:, cols], sem)
        copy.start()
        pushes.append(copy)

    got_e1.wait()
    col1, scale1 = column(u1, 1), scale(1)
    for tile_no in range(tiles1):
        got_x1[tile_no].wait()
        gradient(e1, x1, tile_of(x1.shape[1], tiles1, tile_no), col1, v1, scale1, dw1, dw1_out, dw1_sem.at[tile_no])
    got_dx.wait()
    for place, dst in enumerate((dx_real, dx_fake)):
        copy = pltpu.make_async_copy(dx.at[pl.ds(place * early, early), :], dst.at[pl.ds(0, early), :], out_sem.at[place])
        copy.start()
        pushes.append(copy)
    got_e0.wait()
    for copy in got_x0:
        copy.wait()
    col0, scale0 = column(u0, 0), scale(0)
    for tile_no in range(tiles0):
        gradient(e0, x0, tile_of(x0.shape[1], tiles0, tile_no), col0, v0, scale0, dw0, dw0_out, dw0_sem.at[tile_no])
    for copy in got_2:
        copy.wait()
    col2, scale2 = column(u2, 2), scale(2)
    for tile_no in range(2):
        gradient(e2, x2, tile_of(x2.shape[1], 2, tile_no), col2, v2, scale2, dw2, dw2_out, out_sem.at[2 + tile_no])
    for copy in pushes:
        copy.wait()


def run_grads(x1, e1, x2, e2, x_real, x_fake, e0, dx, u0, u1, u2, v0, v1, v2, sig, cor):
    both, n1 = x1.shape
    n_rows, n0 = x_real.shape
    n2 = x2.shape[1]
    rows2 = e1.shape[0]
    rows1 = e0.shape[0]
    tiles1, tiles0 = 10, 5
    shape = jax.ShapeDtypeStruct
    hbm = pl.BlockSpec(memory_space=pl.ANY)
    vmem = pl.BlockSpec(memory_space=pltpu.VMEM)
    dma = pltpu.SemaphoreType.DMA
    flops = 2 * both * (rows2 * (n1 + n2) + rows1 * n0)
    inputs = (x1, e1, x2, e2, x_real, x_fake, e0, dx, u0, u1, u2, v0, v1, v2, sig, cor)
    return pl.pallas_call(
        grad_kernel,
        out_shape=(
            shape((rows1, n0), F32), shape((rows2, n1), F32), shape((rows2, n2), F32), shape((n_rows, n0), F32), shape((n_rows, n0), F32),
            shape((rows1,), F32), shape((rows2,), F32), shape((rows2,), F32), shape((n0,), F32), shape((n1,), F32), shape((n2,), F32),
            shape((3,), F32), shape((1, 1), F32),
        ),
        in_specs=[hbm] * len(inputs),
        out_specs=[hbm] * 5 + [vmem] * 8,
        scratch_shapes=[
            pltpu.VMEM((both, n1), BF16), pltpu.VMEM((rows2, both), BF16), pltpu.VMEM((both, n2), BF16), pltpu.VMEM((rows2, both), BF16),
            pltpu.VMEM((both, n0), BF16), pltpu.VMEM((rows1, both), BF16), pltpu.VMEM(dx.shape, F32),
            pltpu.VMEM((rows1, n0), F32), pltpu.VMEM((rows2, n1), F32), pltpu.VMEM((rows2, n2), F32),
            *[pltpu.VMEM(array.shape, F32) for array in (u0, u1, u2, v0, v1, v2, sig, cor)],
            dma((15,)), dma((tiles1,)), dma((4,)), dma((tiles1,)), dma((tiles0,)),
        ],
        compiler_params=pltpu.CompilerParams(vmem_limit_bytes=67043328),
        cost_estimate=pl.CostEstimate(flops=flops, bytes_accessed=45 * 1024 * 1024, transcendentals=0),
        name="grads",
    )(*inputs)


def finish_kernel(flip, real_in, fake_in, both_in, came_in, sig_in, real_out, fake_out, both, came, sig, dx, in_sem, out_sem):
    me = lax.axis_index("model")
    batch = me % 2
    if flip:
        batch = 1 - batch
    pieces = out_sem.shape[0]
    late = both.shape[0]
    size = late // pieces
    first = real_out.shape[0] - late
    scale_copy = pltpu.make_async_copy(sig_in, sig, in_sem.at[2 * pieces])
    scale_copy.start()

    def pulls(piece):
        rows = pl.ds(piece * size, size)
        return (
            pltpu.make_async_copy(both_in.at[pl.ds(pl.multiple_of(batch * late + piece * size, size), size), :], both.at[rows, :], in_sem.at[2 * piece]),
            pltpu.make_async_copy(came_in.at[rows, :], came.at[rows, :], in_sem.at[2 * piece + 1]),
        )

    def push(dst, piece):
        return pltpu.make_async_copy(dx.at[pl.ds(piece * size, size), :], dst.at[pl.ds(first + piece * size, size), :], out_sem.at[piece])

    for piece in range(pieces):
        for copy in pulls(piece):
            copy.start()
    scale_copy.wait()
    inv0 = 1.0 / sig[0:1, 0:1]
    for piece in range(pieces):
        for copy in pulls(piece):
            copy.wait()
        rows = pl.ds(piece * size, size)
        dx[rows, :] = (both[rows, :].astype(F32) + came[rows, :].astype(F32)) * inv0

        @pl.when(batch == 0)
        def _():
            push(real_out, piece).start()

        @pl.when(batch == 1)
        def _():
            push(fake_out, piece).start()

    for piece in range(pieces):
        push(real_out, piece).wait()


def run_finish(flip, dx_real, dx_fake, both, came, sig):
    late, n0 = came.shape
    pieces = 4
    hbm = pl.BlockSpec(memory_space=pl.ANY)
    dma = pltpu.SemaphoreType.DMA
    shape = jax.ShapeDtypeStruct(dx_real.shape, F32)
    return pl.pallas_call(
        functools.partial(finish_kernel, flip),
        out_shape=(shape, shape),
        in_specs=[hbm] * 5,
        out_specs=[hbm] * 2,
        scratch_shapes=[
            pltpu.VMEM((late, n0), BF16), pltpu.VMEM((late, n0), BF16), pltpu.VMEM((8, 128), F32), pltpu.VMEM((late, n0), F32),
            dma((2 * pieces + 1,)), dma((pieces,)),
        ],
        input_output_aliases={0: 0, 1: 1},
        compiler_params=pltpu.CompilerParams(vmem_limit_bytes=67043328),
        cost_estimate=pl.CostEstimate(flops=4 * late * n0, bytes_accessed=8 * late * n0, transcendentals=0),
        name="finish",
    )(dx_real, dx_fake, both, came, sig)


def swap(values, bits):
    return lax.ppermute(values, "model", [(dev, dev ^ bits) for dev in range(4)])


def solution(mesh):
    rows_spec = P("rep", None)
    weight_spec = P(("rep", "model"), None)
    left_spec = P(("rep", "model"))
    target_spec = P("rep", "model")
    group_spec = P("rep")

    def local_step(x_real, x_fake, weight0, weight1, weight2, u_left0, u_left1, u_left2, t_real, t_fake):
        x1, x2, e2, e1, e0, dx, sums, both, v0, v1, v2, u0, u1, u2, sig, cor = run_chain(x_real, x_fake, weight0, weight1, weight2, u_left0, u_left1, u_left2, t_real, t_fake)
        came = swap(sums, 2)
        dw0, dw1, dw2, dx_real, dx_fake, u0, u1, u2, v0, v1, v2, sigmas, loss = run_grads(x1, e1, x2, e2, x_real, x_fake, e0, dx, u0, u1, u2, v0, v1, v2, sig, cor)
        came, sigmas = lax.optimization_barrier((came, sigmas))
        came_mate = swap(came, 1)
        dx_real, dx_fake = run_finish(False, dx_real, dx_fake, both, came, sig)
        dx_real, dx_fake = run_finish(True, dx_real, dx_fake, both, came_mate, sig)
        return (loss[0], dx_real, dx_fake, dw0, dw1, dw2, u0, u1, u2, v0, v1, v2, sigmas)

    return jax.shard_map(local_step, mesh=mesh, in_specs=(rows_spec, rows_spec, weight_spec, weight_spec, weight_spec, left_spec, left_spec, left_spec, target_spec, target_spec), out_specs=(group_spec, rows_spec, rows_spec, weight_spec, weight_spec, weight_spec, left_spec, left_spec, left_spec, group_spec, group_spec, group_spec, group_spec), check_vma=False)
```

```python
import functools

import jax
import jax.numpy as jnp
from jax import lax
from jax.experimental import pallas as pl
from jax.experimental.pallas import tpu as pltpu
from jax.sharding import PartitionSpec as P

SLOPE = 0.2
EPSILON = 1e-12
MESH = pl.DeviceIdType.MESH
CHUNKS = 4
EARLY = 2
PIECES = 5
TILE = 256
BF16 = jnp.bfloat16
F32 = jnp.float32


def leaky_relu(values):
    return jnp.where(values > 0, values, SLOPE * values)


def leaky_slope(values):
    return jnp.where(values > 0, 1.0, SLOPE)


def dot_t(left, right):
    return lax.dot_general(left, right, (((1,), (1,)), ((), ())), preferred_element_type=F32)


def dot_n(left, right):
    return lax.dot_general(left, right, (((1,), (0,)), ((), ())), preferred_element_type=F32)


def t_dot(left, right):
    return lax.dot_general(left, right, (((0,), (0,)), ((), ())), preferred_element_type=F32)


def fold(values):
    rows, cols = values.shape
    return jnp.sum(values.reshape(rows // 8, 8, cols), axis=0)


def total(values):
    return jnp.sum(jnp.sum(values, axis=1, keepdims=True), axis=0, keepdims=True)


def chain_kernel(x_real, x_fake, w0_in, w1_in, w2_in, u0_in, u1_in, u2_in, t_real, t_fake,
                 x1_out, x2_out, e2_out, e1_out, e0_out, dx_out, sum_out, both_out, v0_out, v1_out, v2_out, u0_out, u1_out, u2_out, sig_out, cor_out,
                 w0, w1, w1x, w2, x0, x1, x2, y0, y1, tt, e2_t, h2_own, h2_put, h2_got, e1, e1_t, e0, e0_t, h0_put, h0_got, dx,
                 p_buf, p_sum, n_buf, c_buf,
                 eye, load_sem, put_sem, w_send, w_recv, w1x_send, w1x_recv, fwd_send, fwd_recv, small_send, small_recv,
                 x1_send, x1_recv, x2_send, x2_recv, h2_send, h2_recv, e1_send, e1_recv, h0_send, h0_recv, out_send, out_recv, dx_sem, dx_send, dx_recv, sum_sem, both_sem, both_send, both_recv):
    me = lax.axis_index("model")
    chip = me // 2
    core = me % 2
    other = 1 - chip
    mate = me + 1 - 2 * core
    far = me + 2 - 4 * chip
    diag = mate + 2 - 4 * chip
    n_rows, n0 = x0.shape
    wide1 = w0.shape[0]
    rows1 = wide1 // 2
    wide2 = w2.shape[0]
    rows2 = wide2 // 2
    n1 = 2 * wide1
    step = n_rows // CHUNKS
    piece = rows2 // PIECES

    def send(src, dst, send_sem, recv_sem, device):
        return pltpu.make_async_remote_copy(src_ref=src, dst_ref=dst, send_sem=send_sem, recv_sem=recv_sem, device_id={"model": device}, device_id_type=MESH)

    def part(index, size):
        return pl.ds(pl.multiple_of(index * size, size), size)

    barrier = pltpu.get_barrier_semaphore()
    for device in (mate, far, diag):
        pl.semaphore_signal(barrier, inc=1, device_id={"model": device}, device_id_type=MESH)
    pl.semaphore_wait(barrier, 3)

    def w1x_copy(piece_no):
        return send(
            w1_in.at[pl.ds(piece_no * piece, piece), part(other, wide1)],
            w1x.at[pl.ds(pl.multiple_of(core * rows2 + piece_no * piece, piece), piece), :],
            w1x_send.at[piece_no], w1x_recv.at[piece_no], far)

    def w1x_forward(piece_no):
        rows = w1x.at[pl.ds(pl.multiple_of(core * rows2 + piece_no * piece, piece), piece), :]
        return send(rows, rows, fwd_send.at[piece_no], fwd_recv.at[piece_no], mate)

    own1, own2 = part(core, rows1), part(core, rows2)
    loads = [
        pltpu.make_async_copy(w0_in, w0.at[own1, :], load_sem.at[0]),
        pltpu.make_async_copy(w1_in, w1.at[own2, :], load_sem.at[1]),
        pltpu.make_async_copy(w2_in, w2.at[own2, :], load_sem.at[2]),
    ]
    gives = [
        send(w0.at[own1, :], w0.at[own1, :], w_send.at[0], w_recv.at[0], mate),
        send(w1.at[own2, :], w1.at[own2, :], w_send.at[1], w_recv.at[1], mate),
        send(w2.at[own2, :], w2.at[own2, :], w_send.at[2], w_recv.at[2], mate),
    ]
    w1x_copy(0).start()
    for copy in loads:
        copy.start()

    w1x_copy(1).start()

    def mine(x_in, t_own):
        return (
            pltpu.make_async_copy(x_in, x0, load_sem.at[3]),
            pltpu.make_async_copy(t_own, tt.at[own2, :], load_sem.at[4]),
        )

    @pl.when(core == 0)
    def _():
        for copy in mine(x_real, t_real):
            copy.start()

    @pl.when(core == 1)
    def _():
        for copy in mine(x_fake, t_fake):
            copy.start()

    def row(values):
        return jnp.broadcast_to(values.reshape(1, values.size).astype(BF16), (16, values.size))

    lanes = lax.broadcasted_iota(jnp.int32, eye.shape, 1)
    eye[...] = jnp.where(lanes == lax.broadcasted_iota(jnp.int32, eye.shape, 0), 1.0, 0.0).astype(BF16)

    def store_transposed(dst, first, rows, values):
        for begin in range(0, values.shape[1], eye.shape[0]):
            size = min(eye.shape[0], values.shape[1] - begin)
            block = dot_t(eye[0:size, 0:size], values[:, begin:begin + size])
            dst[pl.ds(pl.multiple_of(first + begin, 128), size), rows] = block.astype(BF16)

    u_rows = [row(u0_in[...]), row(u1_in[...]), row(u2_in[...])]
    loads[0].wait()
    p_buf[me, :, pl.ds(0, n0)] = dot_n(u_rows[0], w0[own1, :])[0:1]
    loads[1].wait()

    def p1_tile(tile_no, carry):
        cols = part(tile_no, wide1 // 2)
        p_buf[me, :, pl.ds(pl.multiple_of(n0 + tile_no * (wide1 // 2), 128), wide1 // 2)] = dot_n(u_rows[1], w1[own2, cols])[0:1]
        return carry

    lax.fori_loop(0, 4, p1_tile, 0)
    loads[2].wait()
    p_buf[me, :, pl.ds(n0 + n1, wide2 * 2)] = dot_n(u_rows[2], w2[own2, :])[0:1]

    def spread(buf, first):
        return [send(buf.at[me], buf.at[me], small_send.at[first + which], small_recv.at[first + which], device) for which, device in enumerate((mate, far, diag))]

    p_near = send(p_buf.at[me], p_buf.at[me], small_send.at[0], small_recv.at[0], mate)
    p_near.start()
    gives[0].start()
    p_near.wait()
    p_sum[chip] = p_buf[2 * chip] + p_buf[2 * chip + 1]
    p_far = send(p_sum.at[chip], p_sum.at[chip], small_send.at[1], small_recv.at[1], far)
    p_far.start()
    w1x_copy(2).start()

    pltpu.make_async_copy(x_real, x0, load_sem.at[3]).wait()
    gives[0].wait_recv()

    def y0_tile(tile_no, carry):
        cols = part(tile_no, TILE)
        y0[:, cols] = dot_t(x0[...], w0[cols, :])
        return carry

    lax.fori_loop(0, wide1 // TILE, y0_tile, 0)
    p_far.wait()
    p_all = p_sum[0] + p_sum[1]
    spans = ((0, n0, v0_out), (n0, n1, v1_out), (n0 + n1, 2 * wide2, v2_out))
    for first, size, v_out in spans:
        p_vec = p_all[:, first:first + size]
        v_out[...] = p_vec / jnp.maximum(jnp.sqrt(total(p_vec * p_vec)), EPSILON)
    u0_out[...] = dot_t(row(v0_out[...]), w0[own1, :])[0:1]
    u1_out[...] = dot_t(row(v1_out[...]), w1[own2, :])[0:1]
    u2_out[...] = dot_t(row(v2_out[...]), w2[own2, :])[0:1]
    lane = lax.broadcasted_iota(jnp.int32, (8, 128), 1)

    def pack(values):
        packed = jnp.zeros((8, 128), F32)
        for place, value in enumerate(values):
            packed = jnp.where(lane == place, value, packed)
        return packed

    n_buf[me] = pack([total(u_out[...] * u_out[...]) for u_out in (u0_out, u1_out, u2_out)])
    n_copies = spread(n_buf, 3)
    for copy in n_copies:
        copy.start()
    for piece_no in range(3, PIECES):
        w1x_copy(piece_no).start()
    for copy in gives[1:]:
        copy.start()

    @pl.when(core == 0)
    def _():
        send(t_fake, tt.at[own2, :], w_send.at[3], w_recv.at[3], mate).start()

    @pl.when(core == 1)
    def _():
        send(t_real, tt.at[own2, :], w_send.at[3], w_recv.at[3], mate).start()

    for copy in n_copies:
        copy.wait()
    sigmas = jnp.sqrt(n_buf[0] + n_buf[1] + n_buf[2] + n_buf[3])
    sig_out[...] = sigmas
    sig0, sig1, sig2 = sigmas[0:1, 0:1], sigmas[0:1, 1:2], sigmas[0:1, 2:3]
    inv0, inv1, inv2 = 1.0 / sig0, 1.0 / sig1, 1.0 / sig2
    u0_out[...] = u0_out[...] / sig0
    u1_out[...] = u1_out[...] / sig1
    u2_out[...] = u2_out[...] / sig2

    def chunk_copy(buf, slot, chunk_no, send_sem, recv_sem):
        rows = buf.at[slot, part(chunk_no, step), :]
        return send(rows, rows, send_sem.at[chunk_no], recv_sem.at[chunk_no], far)

    def layer0(chunk_no, carry):
        rows = part(chunk_no, step)
        x1[chip, rows, :] = leaky_relu(y0[rows, :] * inv0).astype(BF16)
        chunk_copy(x1, chip, chunk_no, x1_send, x1_recv).start()
        return carry

    lax.fori_loop(0, CHUNKS, layer0, 0)

    batch = part(core, n_rows)

    def outputs(src, dst, which):
        return (
            pltpu.make_async_copy(src, dst, put_sem.at[which]),
            send(src, dst, out_send.at[which], out_recv.at[which], mate),
        )

    def halves(src, dst, size, which):
        return (
            pltpu.make_async_copy(src.at[part(core, size), :], dst.at[:, batch], put_sem.at[which]),
            send(src.at[part(1 - core, size), :], dst.at[:, batch], out_send.at[which], out_recv.at[which], mate),
        )

    x1_near = outputs(x1.at[chip], x1_out.at[batch, part(chip, wide1)], 0)
    for copy in x1_near:
        copy.start()
    for piece_no in range(PIECES):
        w1x_copy(piece_no).wait_recv()
        w1x_forward(piece_no).start()

    gives[1].wait_recv()

    def layer1(chunk_no, carry):
        rows = part(chunk_no, step)
        chunk_copy(x1, other, chunk_no, x1_send, x1_recv).wait_recv()
        y_val = (dot_t(x1[0, rows, :], w1[:, pl.ds(0, wide1)]) + dot_t(x1[1, rows, :], w1[:, pl.ds(wide1, wide1)])) * inv1
        y1[rows, :] = y_val
        x2[chip, rows, :] = leaky_relu(y_val).astype(BF16)
        chunk_copy(x2, chip, chunk_no, x2_send, x2_recv).start()
        return carry

    lax.fori_loop(0, CHUNKS, layer1, 0)
    x1_far = outputs(x1.at[other], x1_out.at[batch, part(other, wide1)], 1)
    for copy in x1_far:
        copy.start()

    gives[2].wait_recv()
    pltpu.make_async_copy(t_real, tt.at[own2, :], load_sem.at[4]).wait()
    t_give = send(t_real, tt.at[own2, :], w_send.at[3], w_recv.at[3], mate)
    t_give.wait_recv()

    def layer2(chunk_no, carry):
        corr2, loss = carry
        rows = part(chunk_no, step)
        chunk_copy(x2, other, chunk_no, x2_send, x2_recv).wait_recv()
        y_val = (dot_t(x2[0, rows, :], w2[:, pl.ds(0, wide2)]) + dot_t(x2[1, rows, :], w2[:, pl.ds(wide2, wide2)])) * inv2
        e_val = y_val - dot_t(eye[0:step, 0:step], tt[:, rows])
        corr2 = corr2 + fold(e_val * y_val)
        loss = loss + fold(e_val * e_val)
        e_half = e_val.astype(BF16)
        h2_put[rows, :] = dot_n(e_half, w2[:, part(other, wide2)]).astype(BF16)
        send(h2_put.at[rows, :], h2_got.at[rows, :], h2_send.at[chunk_no], h2_recv.at[chunk_no], far).start()
        h2_own[rows, :] = dot_n(e_half, w2[:, part(chip, wide2)])
        store_transposed(e2_t, 0, rows, e_half)
        return corr2, loss

    zero = jnp.zeros((8, wide2), F32)
    corr2, loss = lax.fori_loop(0, CHUNKS, layer2, (zero, zero))

    def back1(chunk_no, corr1):
        rows = part(chunk_no, step)
        send(h2_put.at[rows, :], h2_got.at[rows, :], h2_send.at[chunk_no], h2_recv.at[chunk_no], far).wait_recv()
        y_val = y1[rows, :]
        e_val = (h2_own[rows, :] + h2_got[rows, :].astype(F32)) * (inv2 * leaky_slope(y_val))
        e_half = e_val.astype(BF16)
        e1[chip, rows, :] = e_half
        chunk_copy(e1, chip, chunk_no, e1_send, e1_recv).start()
        store_transposed(e1_t, 0, rows, e_half)
        return corr1 + fold(e_val * y_val)

    corr1 = lax.fori_loop(0, CHUNKS, back1, zero)
    lesser = [
        outputs(x2.at[0], x2_out.at[batch, pl.ds(0, wide2)], 2),
        outputs(x2.at[1], x2_out.at[batch, pl.ds(wide2, wide2)], 3),
        halves(e2_t, e2_out, rows2, 4),
        halves(e1_t, e1_out, rows2, 5),
    ]
    for pair in lesser:
        for copy in pair:
            copy.start()
    for piece_no in range(PIECES):
        w1x_forward(piece_no).wait_recv()

    late = n_rows - EARLY * step

    def h0_copy(chunk_no):
        rows = part(chunk_no, step)
        return send(h0_put.at[rows, :], h0_got.at[rows, :], h0_send.at[chunk_no], h0_recv.at[chunk_no], far)

    def late_copies(chunk_no):
        src = h0_put.at[part(chunk_no, step), :]
        place = chunk_no - EARLY
        dst = both_out.at[pl.ds(pl.multiple_of(core * late + place * step, step), step), :]
        return (
            pltpu.make_async_copy(src, sum_out.at[part(place, step), :], sum_sem.at[place]),
            pltpu.make_async_copy(src, dst, both_sem.at[place]),
            send(src, dst, both_send.at[place], both_recv.at[place], mate),
        )

    def back0(chunk_no, corr0):
        rows = part(chunk_no, step)
        chunk_copy(e1, other, chunk_no, e1_send, e1_recv).wait_recv()

        def h1_tile(tile_no, corr):
            cols = part(tile_no, wide2)
            own_cols = pl.ds(pl.multiple_of(chip * wide1 + tile_no * wide2, 128), wide2)
            h_val = dot_n(e1[chip, rows, :], w1[:, own_cols]) + dot_n(e1[other, rows, :], w1x[:, cols])
            y_val = y0[rows, cols]
            e_val = h_val * (inv1 * leaky_slope(y_val))
            e0[:, cols] = e_val.astype(BF16)
            return corr + fold(e_val * y_val)

        corr0 = lax.fori_loop(0, wide1 // wide2, h1_tile, corr0)
        h0_put[rows, :] = dot_n(e0[...], w0[...]).astype(BF16)
        return corr0

    def transpose0(chunk_no):
        rows = part(chunk_no, step)

        def tile(tile_no, carry):
            store_transposed(e0_t, tile_no * wide2, rows, e0[:, part(tile_no, wide2)])
            return carry

        lax.fori_loop(0, wide1 // wide2, tile, 0)

    def back0_early(chunk_no, corr0):
        corr0 = back0(chunk_no, corr0)
        h0_copy(chunk_no).start()
        transpose0(chunk_no)
        return corr0

    def back0_late(chunk_no, corr0):
        corr0 = back0(chunk_no, corr0)
        for copy in late_copies(chunk_no):
            copy.start()
        transpose0(chunk_no)
        return corr0

    corr0 = lax.fori_loop(0, EARLY, back0_early, zero)
    corr0 = lax.fori_loop(EARLY, CHUNKS, back0_late, corr0)
    e0_pair = halves(e0_t, e0_out, rows1, 6)
    for copy in e0_pair:
        copy.start()
    c_buf[me] = pack([total(corr0) * inv0, total(corr1), total(corr2), total(loss)])
    c_copies = spread(c_buf, 6)
    for copy in c_copies:
        copy.start()

    def dx_copies(chunk_no):
        rows = part(chunk_no, step)
        dst = dx_out.at[pl.ds(pl.multiple_of((core * EARLY + chunk_no) * step, step), step), :]
        return (
            pltpu.make_async_copy(dx.at[rows, :], dst, dx_sem.at[chunk_no]),
            send(dx.at[rows, :], dst, dx_send.at[chunk_no], dx_recv.at[chunk_no], mate),
        )

    def finish(chunk_no, carry):
        rows = part(chunk_no, step)
        h0_copy(chunk_no).wait_recv()
        dx[rows, :] = (h0_put[rows, :].astype(F32) + h0_got[rows, :].astype(F32)) * inv0
        for copy in dx_copies(chunk_no):
            copy.start()
        return carry

    lax.fori_loop(0, EARLY, finish, 0)
    for copy in c_copies:
        copy.wait()
    cor_out[...] = c_buf[0] + c_buf[1] + c_buf[2] + c_buf[3]

    for copy in gives:
        copy.wait_send()
    t_give.wait_send()
    for piece_no in range(PIECES):
        w1x_copy(piece_no).wait_send()
        w1x_forward(piece_no).wait_send()
    for pair in (x1_near, x1_far, *lesser, e0_pair):
        for copy in pair:
            copy.wait()

    def drain(chunk_no, carry):
        rows = part(chunk_no, step)
        chunk_copy(x1, chip, chunk_no, x1_send, x1_recv).wait_send()
        chunk_copy(x2, chip, chunk_no, x2_send, x2_recv).wait_send()
        send(h2_put.at[rows, :], h2_got.at[rows, :], h2_send.at[chunk_no], h2_recv.at[chunk_no], far).wait_send()
        chunk_copy(e1, chip, chunk_no, e1_send, e1_recv).wait_send()
        return carry

    lax.fori_loop(0, CHUNKS, drain, 0)

    def drain_early(chunk_no, carry):
        h0_copy(chunk_no).wait_send()
        for copy in dx_copies(chunk_no):
            copy.wait()
        return carry

    lax.fori_loop(0, EARLY, drain_early, 0)

    def drain_late(chunk_no, carry):
        for copy in late_copies(chunk_no):
            copy.wait()
        return carry

    lax.fori_loop(EARLY, CHUNKS, drain_late, 0)


def run_chain(x_real, x_fake, weight0, weight1, weight2, u_left0, u_left1, u_left2, t_real, t_fake):
    n_rows, n0 = x_real.shape
    rows1 = weight0.shape[0]
    rows2, n1 = weight1.shape
    wide1, wide2 = 2 * rows1, 2 * rows2
    n2 = 2 * wide2
    early = n_rows // CHUNKS * EARLY
    late = n_rows - early
    hbm = pl.BlockSpec(memory_space=pl.ANY)
    vmem = pl.BlockSpec(memory_space=pltpu.VMEM)
    shape = jax.ShapeDtypeStruct
    dma = pltpu.SemaphoreType.DMA
    return pl.pallas_call(
        chain_kernel,
        out_shape=(
            shape((2 * n_rows, n1), BF16), shape((2 * n_rows, n2), BF16), shape((rows2, 2 * n_rows), BF16), shape((rows2, 2 * n_rows), BF16),
            shape((rows1, 2 * n_rows), BF16), shape((2 * early, n0), F32), shape((late, n0), BF16), shape((2 * late, n0), BF16),
            shape((1, n0), F32), shape((1, n1), F32), shape((1, n2), F32),
            shape((1, rows1), F32), shape((1, rows2), F32), shape((1, rows2), F32),
            shape((8, 128), F32), shape((8, 128), F32),
        ),
        in_specs=[hbm] * 5 + [vmem] * 3 + [hbm] * 2,
        out_specs=[hbm] * 8 + [vmem] * 8,
        scratch_shapes=[
            pltpu.VMEM((wide1, n0), BF16), pltpu.VMEM((wide2, n1), BF16), pltpu.VMEM((wide2, wide1), BF16), pltpu.VMEM((wide2, n2), BF16),
            pltpu.VMEM((n_rows, n0), BF16), pltpu.VMEM((2, n_rows, wide1), BF16), pltpu.VMEM((2, n_rows, wide2), BF16),
            pltpu.VMEM((n_rows, wide1), F32), pltpu.VMEM((n_rows, wide2), F32), pltpu.VMEM((wide2, n_rows), BF16),
            pltpu.VMEM((wide2, n_rows), BF16), pltpu.VMEM((n_rows, wide2), F32), pltpu.VMEM((n_rows, wide2), BF16), pltpu.VMEM((n_rows, wide2), BF16),
            pltpu.VMEM((2, n_rows, wide2), BF16), pltpu.VMEM((wide2, n_rows), BF16), pltpu.VMEM((n_rows // CHUNKS, wide1), BF16), pltpu.VMEM((wide1, n_rows), BF16),
            pltpu.VMEM((n_rows, n0), BF16), pltpu.VMEM((early, n0), BF16), pltpu.VMEM((early, n0), F32),
            pltpu.VMEM((4, 1, n0 + n1 + n2), F32), pltpu.VMEM((2, 1, n0 + n1 + n2), F32), pltpu.VMEM((4, 8, 128), F32), pltpu.VMEM((4, 8, 128), F32), pltpu.VMEM((256, 256), BF16),
            dma((5,)), dma((7,)), dma((4,)), dma((4,)), dma((PIECES,)), dma((PIECES,)), dma((PIECES,)), dma((PIECES,)), dma((9,)), dma((9,)),
            dma((CHUNKS,)), dma((CHUNKS,)), dma((CHUNKS,)), dma((CHUNKS,)), dma((CHUNKS,)), dma((CHUNKS,)),
            dma((CHUNKS,)), dma((CHUNKS,)), dma((EARLY,)), dma((EARLY,)), dma((7,)), dma((7,)), dma((EARLY,)), dma((EARLY,)), dma((EARLY,)),
            dma((CHUNKS - EARLY,)), dma((CHUNKS - EARLY,)), dma((CHUNKS - EARLY,)), dma((CHUNKS - EARLY,)),
        ],
        compiler_params=pltpu.CompilerParams(collective_id=0, has_side_effects=True, vmem_limit_bytes=67043328),
        name="chain",
    )(x_real, x_fake, weight0, weight1, weight2, u_left0, u_left1, u_left2, t_real.T, t_fake.T)


def grad_kernel(x1_in, e1_in, x2_in, e2_in, x_real, x_fake, e0_in, dx_in, u0_in, u1_in, u2_in, v0_in, v1_in, v2_in, sig_in, cor_in,
                dw0_out, dw1_out, dw2_out, dx_real, dx_fake, u0_out, u1_out, u2_out, v0_out, v1_out, v2_out, sig_out, loss_out,
                x1, e1, x2, e2, x0, e0, dx, dw0, dw1, dw2, u0, u1, u2, v0, v1, v2, sig, cor, in_sem, x1_sem, out_sem, dw1_sem, dw0_sem):
    n_rows = x_real.shape[0]
    early = dx.shape[0] // 2
    tiles1 = x1_sem.shape[0]
    tiles0 = dw0_sem.shape[0]

    def pull(src, dst, which):
        copy = pltpu.make_async_copy(src, dst, in_sem.at[which])
        copy.start()
        return copy

    small = [pull(src, dst, place) for place, (src, dst) in enumerate((
        (u0_in, u0), (u1_in, u1), (u2_in, u2), (v0_in, v0), (v1_in, v1), (v2_in, v2), (sig_in, sig), (cor_in, cor)))]
    def tile_of(size, tiles, tile_no):
        return pl.ds(tile_no * (size // tiles), size // tiles)

    def load(src, dst, which):
        return pltpu.make_async_copy(src, dst, in_sem.at[which])

    got_e1 = pull(e1_in, e1, 11)
    got_x1 = []
    for tile_no in range(tiles1):
        cols = tile_of(x1.shape[1], tiles1, tile_no)
        got_x1.append(pltpu.make_async_copy(x1_in.at[:, cols], x1.at[:, cols], x1_sem.at[tile_no]))
    got_e0 = load(e0_in, e0, 8)
    got_x0 = [load(x_real, x0.at[pl.ds(0, n_rows), :], 9), load(x_fake, x0.at[pl.ds(n_rows, n_rows), :], 10)]
    got_dx = load(dx_in, dx, 12)
    got_2 = [load(e2_in, e2, 13), load(x2_in, x2, 14)]
    queue = [*got_x1, *got_x0, got_e0, got_dx, *got_2]

    def read_on(count=1):
        for _ in range(min(count, len(queue))):
            queue.pop(0).start()

    read_on(3)

    for copy in small:
        copy.wait()
    for src, dst in ((u0, u0_out), (u1, u1_out), (u2, u2_out), (v0, v0_out), (v1, v1_out), (v2, v2_out)):
        dst[...] = src[...].reshape(dst.shape)
    sig_out[...] = sig[0:1, 0:3].reshape(3)
    loss_out[...] = cor[0:1, 3:4] * (0.5 / n_rows)

    def column(u_new, layer_no):
        return jnp.broadcast_to(u_new[...] * cor[0:1, layer_no:layer_no + 1], (128, u_new.shape[1])).T[:, 0:1]

    def scale(layer_no):
        return 1.0 / (n_rows * sig[0:1, layer_no:layer_no + 1])

    pushes = []

    def gradient(errors, layer_in, cols, col, v_new, rate, dst, out, sem):
        dst[:, cols] = (dot_n(errors[...], layer_in[:, cols]) - col * v_new[:, cols]) * rate
        copy = pltpu.make_async_copy(dst.at[:, cols], out.at[:, cols], sem)
        copy.start()
        pushes.append(copy)

    got_e1.wait()
    col1, scale1 = column(u1, 1), scale(1)
    for tile_no in range(tiles1):
        got_x1[tile_no].wait()
        read_on()
        gradient(e1, x1, tile_of(x1.shape[1], tiles1, tile_no), col1, v1, scale1, dw1, dw1_out, dw1_sem.at[tile_no])
    got_e0.wait()
    read_on(3)
    for copy in got_x0:
        copy.wait()
    col0, scale0 = column(u0, 0), scale(0)
    for tile_no in range(tiles0):
        gradient(e0, x0, tile_of(x0.shape[1], tiles0, tile_no), col0, v0, scale0, dw0, dw0_out, dw0_sem.at[tile_no])
    got_dx.wait()
    for place, dst in enumerate((dx_real, dx_fake)):
        copy = pltpu.make_async_copy(dx.at[pl.ds(place * early, early), :], dst.at[pl.ds(0, early), :], out_sem.at[place])
        copy.start()
        pushes.append(copy)
    for copy in got_2:
        copy.wait()
    col2, scale2 = column(u2, 2), scale(2)
    for tile_no in range(2):
        gradient(e2, x2, tile_of(x2.shape[1], 2, tile_no), col2, v2, scale2, dw2, dw2_out, out_sem.at[2 + tile_no])
    for copy in pushes:
        copy.wait()


def run_grads(x1, e1, x2, e2, x_real, x_fake, e0, dx, u0, u1, u2, v0, v1, v2, sig, cor):
    both, n1 = x1.shape
    n_rows, n0 = x_real.shape
    n2 = x2.shape[1]
    rows2 = e1.shape[0]
    rows1 = e0.shape[0]
    tiles1, tiles0 = 10, 5
    shape = jax.ShapeDtypeStruct
    hbm = pl.BlockSpec(memory_space=pl.ANY)
    vmem = pl.BlockSpec(memory_space=pltpu.VMEM)
    dma = pltpu.SemaphoreType.DMA
    flops = 2 * both * (rows2 * (n1 + n2) + rows1 * n0)
    inputs = (x1, e1, x2, e2, x_real, x_fake, e0, dx, u0, u1, u2, v0, v1, v2, sig, cor)
    return pl.pallas_call(
        grad_kernel,
        out_shape=(
            shape((rows1, n0), F32), shape((rows2, n1), F32), shape((rows2, n2), F32), shape((n_rows, n0), F32), shape((n_rows, n0), F32),
            shape((rows1,), F32), shape((rows2,), F32), shape((rows2,), F32), shape((n0,), F32), shape((n1,), F32), shape((n2,), F32),
            shape((3,), F32), shape((1, 1), F32),
        ),
        in_specs=[hbm] * len(inputs),
        out_specs=[hbm] * 5 + [vmem] * 8,
        scratch_shapes=[
            pltpu.VMEM((both, n1), BF16), pltpu.VMEM((rows2, both), BF16), pltpu.VMEM((both, n2), BF16), pltpu.VMEM((rows2, both), BF16),
            pltpu.VMEM((both, n0), BF16), pltpu.VMEM((rows1, both), BF16), pltpu.VMEM(dx.shape, F32),
            pltpu.VMEM((rows1, n0), F32), pltpu.VMEM((rows2, n1), F32), pltpu.VMEM((rows2, n2), F32),
            *[pltpu.VMEM(array.shape, F32) for array in (u0, u1, u2, v0, v1, v2, sig, cor)],
            dma((15,)), dma((tiles1,)), dma((4,)), dma((tiles1,)), dma((tiles0,)),
        ],
        compiler_params=pltpu.CompilerParams(vmem_limit_bytes=67043328),
        cost_estimate=pl.CostEstimate(flops=flops, bytes_accessed=45 * 1024 * 1024, transcendentals=0),
        name="grads",
    )(*inputs)


def finish_kernel(flip, real_in, fake_in, both_in, came_in, sig_in, real_out, fake_out, both, came, sig, dx, in_sem, out_sem):
    me = lax.axis_index("model")
    batch = me % 2
    if flip:
        batch = 1 - batch
    pieces = out_sem.shape[0]
    late = both.shape[0]
    size = late // pieces
    first = real_out.shape[0] - late
    scale_copy = pltpu.make_async_copy(sig_in, sig, in_sem.at[2 * pieces])
    scale_copy.start()

    def pulls(piece):
        rows = pl.ds(piece * size, size)
        return (
            pltpu.make_async_copy(both_in.at[pl.ds(pl.multiple_of(batch * late + piece * size, size), size), :], both.at[rows, :], in_sem.at[2 * piece]),
            pltpu.make_async_copy(came_in.at[rows, :], came.at[rows, :], in_sem.at[2 * piece + 1]),
        )

    def push(dst, piece):
        return pltpu.make_async_copy(dx.at[pl.ds(piece * size, size), :], dst.at[pl.ds(first + piece * size, size), :], out_sem.at[piece])

    for piece in range(pieces):
        for copy in pulls(piece):
            copy.start()
    scale_copy.wait()
    inv0 = 1.0 / sig[0:1, 0:1]
    for piece in range(pieces):
        for copy in pulls(piece):
            copy.wait()
        rows = pl.ds(piece * size, size)
        dx[rows, :] = (both[rows, :].astype(F32) + came[rows, :].astype(F32)) * inv0

        @pl.when(batch == 0)
        def _():
            push(real_out, piece).start()

        @pl.when(batch == 1)
        def _():
            push(fake_out, piece).start()

    for piece in range(pieces):
        push(real_out, piece).wait()


def run_finish(flip, dx_real, dx_fake, both, came, sig):
    late, n0 = came.shape
    pieces = 4
    hbm = pl.BlockSpec(memory_space=pl.ANY)
    dma = pltpu.SemaphoreType.DMA
    shape = jax.ShapeDtypeStruct(dx_real.shape, F32)
    return pl.pallas_call(
        functools.partial(finish_kernel, flip),
        out_shape=(shape, shape),
        in_specs=[hbm] * 5,
        out_specs=[hbm] * 2,
        scratch_shapes=[
            pltpu.VMEM((late, n0), BF16), pltpu.VMEM((late, n0), BF16), pltpu.VMEM((8, 128), F32), pltpu.VMEM((late, n0), F32),
            dma((2 * pieces + 1,)), dma((pieces,)),
        ],
        input_output_aliases={0: 0, 1: 1},
        compiler_params=pltpu.CompilerParams(vmem_limit_bytes=67043328),
        cost_estimate=pl.CostEstimate(flops=4 * late * n0, bytes_accessed=8 * late * n0, transcendentals=0),
        name="finish",
    )(dx_real, dx_fake, both, came, sig)


def swap(values, bits):
    return lax.ppermute(values, "model", [(dev, dev ^ bits) for dev in range(4)])


def solution(mesh):
    rows_spec = P("rep", None)
    weight_spec = P(("rep", "model"), None)
    left_spec = P(("rep", "model"))
    target_spec = P("rep", "model")
    group_spec = P("rep")

    def local_step(x_real, x_fake, weight0, weight1, weight2, u_left0, u_left1, u_left2, t_real, t_fake):
        x1, x2, e2, e1, e0, dx, sums, both, v0, v1, v2, u0, u1, u2, sig, cor = run_chain(x_real, x_fake, weight0, weight1, weight2, u_left0, u_left1, u_left2, t_real, t_fake)
        came = swap(sums, 2)
        dw0, dw1, dw2, dx_real, dx_fake, u0, u1, u2, v0, v1, v2, sigmas, loss = run_grads(x1, e1, x2, e2, x_real, x_fake, e0, dx, u0, u1, u2, v0, v1, v2, sig, cor)
        came, sigmas = lax.optimization_barrier((came, sigmas))
        came_mate = swap(came, 1)
        dx_real, dx_fake = run_finish(False, dx_real, dx_fake, both, came, sig)
        dx_real, dx_fake = run_finish(True, dx_real, dx_fake, both, came_mate, sig)
        return (loss[0], dx_real, dx_fake, dw0, dw1, dw2, u0, u1, u2, v0, v1, v2, sigmas)

    return jax.shard_map(local_step, mesh=mesh, in_specs=(rows_spec, rows_spec, weight_spec, weight_spec, weight_spec, left_spec, left_spec, left_spec, target_spec, target_spec), out_specs=(group_spec, rows_spec, rows_spec, weight_spec, weight_spec, weight_spec, left_spec, left_spec, left_spec, group_spec, group_spec, group_spec, group_spec), check_vma=False)
```

```python
import functools

import jax
import jax.numpy as jnp
from jax import lax
from jax.experimental import pallas as pl
from jax.experimental.pallas import tpu as pltpu
from jax.sharding import PartitionSpec as P

SLOPE = 0.2
EPSILON = 1e-12
MESH = pl.DeviceIdType.MESH
CHUNKS = 4
EARLY = 1
PIECES = 5
TILE = 256
BF16 = jnp.bfloat16
F32 = jnp.float32


def leaky_relu(values):
    return jnp.where(values > 0, values, SLOPE * values)


def leaky_slope(values):
    return jnp.where(values > 0, 1.0, SLOPE)


def dot_t(left, right):
    return lax.dot_general(left, right, (((1,), (1,)), ((), ())), preferred_element_type=F32)


def dot_n(left, right):
    return lax.dot_general(left, right, (((1,), (0,)), ((), ())), preferred_element_type=F32)


def t_dot(left, right):
    return lax.dot_general(left, right, (((0,), (0,)), ((), ())), preferred_element_type=F32)


def fold(values):
    rows, cols = values.shape
    return jnp.sum(values.reshape(rows // 8, 8, cols), axis=0)


def total(values):
    return jnp.sum(jnp.sum(values, axis=1, keepdims=True), axis=0, keepdims=True)


def chain_kernel(x_real, x_fake, w0_in, w1_in, w2_in, u0_in, u1_in, u2_in, t_real, t_fake,
                 x1_out, x2_out, e2_out, e1_out, e0_out, dx_out, sum_out, both_out, v0_out, v1_out, v2_out, u0_out, u1_out, u2_out, sig_out, cor_out,
                 w0, w1, w1x, w2, x0, x1, x2, y0, y1, tt, e2_t, h2_own, h2_put, h2_got, e1, e1_t, e0, e0_t, h0_put, h0_got, dx,
                 p_buf, p_sum, n_buf, c_buf,
                 eye, load_sem, put_sem, w_send, w_recv, w1x_send, w1x_recv, fwd_send, fwd_recv, small_send, small_recv,
                 x1_send, x1_recv, x2_send, x2_recv, h2_send, h2_recv, e1_send, e1_recv, h0_send, h0_recv, out_send, out_recv, dx_sem, dx_send, dx_recv, sum_sem, both_sem, both_send, both_recv):
    me = lax.axis_index("model")
    chip = me // 2
    core = me % 2
    other = 1 - chip
    mate = me + 1 - 2 * core
    far = me + 2 - 4 * chip
    diag = mate + 2 - 4 * chip
    n_rows, n0 = x0.shape
    wide1 = w0.shape[0]
    rows1 = wide1 // 2
    wide2 = w2.shape[0]
    rows2 = wide2 // 2
    n1 = 2 * wide1
    step = n_rows // CHUNKS
    piece = rows2 // PIECES

    def send(src, dst, send_sem, recv_sem, device):
        return pltpu.make_async_remote_copy(src_ref=src, dst_ref=dst, send_sem=send_sem, recv_sem=recv_sem, device_id={"model": device}, device_id_type=MESH)

    def part(index, size):
        return pl.ds(pl.multiple_of(index * size, size), size)

    barrier = pltpu.get_barrier_semaphore()
    for device in (mate, far, diag):
        pl.semaphore_signal(barrier, inc=1, device_id={"model": device}, device_id_type=MESH)
    pl.semaphore_wait(barrier, 3)

    def w1x_copy(piece_no):
        return send(
            w1_in.at[pl.ds(piece_no * piece, piece), part(other, wide1)],
            w1x.at[pl.ds(pl.multiple_of(core * rows2 + piece_no * piece, piece), piece), :],
            w1x_send.at[piece_no], w1x_recv.at[piece_no], far)

    def w1x_forward(piece_no):
        rows = w1x.at[pl.ds(pl.multiple_of(core * rows2 + piece_no * piece, piece), piece), :]
        return send(rows, rows, fwd_send.at[piece_no], fwd_recv.at[piece_no], mate)

    own1, own2 = part(core, rows1), part(core, rows2)
    loads = [
        pltpu.make_async_copy(w0_in, w0.at[own1, :], load_sem.at[0]),
        pltpu.make_async_copy(w1_in, w1.at[own2, :], load_sem.at[1]),
        pltpu.make_async_copy(w2_in, w2.at[own2, :], load_sem.at[2]),
    ]
    gives = [
        send(w0.at[own1, :], w0.at[own1, :], w_send.at[0], w_recv.at[0], mate),
        send(w1.at[own2, :], w1.at[own2, :], w_send.at[1], w_recv.at[1], mate),
        send(w2.at[own2, :], w2.at[own2, :], w_send.at[2], w_recv.at[2], mate),
    ]
    w1x_copy(0).start()
    for copy in loads:
        copy.start()

    w1x_copy(1).start()

    def mine(x_in, t_own):
        return (
            pltpu.make_async_copy(x_in, x0, load_sem.at[3]),
            pltpu.make_async_copy(t_own, tt.at[own2, :], load_sem.at[4]),
        )

    @pl.when(core == 0)
    def _():
        for copy in mine(x_real, t_real):
            copy.start()

    @pl.when(core == 1)
    def _():
        for copy in mine(x_fake, t_fake):
            copy.start()

    def row(values):
        return jnp.broadcast_to(values.reshape(1, values.size).astype(BF16), (16, values.size))

    lanes = lax.broadcasted_iota(jnp.int32, eye.shape, 1)
    eye[...] = jnp.where(lanes == lax.broadcasted_iota(jnp.int32, eye.shape, 0), 1.0, 0.0).astype(BF16)

    def store_transposed(dst, first, rows, values):
        for begin in range(0, values.shape[1], eye.shape[0]):
            size = min(eye.shape[0], values.shape[1] - begin)
            block = dot_t(eye[0:size, 0:size], values[:, begin:begin + size])
            dst[pl.ds(pl.multiple_of(first + begin, 128), size), rows] = block.astype(BF16)

    u_rows = [row(u0_in[...]), row(u1_in[...]), row(u2_in[...])]
    loads[0].wait()
    p_buf[me, :, pl.ds(0, n0)] = dot_n(u_rows[0], w0[own1, :])[0:1]
    loads[1].wait()

    def p1_tile(tile_no, carry):
        cols = part(tile_no, wide1 // 2)
        p_buf[me, :, pl.ds(pl.multiple_of(n0 + tile_no * (wide1 // 2), 128), wide1 // 2)] = dot_n(u_rows[1], w1[own2, cols])[0:1]
        return carry

    lax.fori_loop(0, 4, p1_tile, 0)
    loads[2].wait()
    p_buf[me, :, pl.ds(n0 + n1, wide2 * 2)] = dot_n(u_rows[2], w2[own2, :])[0:1]

    def spread(buf, first):
        return [send(buf.at[me], buf.at[me], small_send.at[first + which], small_recv.at[first + which], device) for which, device in enumerate((mate, far, diag))]

    p_near = send(p_buf.at[me], p_buf.at[me], small_send.at[0], small_recv.at[0], mate)
    p_near.start()
    gives[0].start()
    p_near.wait()
    p_sum[chip] = p_buf[2 * chip] + p_buf[2 * chip + 1]
    p_far = send(p_sum.at[chip], p_sum.at[chip], small_send.at[1], small_recv.at[1], far)
    p_far.start()
    w1x_copy(2).start()

    pltpu.make_async_copy(x_real, x0, load_sem.at[3]).wait()
    gives[0].wait_recv()

    def y0_tile(tile_no, carry):
        cols = part(tile_no, TILE)
        y0[:, cols] = dot_t(x0[...], w0[cols, :])
        return carry

    lax.fori_loop(0, wide1 // TILE, y0_tile, 0)
    p_far.wait()
    p_all = p_sum[0] + p_sum[1]
    spans = ((0, n0, v0_out), (n0, n1, v1_out), (n0 + n1, 2 * wide2, v2_out))
    for first, size, v_out in spans:
        p_vec = p_all[:, first:first + size]
        v_out[...] = p_vec / jnp.maximum(jnp.sqrt(total(p_vec * p_vec)), EPSILON)
    u0_out[...] = dot_t(row(v0_out[...]), w0[own1, :])[0:1]
    u1_out[...] = dot_t(row(v1_out[...]), w1[own2, :])[0:1]
    u2_out[...] = dot_t(row(v2_out[...]), w2[own2, :])[0:1]
    lane = lax.broadcasted_iota(jnp.int32, (8, 128), 1)

    def pack(values):
        packed = jnp.zeros((8, 128), F32)
        for place, value in enumerate(values):
            packed = jnp.where(lane == place, value, packed)
        return packed

    n_buf[me] = pack([total(u_out[...] * u_out[...]) for u_out in (u0_out, u1_out, u2_out)])
    n_copies = spread(n_buf, 3)
    for copy in n_copies:
        copy.start()
    for piece_no in range(3, PIECES):
        w1x_copy(piece_no).start()
    for copy in gives[1:]:
        copy.start()

    @pl.when(core == 0)
    def _():
        send(t_fake, tt.at[own2, :], w_send.at[3], w_recv.at[3], mate).start()

    @pl.when(core == 1)
    def _():
        send(t_real, tt.at[own2, :], w_send.at[3], w_recv.at[3], mate).start()

    for copy in n_copies:
        copy.wait()
    sigmas = jnp.sqrt(n_buf[0] + n_buf[1] + n_buf[2] + n_buf[3])
    sig_out[...] = sigmas
    sig0, sig1, sig2 = sigmas[0:1, 0:1], sigmas[0:1, 1:2], sigmas[0:1, 2:3]
    inv0, inv1, inv2 = 1.0 / sig0, 1.0 / sig1, 1.0 / sig2
    u0_out[...] = u0_out[...] / sig0
    u1_out[...] = u1_out[...] / sig1
    u2_out[...] = u2_out[...] / sig2

    def chunk_copy(buf, slot, chunk_no, send_sem, recv_sem):
        rows = buf.at[slot, part(chunk_no, step), :]
        return send(rows, rows, send_sem.at[chunk_no], recv_sem.at[chunk_no], far)

    def layer0(chunk_no, carry):
        rows = part(chunk_no, step)
        x1[chip, rows, :] = leaky_relu(y0[rows, :] * inv0).astype(BF16)
        chunk_copy(x1, chip, chunk_no, x1_send, x1_recv).start()
        return carry

    lax.fori_loop(0, CHUNKS, layer0, 0)

    batch = part(core, n_rows)

    def outputs(src, dst, which):
        return (
            pltpu.make_async_copy(src, dst, put_sem.at[which]),
            send(src, dst, out_send.at[which], out_recv.at[which], mate),
        )

    def halves(src, dst, size, which):
        return (
            pltpu.make_async_copy(src.at[part(core, size), :], dst.at[:, batch], put_sem.at[which]),
            send(src.at[part(1 - core, size), :], dst.at[:, batch], out_send.at[which], out_recv.at[which], mate),
        )

    x1_near = outputs(x1.at[chip], x1_out.at[batch, part(chip, wide1)], 0)
    for copy in x1_near:
        copy.start()
    for piece_no in range(PIECES):
        w1x_copy(piece_no).wait_recv()
        w1x_forward(piece_no).start()

    gives[1].wait_recv()

    def layer1(chunk_no, carry):
        rows = part(chunk_no, step)
        chunk_copy(x1, other, chunk_no, x1_send, x1_recv).wait_recv()
        y_val = (dot_t(x1[0, rows, :], w1[:, pl.ds(0, wide1)]) + dot_t(x1[1, rows, :], w1[:, pl.ds(wide1, wide1)])) * inv1
        y1[rows, :] = y_val
        x2[chip, rows, :] = leaky_relu(y_val).astype(BF16)
        chunk_copy(x2, chip, chunk_no, x2_send, x2_recv).start()
        return carry

    lax.fori_loop(0, CHUNKS, layer1, 0)
    x1_far = outputs(x1.at[other], x1_out.at[batch, part(other, wide1)], 1)
    for copy in x1_far:
        copy.start()

    gives[2].wait_recv()
    pltpu.make_async_copy(t_real, tt.at[own2, :], load_sem.at[4]).wait()
    t_give = send(t_real, tt.at[own2, :], w_send.at[3], w_recv.at[3], mate)
    t_give.wait_recv()

    def layer2(chunk_no, carry):
        corr2, loss = carry
        rows = part(chunk_no, step)
        chunk_copy(x2, other, chunk_no, x2_send, x2_recv).wait_recv()
        y_val = (dot_t(x2[0, rows, :], w2[:, pl.ds(0, wide2)]) + dot_t(x2[1, rows, :], w2[:, pl.ds(wide2, wide2)])) * inv2
        e_val = y_val - dot_t(eye[0:step, 0:step], tt[:, rows])
        corr2 = corr2 + fold(e_val * y_val)
        loss = loss + fold(e_val * e_val)
        e_half = e_val.astype(BF16)
        h2_put[rows, :] = dot_n(e_half, w2[:, part(other, wide2)]).astype(BF16)
        send(h2_put.at[rows, :], h2_got.at[rows, :], h2_send.at[chunk_no], h2_recv.at[chunk_no], far).start()
        h2_own[rows, :] = dot_n(e_half, w2[:, part(chip, wide2)])
        store_transposed(e2_t, 0, rows, e_half)
        return corr2, loss

    zero = jnp.zeros((8, wide2), F32)
    corr2, loss = lax.fori_loop(0, CHUNKS, layer2, (zero, zero))

    def back1(chunk_no, corr1):
        rows = part(chunk_no, step)
        send(h2_put.at[rows, :], h2_got.at[rows, :], h2_send.at[chunk_no], h2_recv.at[chunk_no], far).wait_recv()
        y_val = y1[rows, :]
        e_val = (h2_own[rows, :] + h2_got[rows, :].astype(F32)) * (inv2 * leaky_slope(y_val))
        e_half = e_val.astype(BF16)
        e1[chip, rows, :] = e_half
        chunk_copy(e1, chip, chunk_no, e1_send, e1_recv).start()
        store_transposed(e1_t, 0, rows, e_half)
        return corr1 + fold(e_val * y_val)

    corr1 = lax.fori_loop(0, CHUNKS, back1, zero)
    lesser = [
        outputs(x2.at[0], x2_out.at[batch, pl.ds(0, wide2)], 2),
        outputs(x2.at[1], x2_out.at[batch, pl.ds(wide2, wide2)], 3),
        halves(e2_t, e2_out, rows2, 4),
        halves(e1_t, e1_out, rows2, 5),
    ]
    for pair in lesser:
        for copy in pair:
            copy.start()
    for piece_no in range(PIECES):
        w1x_forward(piece_no).wait_recv()

    late = n_rows - EARLY * step

    def h0_copy(chunk_no):
        rows = part(chunk_no, step)
        return send(h0_put.at[rows, :], h0_got.at[rows, :], h0_send.at[chunk_no], h0_recv.at[chunk_no], far)

    def late_copies(chunk_no):
        src = h0_put.at[part(chunk_no, step), :]
        place = chunk_no - EARLY
        dst = both_out.at[pl.ds(pl.multiple_of(core * late + place * step, step), step), :]
        return (
            pltpu.make_async_copy(src, sum_out.at[part(place, step), :], sum_sem.at[place]),
            pltpu.make_async_copy(src, dst, both_sem.at[place]),
            send(src, dst, both_send.at[place], both_recv.at[place], mate),
        )

    def back0(chunk_no, corr0):
        rows = part(chunk_no, step)
        chunk_copy(e1, other, chunk_no, e1_send, e1_recv).wait_recv()

        def h1_tile(tile_no, corr):
            cols = part(tile_no, wide2)
            own_cols = pl.ds(pl.multiple_of(chip * wide1 + tile_no * wide2, 128), wide2)
            h_val = dot_n(e1[chip, rows, :], w1[:, own_cols]) + dot_n(e1[other, rows, :], w1x[:, cols])
            y_val = y0[rows, cols]
            e_val = h_val * (inv1 * leaky_slope(y_val))
            e0[:, cols] = e_val.astype(BF16)
            return corr + fold(e_val * y_val)

        corr0 = lax.fori_loop(0, wide1 // wide2, h1_tile, corr0)
        h0_put[rows, :] = dot_n(e0[...], w0[...]).astype(BF16)
        return corr0

    def transpose0(chunk_no):
        rows = part(chunk_no, step)

        def tile(tile_no, carry):
            store_transposed(e0_t, tile_no * wide2, rows, e0[:, part(tile_no, wide2)])
            return carry

        lax.fori_loop(0, wide1 // wide2, tile, 0)

    def back0_early(chunk_no, corr0):
        corr0 = back0(chunk_no, corr0)
        h0_copy(chunk_no).start()
        transpose0(chunk_no)
        return corr0

    def back0_late(chunk_no, corr0):
        corr0 = back0(chunk_no, corr0)
        for copy in late_copies(chunk_no):
            copy.start()
        transpose0(chunk_no)
        return corr0

    corr0 = lax.fori_loop(0, EARLY, back0_early, zero)
    corr0 = lax.fori_loop(EARLY, CHUNKS, back0_late, corr0)
    e0_pair = halves(e0_t, e0_out, rows1, 6)
    for copy in e0_pair:
        copy.start()
    c_buf[me] = pack([total(corr0) * inv0, total(corr1), total(corr2), total(loss)])
    c_copies = spread(c_buf, 6)
    for copy in c_copies:
        copy.start()

    def dx_copies(chunk_no):
        rows = part(chunk_no, step)
        dst = dx_out.at[pl.ds(pl.multiple_of((core * EARLY + chunk_no) * step, step), step), :]
        return (
            pltpu.make_async_copy(dx.at[rows, :], dst, dx_sem.at[chunk_no]),
            send(dx.at[rows, :], dst, dx_send.at[chunk_no], dx_recv.at[chunk_no], mate),
        )

    def finish(chunk_no, carry):
        rows = part(chunk_no, step)
        h0_copy(chunk_no).wait_recv()
        dx[rows, :] = (h0_put[rows, :].astype(F32) + h0_got[rows, :].astype(F32)) * inv0
        for copy in dx_copies(chunk_no):
            copy.start()
        return carry

    lax.fori_loop(0, EARLY, finish, 0)
    for copy in c_copies:
        copy.wait()
    cor_out[...] = c_buf[0] + c_buf[1] + c_buf[2] + c_buf[3]

    for copy in gives:
        copy.wait_send()
    t_give.wait_send()
    for piece_no in range(PIECES):
        w1x_copy(piece_no).wait_send()
        w1x_forward(piece_no).wait_send()
    for pair in (x1_near, x1_far, *lesser, e0_pair):
        for copy in pair:
            copy.wait()

    def drain(chunk_no, carry):
        rows = part(chunk_no, step)
        chunk_copy(x1, chip, chunk_no, x1_send, x1_recv).wait_send()
        chunk_copy(x2, chip, chunk_no, x2_send, x2_recv).wait_send()
        send(h2_put.at[rows, :], h2_got.at[rows, :], h2_send.at[chunk_no], h2_recv.at[chunk_no], far).wait_send()
        chunk_copy(e1, chip, chunk_no, e1_send, e1_recv).wait_send()
        return carry

    lax.fori_loop(0, CHUNKS, drain, 0)

    def drain_early(chunk_no, carry):
        h0_copy(chunk_no).wait_send()
        for copy in dx_copies(chunk_no):
            copy.wait()
        return carry

    lax.fori_loop(0, EARLY, drain_early, 0)

    def drain_late(chunk_no, carry):
        for copy in late_copies(chunk_no):
            copy.wait()
        return carry

    lax.fori_loop(EARLY, CHUNKS, drain_late, 0)


def run_chain(x_real, x_fake, weight0, weight1, weight2, u_left0, u_left1, u_left2, t_real, t_fake):
    n_rows, n0 = x_real.shape
    rows1 = weight0.shape[0]
    rows2, n1 = weight1.shape
    wide1, wide2 = 2 * rows1, 2 * rows2
    n2 = 2 * wide2
    early = n_rows // CHUNKS * EARLY
    late = n_rows - early
    hbm = pl.BlockSpec(memory_space=pl.ANY)
    vmem = pl.BlockSpec(memory_space=pltpu.VMEM)
    shape = jax.ShapeDtypeStruct
    dma = pltpu.SemaphoreType.DMA
    return pl.pallas_call(
        chain_kernel,
        out_shape=(
            shape((2 * n_rows, n1), BF16), shape((2 * n_rows, n2), BF16), shape((rows2, 2 * n_rows), BF16), shape((rows2, 2 * n_rows), BF16),
            shape((rows1, 2 * n_rows), BF16), shape((2 * early, n0), F32), shape((late, n0), BF16), shape((2 * late, n0), BF16),
            shape((1, n0), F32), shape((1, n1), F32), shape((1, n2), F32),
            shape((1, rows1), F32), shape((1, rows2), F32), shape((1, rows2), F32),
            shape((8, 128), F32), shape((8, 128), F32),
        ),
        in_specs=[hbm] * 5 + [vmem] * 3 + [hbm] * 2,
        out_specs=[hbm] * 8 + [vmem] * 8,
        scratch_shapes=[
            pltpu.VMEM((wide1, n0), BF16), pltpu.VMEM((wide2, n1), BF16), pltpu.VMEM((wide2, wide1), BF16), pltpu.VMEM((wide2, n2), BF16),
            pltpu.VMEM((n_rows, n0), BF16), pltpu.VMEM((2, n_rows, wide1), BF16), pltpu.VMEM((2, n_rows, wide2), BF16),
            pltpu.VMEM((n_rows, wide1), F32), pltpu.VMEM((n_rows, wide2), F32), pltpu.VMEM((wide2, n_rows), BF16),
            pltpu.VMEM((wide2, n_rows), BF16), pltpu.VMEM((n_rows, wide2), F32), pltpu.VMEM((n_rows, wide2), BF16), pltpu.VMEM((n_rows, wide2), BF16),
            pltpu.VMEM((2, n_rows, wide2), BF16), pltpu.VMEM((wide2, n_rows), BF16), pltpu.VMEM((n_rows // CHUNKS, wide1), BF16), pltpu.VMEM((wide1, n_rows), BF16),
            pltpu.VMEM((n_rows, n0), BF16), pltpu.VMEM((early, n0), BF16), pltpu.VMEM((early, n0), F32),
            pltpu.VMEM((4, 1, n0 + n1 + n2), F32), pltpu.VMEM((2, 1, n0 + n1 + n2), F32), pltpu.VMEM((4, 8, 128), F32), pltpu.VMEM((4, 8, 128), F32), pltpu.VMEM((256, 256), BF16),
            dma((5,)), dma((7,)), dma((4,)), dma((4,)), dma((PIECES,)), dma((PIECES,)), dma((PIECES,)), dma((PIECES,)), dma((9,)), dma((9,)),
            dma((CHUNKS,)), dma((CHUNKS,)), dma((CHUNKS,)), dma((CHUNKS,)), dma((CHUNKS,)), dma((CHUNKS,)),
            dma((CHUNKS,)), dma((CHUNKS,)), dma((EARLY,)), dma((EARLY,)), dma((7,)), dma((7,)), dma((EARLY,)), dma((EARLY,)), dma((EARLY,)),
            dma((CHUNKS - EARLY,)), dma((CHUNKS - EARLY,)), dma((CHUNKS - EARLY,)), dma((CHUNKS - EARLY,)),
        ],
        compiler_params=pltpu.CompilerParams(collective_id=0, has_side_effects=True, vmem_limit_bytes=67043328),
        name="chain",
    )(x_real, x_fake, weight0, weight1, weight2, u_left0, u_left1, u_left2, t_real.T, t_fake.T)


def grad_kernel(x1_in, e1_in, x2_in, e2_in, x_real, x_fake, e0_in, dx_in, u0_in, u1_in, u2_in, v0_in, v1_in, v2_in, sig_in, cor_in,
                dw0_out, dw1_out, dw2_out, dx_real, dx_fake, u0_out, u1_out, u2_out, v0_out, v1_out, v2_out, sig_out, loss_out,
                x1, e1, x2, e2, x0, e0, dx, dw0, dw1, dw2, u0, u1, u2, v0, v1, v2, sig, cor, in_sem, x1_sem, out_sem, dw1_sem, dw0_sem):
    n_rows = x_real.shape[0]
    early = dx.shape[0] // 2
    tiles1 = x1_sem.shape[0]
    tiles0 = dw0_sem.shape[0]

    def pull(src, dst, which):
        copy = pltpu.make_async_copy(src, dst, in_sem.at[which])
        copy.start()
        return copy

    small = [pull(src, dst, place) for place, (src, dst) in enumerate((
        (u0_in, u0), (u1_in, u1), (u2_in, u2), (v0_in, v0), (v1_in, v1), (v2_in, v2), (sig_in, sig), (cor_in, cor)))]
    def tile_of(size, tiles, tile_no):
        return pl.ds(tile_no * (size // tiles), size // tiles)

    def load(src, dst, which):
        return pltpu.make_async_copy(src, dst, in_sem.at[which])

    got_e1 = pull(e1_in, e1, 11)
    got_x1 = []
    for tile_no in range(tiles1):
        cols = tile_of(x1.shape[1], tiles1, tile_no)
        got_x1.append(pltpu.make_async_copy(x1_in.at[:, cols], x1.at[:, cols], x1_sem.at[tile_no]))
    got_e0 = load(e0_in, e0, 8)
    got_x0 = [load(x_real, x0.at[pl.ds(0, n_rows), :], 9), load(x_fake, x0.at[pl.ds(n_rows, n_rows), :], 10)]
    got_dx = load(dx_in, dx, 12)
    got_2 = [load(e2_in, e2, 13), load(x2_in, x2, 14)]
    queue = [*got_x1, *got_x0, got_e0, got_dx, *got_2]

    def read_on(count=1):
        for _ in range(min(count, len(queue))):
            queue.pop(0).start()

    read_on(3)

    for copy in small:
        copy.wait()
    for src, dst in ((u0, u0_out), (u1, u1_out), (u2, u2_out), (v0, v0_out), (v1, v1_out), (v2, v2_out)):
        dst[...] = src[...].reshape(dst.shape)
    sig_out[...] = sig[0:1, 0:3].reshape(3)
    loss_out[...] = cor[0:1, 3:4] * (0.5 / n_rows)

    def column(u_new, layer_no):
        return jnp.broadcast_to(u_new[...] * cor[0:1, layer_no:layer_no + 1], (128, u_new.shape[1])).T[:, 0:1]

    def scale(layer_no):
        return 1.0 / (n_rows * sig[0:1, layer_no:layer_no + 1])

    pushes = []

    def gradient(errors, layer_in, cols, col, v_new, rate, dst, out, sem):
        dst[:, cols] = (dot_n(errors[...], layer_in[:, cols]) - col * v_new[:, cols]) * rate
        copy = pltpu.make_async_copy(dst.at[:, cols], out.at[:, cols], sem)
        copy.start()
        pushes.append(copy)

    got_e1.wait()
    col1, scale1 = column(u1, 1), scale(1)
    for tile_no in range(tiles1):
        got_x1[tile_no].wait()
        read_on()
        gradient(e1, x1, tile_of(x1.shape[1], tiles1, tile_no), col1, v1, scale1, dw1, dw1_out, dw1_sem.at[tile_no])
    got_e0.wait()
    read_on(3)
    for copy in got_x0:
        copy.wait()
    col0, scale0 = column(u0, 0), scale(0)
    for tile_no in range(tiles0):
        gradient(e0, x0, tile_of(x0.shape[1], tiles0, tile_no), col0, v0, scale0, dw0, dw0_out, dw0_sem.at[tile_no])
    got_dx.wait()
    for place, dst in enumerate((dx_real, dx_fake)):
        copy = pltpu.make_async_copy(dx.at[pl.ds(place * early, early), :], dst.at[pl.ds(0, early), :], out_sem.at[place])
        copy.start()
        pushes.append(copy)
    for copy in got_2:
        copy.wait()
    col2, scale2 = column(u2, 2), scale(2)
    for tile_no in range(2):
        gradient(e2, x2, tile_of(x2.shape[1], 2, tile_no), col2, v2, scale2, dw2, dw2_out, out_sem.at[2 + tile_no])
    for copy in pushes:
        copy.wait()


def run_grads(x1, e1, x2, e2, x_real, x_fake, e0, dx, u0, u1, u2, v0, v1, v2, sig, cor):
    both, n1 = x1.shape
    n_rows, n0 = x_real.shape
    n2 = x2.shape[1]
    rows2 = e1.shape[0]
    rows1 = e0.shape[0]
    tiles1, tiles0 = 10, 5
    shape = jax.ShapeDtypeStruct
    hbm = pl.BlockSpec(memory_space=pl.ANY)
    vmem = pl.BlockSpec(memory_space=pltpu.VMEM)
    dma = pltpu.SemaphoreType.DMA
    flops = 2 * both * (rows2 * (n1 + n2) + rows1 * n0)
    inputs = (x1, e1, x2, e2, x_real, x_fake, e0, dx, u0, u1, u2, v0, v1, v2, sig, cor)
    return pl.pallas_call(
        grad_kernel,
        out_shape=(
            shape((rows1, n0), F32), shape((rows2, n1), F32), shape((rows2, n2), F32), shape((n_rows, n0), F32), shape((n_rows, n0), F32),
            shape((rows1,), F32), shape((rows2,), F32), shape((rows2,), F32), shape((n0,), F32), shape((n1,), F32), shape((n2,), F32),
            shape((3,), F32), shape((1, 1), F32),
        ),
        in_specs=[hbm] * len(inputs),
        out_specs=[hbm] * 5 + [vmem] * 8,
        scratch_shapes=[
            pltpu.VMEM((both, n1), BF16), pltpu.VMEM((rows2, both), BF16), pltpu.VMEM((both, n2), BF16), pltpu.VMEM((rows2, both), BF16),
            pltpu.VMEM((both, n0), BF16), pltpu.VMEM((rows1, both), BF16), pltpu.VMEM(dx.shape, F32),
            pltpu.VMEM((rows1, n0), F32), pltpu.VMEM((rows2, n1), F32), pltpu.VMEM((rows2, n2), F32),
            *[pltpu.VMEM(array.shape, F32) for array in (u0, u1, u2, v0, v1, v2, sig, cor)],
            dma((15,)), dma((tiles1,)), dma((4,)), dma((tiles1,)), dma((tiles0,)),
        ],
        compiler_params=pltpu.CompilerParams(vmem_limit_bytes=67043328),
        cost_estimate=pl.CostEstimate(flops=flops, bytes_accessed=45 * 1024 * 1024, transcendentals=0),
        name="grads",
    )(*inputs)


def finish_kernel(flip, real_in, fake_in, both_in, came_in, sig_in, real_out, fake_out, both, came, sig, dx, in_sem, out_sem):
    me = lax.axis_index("model")
    batch = me % 2
    if flip:
        batch = 1 - batch
    pieces = out_sem.shape[0]
    late = both.shape[0]
    size = late // pieces
    first = real_out.shape[0] - late
    scale_copy = pltpu.make_async_copy(sig_in, sig, in_sem.at[2 * pieces])
    scale_copy.start()

    def pulls(piece):
        rows = pl.ds(piece * size, size)
        return (
            pltpu.make_async_copy(both_in.at[pl.ds(pl.multiple_of(batch * late + piece * size, size), size), :], both.at[rows, :], in_sem.at[2 * piece]),
            pltpu.make_async_copy(came_in.at[rows, :], came.at[rows, :], in_sem.at[2 * piece + 1]),
        )

    def push(dst, piece):
        return pltpu.make_async_copy(dx.at[pl.ds(piece * size, size), :], dst.at[pl.ds(first + piece * size, size), :], out_sem.at[piece])

    for piece in range(pieces):
        for copy in pulls(piece):
            copy.start()
    scale_copy.wait()
    inv0 = 1.0 / sig[0:1, 0:1]
    for piece in range(pieces):
        for copy in pulls(piece):
            copy.wait()
        rows = pl.ds(piece * size, size)
        dx[rows, :] = (both[rows, :].astype(F32) + came[rows, :].astype(F32)) * inv0

        @pl.when(batch == 0)
        def _():
            push(real_out, piece).start()

        @pl.when(batch == 1)
        def _():
            push(fake_out, piece).start()

    for piece in range(pieces):
        push(real_out, piece).wait()


def run_finish(flip, dx_real, dx_fake, both, came, sig):
    late, n0 = came.shape
    pieces = 4
    hbm = pl.BlockSpec(memory_space=pl.ANY)
    dma = pltpu.SemaphoreType.DMA
    shape = jax.ShapeDtypeStruct(dx_real.shape, F32)
    return pl.pallas_call(
        functools.partial(finish_kernel, flip),
        out_shape=(shape, shape),
        in_specs=[hbm] * 5,
        out_specs=[hbm] * 2,
        scratch_shapes=[
            pltpu.VMEM((late, n0), BF16), pltpu.VMEM((late, n0), BF16), pltpu.VMEM((8, 128), F32), pltpu.VMEM((late, n0), F32),
            dma((2 * pieces + 1,)), dma((pieces,)),
        ],
        input_output_aliases={0: 0, 1: 1},
        compiler_params=pltpu.CompilerParams(vmem_limit_bytes=67043328),
        cost_estimate=pl.CostEstimate(flops=4 * late * n0, bytes_accessed=8 * late * n0, transcendentals=0),
        name="finish",
    )(dx_real, dx_fake, both, came, sig)


def swap(values, bits):
    return lax.ppermute(values, "model", [(dev, dev ^ bits) for dev in range(4)])


def solution(mesh):
    rows_spec = P("rep", None)
    weight_spec = P(("rep", "model"), None)
    left_spec = P(("rep", "model"))
    target_spec = P("rep", "model")
    group_spec = P("rep")

    def local_step(x_real, x_fake, weight0, weight1, weight2, u_left0, u_left1, u_left2, t_real, t_fake):
        x1, x2, e2, e1, e0, dx, sums, both, v0, v1, v2, u0, u1, u2, sig, cor = run_chain(x_real, x_fake, weight0, weight1, weight2, u_left0, u_left1, u_left2, t_real, t_fake)
        came = swap(sums, 2)
        dw0, dw1, dw2, dx_real, dx_fake, u0, u1, u2, v0, v1, v2, sigmas, loss = run_grads(x1, e1, x2, e2, x_real, x_fake, e0, dx, u0, u1, u2, v0, v1, v2, sig, cor)
        came, sigmas = lax.optimization_barrier((came, sigmas))
        came_mate = swap(came, 1)
        dx_real, dx_fake = run_finish(False, dx_real, dx_fake, both, came, sig)
        dx_real, dx_fake = run_finish(True, dx_real, dx_fake, both, came_mate, sig)
        return (loss[0], dx_real, dx_fake, dw0, dw1, dw2, u0, u1, u2, v0, v1, v2, sigmas)

    return jax.shard_map(local_step, mesh=mesh, in_specs=(rows_spec, rows_spec, weight_spec, weight_spec, weight_spec, left_spec, left_spec, left_spec, target_spec, target_spec), out_specs=(group_spec, rows_spec, rows_spec, weight_spec, weight_spec, weight_spec, left_spec, left_spec, left_spec, group_spec, group_spec, group_spec, group_spec), check_vma=False)
```

```python
import functools

import jax
import jax.numpy as jnp
from jax import lax
from jax.experimental import pallas as pl
from jax.experimental.pallas import tpu as pltpu
from jax.sharding import PartitionSpec as P

SLOPE = 0.2
EPSILON = 1e-12
MESH = pl.DeviceIdType.MESH
CHUNKS = 4
EARLY = 1
PIECES = 5
TILE = 256
BF16 = jnp.bfloat16
F32 = jnp.float32


def leaky_relu(values):
    return jnp.where(values > 0, values, SLOPE * values)


def leaky_slope(values):
    return jnp.where(values > 0, 1.0, SLOPE)


def dot_t(left, right):
    return lax.dot_general(left, right, (((1,), (1,)), ((), ())), preferred_element_type=F32)


def dot_n(left, right):
    return lax.dot_general(left, right, (((1,), (0,)), ((), ())), preferred_element_type=F32)


def t_dot(left, right):
    return lax.dot_general(left, right, (((0,), (0,)), ((), ())), preferred_element_type=F32)


def fold(values):
    rows, cols = values.shape
    return jnp.sum(values.reshape(rows // 8, 8, cols), axis=0)


def total(values):
    return jnp.sum(jnp.sum(values, axis=1, keepdims=True), axis=0, keepdims=True)


def chain_kernel(x_real, x_fake, w0_in, w1_in, w2_in, u0_in, u1_in, u2_in, t_real, t_fake,
                 x1_out, x2_out, e2_out, e1_out, e0_out, dx_out, sum_out, both_out, v0_out, v1_out, v2_out, u0_out, u1_out, u2_out, sig_out, cor_out,
                 w0, w1, w1x, w2, x0, x1, x2, y0, y1, tt, e2_t, h2_own, h2_put, h2_got, e1, e1_t, e0, e0_t, h0_put, h0_got, dx,
                 p_buf, p_sum, n_buf, c_buf,
                 eye, load_sem, put_sem, w_send, w_recv, w1x_send, w1x_recv, fwd_send, fwd_recv, small_send, small_recv,
                 x1_send, x1_recv, x2_send, x2_recv, h2_send, h2_recv, e1_send, e1_recv, h0_send, h0_recv, out_send, out_recv, dx_sem, dx_send, dx_recv, sum_sem, both_sem, both_send, both_recv):
    me = lax.axis_index("model")
    chip = me // 2
    core = me % 2
    other = 1 - chip
    mate = me + 1 - 2 * core
    far = me + 2 - 4 * chip
    diag = mate + 2 - 4 * chip
    n_rows, n0 = x0.shape
    wide1 = w0.shape[0]
    rows1 = wide1 // 2
    wide2 = w2.shape[0]
    rows2 = wide2 // 2
    n1 = 2 * wide1
    step = n_rows // CHUNKS
    piece = rows2 // PIECES

    def send(src, dst, send_sem, recv_sem, device):
        return pltpu.make_async_remote_copy(src_ref=src, dst_ref=dst, send_sem=send_sem, recv_sem=recv_sem, device_id={"model": device}, device_id_type=MESH)

    def part(index, size):
        return pl.ds(pl.multiple_of(index * size, size), size)

    barrier = pltpu.get_barrier_semaphore()
    for device in (mate, far, diag):
        pl.semaphore_signal(barrier, inc=1, device_id={"model": device}, device_id_type=MESH)
    pl.semaphore_wait(barrier, 3)

    def w1x_copy(piece_no):
        return send(
            w1_in.at[pl.ds(piece_no * piece, piece), part(other, wide1)],
            w1x.at[pl.ds(pl.multiple_of(core * rows2 + piece_no * piece, piece), piece), :],
            w1x_send.at[piece_no], w1x_recv.at[piece_no], far)

    def w1x_forward(piece_no):
        rows = w1x.at[pl.ds(pl.multiple_of(core * rows2 + piece_no * piece, piece), piece), :]
        return send(rows, rows, fwd_send.at[piece_no], fwd_recv.at[piece_no], mate)

    own1, own2 = part(core, rows1), part(core, rows2)
    loads = [
        pltpu.make_async_copy(w0_in, w0.at[own1, :], load_sem.at[0]),
        pltpu.make_async_copy(w1_in, w1.at[own2, :], load_sem.at[1]),
        pltpu.make_async_copy(w2_in, w2.at[own2, :], load_sem.at[2]),
    ]
    gives = [
        send(w0.at[own1, :], w0.at[own1, :], w_send.at[0], w_recv.at[0], mate),
        send(w1.at[own2, :], w1.at[own2, :], w_send.at[1], w_recv.at[1], mate),
        send(w2.at[own2, :], w2.at[own2, :], w_send.at[2], w_recv.at[2], mate),
    ]
    w1x_copy(0).start()
    for copy in loads:
        copy.start()

    w1x_copy(1).start()

    def mine(x_in, t_own):
        return (
            pltpu.make_async_copy(x_in, x0, load_sem.at[3]),
            pltpu.make_async_copy(t_own, tt.at[own2, :], load_sem.at[4]),
        )

    @pl.when(core == 0)
    def _():
        for copy in mine(x_real, t_real):
            copy.start()

    @pl.when(core == 1)
    def _():
        for copy in mine(x_fake, t_fake):
            copy.start()

    def row(values):
        return jnp.broadcast_to(values.reshape(1, values.size).astype(BF16), (16, values.size))

    lanes = lax.broadcasted_iota(jnp.int32, eye.shape, 1)
    eye[...] = jnp.where(lanes == lax.broadcasted_iota(jnp.int32, eye.shape, 0), 1.0, 0.0).astype(BF16)

    def store_transposed(dst, first, rows, values):
        for begin in range(0, values.shape[1], eye.shape[0]):
            size = min(eye.shape[0], values.shape[1] - begin)
            block = dot_t(eye[0:size, 0:size], values[:, begin:begin + size])
            dst[pl.ds(pl.multiple_of(first + begin, 128), size), rows] = block.astype(BF16)

    u_rows = [row(u0_in[...]), row(u1_in[...]), row(u2_in[...])]
    loads[0].wait()
    p_buf[me, :, pl.ds(0, n0)] = dot_n(u_rows[0], w0[own1, :])[0:1]
    loads[1].wait()

    def p1_tile(tile_no, carry):
        cols = part(tile_no, wide1 // 2)
        p_buf[me, :, pl.ds(pl.multiple_of(n0 + tile_no * (wide1 // 2), 128), wide1 // 2)] = dot_n(u_rows[1], w1[own2, cols])[0:1]
        return carry

    lax.fori_loop(0, 4, p1_tile, 0)
    loads[2].wait()
    p_buf[me, :, pl.ds(n0 + n1, wide2 * 2)] = dot_n(u_rows[2], w2[own2, :])[0:1]

    def spread(buf, first):
        return [send(buf.at[me], buf.at[me], small_send.at[first + which], small_recv.at[first + which], device) for which, device in enumerate((mate, far, diag))]

    p_near = send(p_buf.at[me], p_buf.at[me], small_send.at[0], small_recv.at[0], mate)
    p_near.start()
    gives[0].start()
    p_near.wait()
    p_sum[chip] = p_buf[2 * chip] + p_buf[2 * chip + 1]
    p_far = send(p_sum.at[chip], p_sum.at[chip], small_send.at[1], small_recv.at[1], far)
    p_far.start()
    w1x_copy(2).start()
    w1x_copy(3).start()

    pltpu.make_async_copy(x_real, x0, load_sem.at[3]).wait()
    gives[0].wait_recv()

    def y0_tile(tile_no, carry):
        cols = part(tile_no, TILE)
        y0[:, cols] = dot_t(x0[...], w0[cols, :])
        return carry

    lax.fori_loop(0, wide1 // TILE, y0_tile, 0)
    p_far.wait()
    p_all = p_sum[0] + p_sum[1]
    spans = ((0, n0, v0_out), (n0, n1, v1_out), (n0 + n1, 2 * wide2, v2_out))
    for first, size, v_out in spans:
        p_vec = p_all[:, first:first + size]
        v_out[...] = p_vec / jnp.maximum(jnp.sqrt(total(p_vec * p_vec)), EPSILON)
    u0_out[...] = dot_t(row(v0_out[...]), w0[own1, :])[0:1]
    u1_out[...] = dot_t(row(v1_out[...]), w1[own2, :])[0:1]
    u2_out[...] = dot_t(row(v2_out[...]), w2[own2, :])[0:1]
    lane = lax.broadcasted_iota(jnp.int32, (8, 128), 1)

    def pack(values):
        packed = jnp.zeros((8, 128), F32)
        for place, value in enumerate(values):
            packed = jnp.where(lane == place, value, packed)
        return packed

    n_buf[me] = pack([total(u_out[...] * u_out[...]) for u_out in (u0_out, u1_out, u2_out)])
    n_copies = spread(n_buf, 3)
    for copy in n_copies:
        copy.start()
    for piece_no in range(4, PIECES):
        w1x_copy(piece_no).start()
    for copy in gives[1:]:
        copy.start()

    @pl.when(core == 0)
    def _():
        send(t_fake, tt.at[own2, :], w_send.at[3], w_recv.at[3], mate).start()

    @pl.when(core == 1)
    def _():
        send(t_real, tt.at[own2, :], w_send.at[3], w_recv.at[3], mate).start()

    for copy in n_copies:
        copy.wait()
    sigmas = jnp.sqrt(n_buf[0] + n_buf[1] + n_buf[2] + n_buf[3])
    sig_out[...] = sigmas
    sig0, sig1, sig2 = sigmas[0:1, 0:1], sigmas[0:1, 1:2], sigmas[0:1, 2:3]
    inv0, inv1, inv2 = 1.0 / sig0, 1.0 / sig1, 1.0 / sig2
    u0_out[...] = u0_out[...] / sig0
    u1_out[...] = u1_out[...] / sig1
    u2_out[...] = u2_out[...] / sig2

    def chunk_copy(buf, slot, chunk_no, send_sem, recv_sem):
        rows = buf.at[slot, part(chunk_no, step), :]
        return send(rows, rows, send_sem.at[chunk_no], recv_sem.at[chunk_no], far)

    def layer0(chunk_no, carry):
        rows = part(chunk_no, step)
        x1[chip, rows, :] = leaky_relu(y0[rows, :] * inv0).astype(BF16)
        chunk_copy(x1, chip, chunk_no, x1_send, x1_recv).start()
        return carry

    lax.fori_loop(0, CHUNKS, layer0, 0)

    batch = part(core, n_rows)

    def outputs(src, dst, which):
        return (
            pltpu.make_async_copy(src, dst, put_sem.at[which]),
            send(src, dst, out_send.at[which], out_recv.at[which], mate),
        )

    def halves(src, dst, size, which):
        return (
            pltpu.make_async_copy(src.at[part(core, size), :], dst.at[:, batch], put_sem.at[which]),
            send(src.at[part(1 - core, size), :], dst.at[:, batch], out_send.at[which], out_recv.at[which], mate),
        )

    x1_near = outputs(x1.at[chip], x1_out.at[batch, part(chip, wide1)], 0)
    for copy in x1_near:
        copy.start()
    for piece_no in range(PIECES):
        w1x_copy(piece_no).wait_recv()
        w1x_forward(piece_no).start()

    gives[1].wait_recv()

    def layer1(chunk_no, carry):
        rows = part(chunk_no, step)
        chunk_copy(x1, other, chunk_no, x1_send, x1_recv).wait_recv()
        y_val = (dot_t(x1[0, rows, :], w1[:, pl.ds(0, wide1)]) + dot_t(x1[1, rows, :], w1[:, pl.ds(wide1, wide1)])) * inv1
        y1[rows, :] = y_val
        x2[chip, rows, :] = leaky_relu(y_val).astype(BF16)
        chunk_copy(x2, chip, chunk_no, x2_send, x2_recv).start()
        return carry

    lax.fori_loop(0, CHUNKS, layer1, 0)
    x1_far = outputs(x1.at[other], x1_out.at[batch, part(other, wide1)], 1)
    for copy in x1_far:
        copy.start()

    gives[2].wait_recv()
    pltpu.make_async_copy(t_real, tt.at[own2, :], load_sem.at[4]).wait()
    t_give = send(t_real, tt.at[own2, :], w_send.at[3], w_recv.at[3], mate)
    t_give.wait_recv()

    def layer2(chunk_no, carry):
        corr2, loss = carry
        rows = part(chunk_no, step)
        chunk_copy(x2, other, chunk_no, x2_send, x2_recv).wait_recv()
        y_val = (dot_t(x2[0, rows, :], w2[:, pl.ds(0, wide2)]) + dot_t(x2[1, rows, :], w2[:, pl.ds(wide2, wide2)])) * inv2
        e_val = y_val - dot_t(eye[0:step, 0:step], tt[:, rows])
        corr2 = corr2 + fold(e_val * y_val)
        loss = loss + fold(e_val * e_val)
        e_half = e_val.astype(BF16)
        h2_put[rows, :] = dot_n(e_half, w2[:, part(other, wide2)]).astype(BF16)
        send(h2_put.at[rows, :], h2_got.at[rows, :], h2_send.at[chunk_no], h2_recv.at[chunk_no], far).start()
        h2_own[rows, :] = dot_n(e_half, w2[:, part(chip, wide2)])
        store_transposed(e2_t, 0, rows, e_half)
        return corr2, loss

    zero = jnp.zeros((8, wide2), F32)
    corr2, loss = lax.fori_loop(0, CHUNKS, layer2, (zero, zero))

    def back1(chunk_no, corr1):
        rows = part(chunk_no, step)
        send(h2_put.at[rows, :], h2_got.at[rows, :], h2_send.at[chunk_no], h2_recv.at[chunk_no], far).wait_recv()
        y_val = y1[rows, :]
        e_val = (h2_own[rows, :] + h2_got[rows, :].astype(F32)) * (inv2 * leaky_slope(y_val))
        e_half = e_val.astype(BF16)
        e1[chip, rows, :] = e_half
        chunk_copy(e1, chip, chunk_no, e1_send, e1_recv).start()
        store_transposed(e1_t, 0, rows, e_half)
        return corr1 + fold(e_val * y_val)

    corr1 = lax.fori_loop(0, CHUNKS, back1, zero)
    lesser = [
        outputs(x2.at[0], x2_out.at[batch, pl.ds(0, wide2)], 2),
        outputs(x2.at[1], x2_out.at[batch, pl.ds(wide2, wide2)], 3),
        halves(e2_t, e2_out, rows2, 4),
        halves(e1_t, e1_out, rows2, 5),
    ]
    for pair in lesser:
        for copy in pair:
            copy.start()
    for piece_no in range(PIECES):
        w1x_forward(piece_no).wait_recv()

    late = n_rows - EARLY * step

    def h0_copy(chunk_no):
        rows = part(chunk_no, step)
        return send(h0_put.at[rows, :], h0_got.at[rows, :], h0_send.at[chunk_no], h0_recv.at[chunk_no], far)

    def late_copies(chunk_no):
        src = h0_put.at[part(chunk_no, step), :]
        place = chunk_no - EARLY
        dst = both_out.at[pl.ds(pl.multiple_of(core * late + place * step, step), step), :]
        return (
            pltpu.make_async_copy(src, sum_out.at[part(place, step), :], sum_sem.at[place]),
            pltpu.make_async_copy(src, dst, both_sem.at[place]),
            send(src, dst, both_send.at[place], both_recv.at[place], mate),
        )

    def back0(chunk_no, corr0):
        rows = part(chunk_no, step)
        chunk_copy(e1, other, chunk_no, e1_send, e1_recv).wait_recv()

        def h1_tile(tile_no, corr):
            cols = part(tile_no, wide2)
            own_cols = pl.ds(pl.multiple_of(chip * wide1 + tile_no * wide2, 128), wide2)
            h_val = dot_n(e1[chip, rows, :], w1[:, own_cols]) + dot_n(e1[other, rows, :], w1x[:, cols])
            y_val = y0[rows, cols]
            e_val = h_val * (inv1 * leaky_slope(y_val))
            e0[:, cols] = e_val.astype(BF16)
            return corr + fold(e_val * y_val)

        corr0 = lax.fori_loop(0, wide1 // wide2, h1_tile, corr0)
        h0_put[rows, :] = dot_n(e0[...], w0[...]).astype(BF16)
        return corr0

    def transpose0(chunk_no):
        rows = part(chunk_no, step)

        def tile(tile_no, carry):
            store_transposed(e0_t, tile_no * wide2, rows, e0[:, part(tile_no, wide2)])
            return carry

        lax.fori_loop(0, wide1 // wide2, tile, 0)

    def back0_early(chunk_no, corr0):
        corr0 = back0(chunk_no, corr0)
        h0_copy(chunk_no).start()
        transpose0(chunk_no)
        return corr0

    def back0_late(chunk_no, corr0):
        corr0 = back0(chunk_no, corr0)
        for copy in late_copies(chunk_no):
            copy.start()
        transpose0(chunk_no)
        return corr0

    corr0 = lax.fori_loop(0, EARLY, back0_early, zero)
    corr0 = lax.fori_loop(EARLY, CHUNKS, back0_late, corr0)
    e0_pair = halves(e0_t, e0_out, rows1, 6)
    for copy in e0_pair:
        copy.start()
    c_buf[me] = pack([total(corr0) * inv0, total(corr1), total(corr2), total(loss)])
    c_copies = spread(c_buf, 6)
    for copy in c_copies:
        copy.start()

    def dx_copies(chunk_no):
        rows = part(chunk_no, step)
        dst = dx_out.at[pl.ds(pl.multiple_of((core * EARLY + chunk_no) * step, step), step), :]
        return (
            pltpu.make_async_copy(dx.at[rows, :], dst, dx_sem.at[chunk_no]),
            send(dx.at[rows, :], dst, dx_send.at[chunk_no], dx_recv.at[chunk_no], mate),
        )

    def finish(chunk_no, carry):
        rows = part(chunk_no, step)
        h0_copy(chunk_no).wait_recv()
        dx[rows, :] = (h0_put[rows, :].astype(F32) + h0_got[rows, :].astype(F32)) * inv0
        for copy in dx_copies(chunk_no):
            copy.start()
        return carry

    lax.fori_loop(0, EARLY, finish, 0)
    for copy in c_copies:
        copy.wait()
    cor_out[...] = c_buf[0] + c_buf[1] + c_buf[2] + c_buf[3]

    for copy in gives:
        copy.wait_send()
    t_give.wait_send()
    for piece_no in range(PIECES):
        w1x_copy(piece_no).wait_send()
        w1x_forward(piece_no).wait_send()
    for pair in (x1_near, x1_far, *lesser, e0_pair):
        for copy in pair:
            copy.wait()

    def drain(chunk_no, carry):
        rows = part(chunk_no, step)
        chunk_copy(x1, chip, chunk_no, x1_send, x1_recv).wait_send()
        chunk_copy(x2, chip, chunk_no, x2_send, x2_recv).wait_send()
        send(h2_put.at[rows, :], h2_got.at[rows, :], h2_send.at[chunk_no], h2_recv.at[chunk_no], far).wait_send()
        chunk_copy(e1, chip, chunk_no, e1_send, e1_recv).wait_send()
        return carry

    lax.fori_loop(0, CHUNKS, drain, 0)

    def drain_early(chunk_no, carry):
        h0_copy(chunk_no).wait_send()
        for copy in dx_copies(chunk_no):
            copy.wait()
        return carry

    lax.fori_loop(0, EARLY, drain_early, 0)

    def drain_late(chunk_no, carry):
        for copy in late_copies(chunk_no):
            copy.wait()
        return carry

    lax.fori_loop(EARLY, CHUNKS, drain_late, 0)


def run_chain(x_real, x_fake, weight0, weight1, weight2, u_left0, u_left1, u_left2, t_real, t_fake):
    n_rows, n0 = x_real.shape
    rows1 = weight0.shape[0]
    rows2, n1 = weight1.shape
    wide1, wide2 = 2 * rows1, 2 * rows2
    n2 = 2 * wide2
    early = n_rows // CHUNKS * EARLY
    late = n_rows - early
    hbm = pl.BlockSpec(memory_space=pl.ANY)
    vmem = pl.BlockSpec(memory_space=pltpu.VMEM)
    shape = jax.ShapeDtypeStruct
    dma = pltpu.SemaphoreType.DMA
    return pl.pallas_call(
        chain_kernel,
        out_shape=(
            shape((2 * n_rows, n1), BF16), shape((2 * n_rows, n2), BF16), shape((rows2, 2 * n_rows), BF16), shape((rows2, 2 * n_rows), BF16),
            shape((rows1, 2 * n_rows), BF16), shape((2 * early, n0), F32), shape((late, n0), BF16), shape((2 * late, n0), BF16),
            shape((1, n0), F32), shape((1, n1), F32), shape((1, n2), F32),
            shape((1, rows1), F32), shape((1, rows2), F32), shape((1, rows2), F32),
            shape((8, 128), F32), shape((8, 128), F32),
        ),
        in_specs=[hbm] * 5 + [vmem] * 3 + [hbm] * 2,
        out_specs=[hbm] * 8 + [vmem] * 8,
        scratch_shapes=[
            pltpu.VMEM((wide1, n0), BF16), pltpu.VMEM((wide2, n1), BF16), pltpu.VMEM((wide2, wide1), BF16), pltpu.VMEM((wide2, n2), BF16),
            pltpu.VMEM((n_rows, n0), BF16), pltpu.VMEM((2, n_rows, wide1), BF16), pltpu.VMEM((2, n_rows, wide2), BF16),
            pltpu.VMEM((n_rows, wide1), F32), pltpu.VMEM((n_rows, wide2), F32), pltpu.VMEM((wide2, n_rows), BF16),
            pltpu.VMEM((wide2, n_rows), BF16), pltpu.VMEM((n_rows, wide2), F32), pltpu.VMEM((n_rows, wide2), BF16), pltpu.VMEM((n_rows, wide2), BF16),
            pltpu.VMEM((2, n_rows, wide2), BF16), pltpu.VMEM((wide2, n_rows), BF16), pltpu.VMEM((n_rows // CHUNKS, wide1), BF16), pltpu.VMEM((wide1, n_rows), BF16),
            pltpu.VMEM((n_rows, n0), BF16), pltpu.VMEM((early, n0), BF16), pltpu.VMEM((early, n0), F32),
            pltpu.VMEM((4, 1, n0 + n1 + n2), F32), pltpu.VMEM((2, 1, n0 + n1 + n2), F32), pltpu.VMEM((4, 8, 128), F32), pltpu.VMEM((4, 8, 128), F32), pltpu.VMEM((256, 256), BF16),
            dma((5,)), dma((7,)), dma((4,)), dma((4,)), dma((PIECES,)), dma((PIECES,)), dma((PIECES,)), dma((PIECES,)), dma((9,)), dma((9,)),
            dma((CHUNKS,)), dma((CHUNKS,)), dma((CHUNKS,)), dma((CHUNKS,)), dma((CHUNKS,)), dma((CHUNKS,)),
            dma((CHUNKS,)), dma((CHUNKS,)), dma((EARLY,)), dma((EARLY,)), dma((7,)), dma((7,)), dma((EARLY,)), dma((EARLY,)), dma((EARLY,)),
            dma((CHUNKS - EARLY,)), dma((CHUNKS - EARLY,)), dma((CHUNKS - EARLY,)), dma((CHUNKS - EARLY,)),
        ],
        compiler_params=pltpu.CompilerParams(collective_id=0, has_side_effects=True, vmem_limit_bytes=67043328),
        name="chain",
    )(x_real, x_fake, weight0, weight1, weight2, u_left0, u_left1, u_left2, t_real.T, t_fake.T)


def grad_kernel(x1_in, e1_in, x2_in, e2_in, x_real, x_fake, e0_in, dx_in, u0_in, u1_in, u2_in, v0_in, v1_in, v2_in, sig_in, cor_in,
                dw0_out, dw1_out, dw2_out, dx_real, dx_fake, u0_out, u1_out, u2_out, v0_out, v1_out, v2_out, sig_out, loss_out,
                x1, e1, x2, e2, x0, e0, dx, dw0, dw1, dw2, u0, u1, u2, v0, v1, v2, sig, cor, in_sem, x1_sem, out_sem, dw1_sem, dw0_sem):
    n_rows = x_real.shape[0]
    early = dx.shape[0] // 2
    tiles1 = x1_sem.shape[0]
    tiles0 = dw0_sem.shape[0]

    def pull(src, dst, which):
        copy = pltpu.make_async_copy(src, dst, in_sem.at[which])
        copy.start()
        return copy

    small = [pull(src, dst, place) for place, (src, dst) in enumerate((
        (u0_in, u0), (u1_in, u1), (u2_in, u2), (v0_in, v0), (v1_in, v1), (v2_in, v2), (sig_in, sig), (cor_in, cor)))]
    def tile_of(size, tiles, tile_no):
        return pl.ds(tile_no * (size // tiles), size // tiles)

    def load(src, dst, which):
        return pltpu.make_async_copy(src, dst, in_sem.at[which])

    got_e1 = pull(e1_in, e1, 11)
    got_x1 = []
    for tile_no in range(tiles1):
        cols = tile_of(x1.shape[1], tiles1, tile_no)
        got_x1.append(pltpu.make_async_copy(x1_in.at[:, cols], x1.at[:, cols], x1_sem.at[tile_no]))
    got_e0 = load(e0_in, e0, 8)
    got_x0 = [load(x_real, x0.at[pl.ds(0, n_rows), :], 9), load(x_fake, x0.at[pl.ds(n_rows, n_rows), :], 10)]
    got_dx = load(dx_in, dx, 12)
    got_2 = [load(e2_in, e2, 13), load(x2_in, x2, 14)]
    queue = [*got_x1, *got_x0, got_e0, got_dx, *got_2]

    def read_on(count=1):
        for _ in range(min(count, len(queue))):
            queue.pop(0).start()

    read_on(3)

    for copy in small:
        copy.wait()
    for src, dst in ((u0, u0_out), (u1, u1_out), (u2, u2_out), (v0, v0_out), (v1, v1_out), (v2, v2_out)):
        dst[...] = src[...].reshape(dst.shape)
    sig_out[...] = sig[0:1, 0:3].reshape(3)
    loss_out[...] = cor[0:1, 3:4] * (0.5 / n_rows)

    def column(u_new, layer_no):
        return jnp.broadcast_to(u_new[...] * cor[0:1, layer_no:layer_no + 1], (128, u_new.shape[1])).T[:, 0:1]

    def scale(layer_no):
        return 1.0 / (n_rows * sig[0:1, layer_no:layer_no + 1])

    pushes = []

    def gradient(errors, layer_in, cols, col, v_new, rate, dst, out, sem):
        dst[:, cols] = (dot_n(errors[...], layer_in[:, cols]) - col * v_new[:, cols]) * rate
        copy = pltpu.make_async_copy(dst.at[:, cols], out.at[:, cols], sem)
        copy.start()
        pushes.append(copy)

    got_e1.wait()
    col1, scale1 = column(u1, 1), scale(1)
    for tile_no in range(tiles1):
        got_x1[tile_no].wait()
        read_on()
        gradient(e1, x1, tile_of(x1.shape[1], tiles1, tile_no), col1, v1, scale1, dw1, dw1_out, dw1_sem.at[tile_no])
    got_e0.wait()
    read_on(3)
    for copy in got_x0:
        copy.wait()
    col0, scale0 = column(u0, 0), scale(0)
    for tile_no in range(tiles0):
        gradient(e0, x0, tile_of(x0.shape[1], tiles0, tile_no), col0, v0, scale0, dw0, dw0_out, dw0_sem.at[tile_no])
    got_dx.wait()
    for place, dst in enumerate((dx_real, dx_fake)):
        copy = pltpu.make_async_copy(dx.at[pl.ds(place * early, early), :], dst.at[pl.ds(0, early), :], out_sem.at[place])
        copy.start()
        pushes.append(copy)
    for copy in got_2:
        copy.wait()
    col2, scale2 = column(u2, 2), scale(2)
    for tile_no in range(2):
        gradient(e2, x2, tile_of(x2.shape[1], 2, tile_no), col2, v2, scale2, dw2, dw2_out, out_sem.at[2 + tile_no])
    for copy in pushes:
        copy.wait()


def run_grads(x1, e1, x2, e2, x_real, x_fake, e0, dx, u0, u1, u2, v0, v1, v2, sig, cor):
    both, n1 = x1.shape
    n_rows, n0 = x_real.shape
    n2 = x2.shape[1]
    rows2 = e1.shape[0]
    rows1 = e0.shape[0]
    tiles1, tiles0 = 10, 5
    shape = jax.ShapeDtypeStruct
    hbm = pl.BlockSpec(memory_space=pltpu.HBM)
    vmem = pl.BlockSpec(memory_space=pltpu.VMEM)
    dma = pltpu.SemaphoreType.DMA
    flops = 2 * both * (rows2 * (n1 + n2) + rows1 * n0)
    inputs = (x1, e1, x2, e2, x_real, x_fake, e0, dx, u0, u1, u2, v0, v1, v2, sig, cor)
    inputs = tuple(pltpu.with_memory_space_constraint(array, pltpu.HBM) for array in inputs)
    return pl.pallas_call(
        grad_kernel,
        out_shape=(
            shape((rows1, n0), F32), shape((rows2, n1), F32), shape((rows2, n2), F32), shape((n_rows, n0), F32), shape((n_rows, n0), F32),
            shape((rows1,), F32), shape((rows2,), F32), shape((rows2,), F32), shape((n0,), F32), shape((n1,), F32), shape((n2,), F32),
            shape((3,), F32), shape((1, 1), F32),
        ),
        in_specs=[hbm] * len(inputs),
        out_specs=[hbm] * 5 + [vmem] * 8,
        scratch_shapes=[
            pltpu.VMEM((both, n1), BF16), pltpu.VMEM((rows2, both), BF16), pltpu.VMEM((both, n2), BF16), pltpu.VMEM((rows2, both), BF16),
            pltpu.VMEM((both, n0), BF16), pltpu.VMEM((rows1, both), BF16), pltpu.VMEM(dx.shape, F32),
            pltpu.VMEM((rows1, n0), F32), pltpu.VMEM((rows2, n1), F32), pltpu.VMEM((rows2, n2), F32),
            *[pltpu.VMEM(array.shape, F32) for array in (u0, u1, u2, v0, v1, v2, sig, cor)],
            dma((15,)), dma((tiles1,)), dma((4,)), dma((tiles1,)), dma((tiles0,)),
        ],
        compiler_params=pltpu.CompilerParams(vmem_limit_bytes=48 * 1024 * 1024),
        cost_estimate=pl.CostEstimate(flops=flops, bytes_accessed=45 * 1024 * 1024, transcendentals=0),
        name="grads",
    )(*inputs)


def finish_kernel(flip, real_in, fake_in, both, came, sig, real_out, fake_out, dx, out_sem):
    me = lax.axis_index("model")
    batch = me % 2
    if flip:
        batch = 1 - batch
    pieces = out_sem.shape[0]
    late = came.shape[0]
    size = late // pieces
    first = real_out.shape[0] - late
    inv0 = 1.0 / sig[0:1, 0:1]

    def push(dst, piece):
        return pltpu.make_async_copy(dx.at[pl.ds(piece * size, size), :], dst.at[pl.ds(first + piece * size, size), :], out_sem.at[piece])

    for piece in range(pieces):
        rows = pl.ds(piece * size, size)
        own = pl.ds(pl.multiple_of(batch * late + piece * size, size), size)
        dx[rows, :] = (both[own, :].astype(F32) + came[rows, :].astype(F32)) * inv0

        @pl.when(batch == 0)
        def _():
            push(real_out, piece).start()

        @pl.when(batch == 1)
        def _():
            push(fake_out, piece).start()

    for piece in range(pieces):
        push(real_out, piece).wait()


def run_finish(flip, dx_real, dx_fake, both, came, sig):
    late, n0 = came.shape
    pieces = 4
    hbm = pl.BlockSpec(memory_space=pltpu.HBM)
    vmem = pl.BlockSpec(memory_space=pltpu.VMEM)
    shape = jax.ShapeDtypeStruct(dx_real.shape, F32)
    return pl.pallas_call(
        functools.partial(finish_kernel, flip),
        out_shape=(shape, shape),
        in_specs=[hbm] * 2 + [vmem] * 3,
        out_specs=[hbm] * 2,
        scratch_shapes=[pltpu.VMEM((late, n0), F32), pltpu.SemaphoreType.DMA((pieces,))],
        input_output_aliases={0: 0, 1: 1},
        compiler_params=pltpu.CompilerParams(vmem_limit_bytes=16 * 1024 * 1024),
        cost_estimate=pl.CostEstimate(flops=4 * late * n0, bytes_accessed=8 * late * n0, transcendentals=0),
        name="finish",
    )(dx_real, dx_fake, both, came, sig)


def swap(values, bits):
    return lax.ppermute(values, "model", [(dev, dev ^ bits) for dev in range(4)])


def solution(mesh):
    rows_spec = P("rep", None)
    weight_spec = P(("rep", "model"), None)
    left_spec = P(("rep", "model"))
    target_spec = P("rep", "model")
    group_spec = P("rep")

    def local_step(x_real, x_fake, weight0, weight1, weight2, u_left0, u_left1, u_left2, t_real, t_fake):
        x1, x2, e2, e1, e0, dx, sums, both, v0, v1, v2, u0, u1, u2, sig, cor = run_chain(x_real, x_fake, weight0, weight1, weight2, u_left0, u_left1, u_left2, t_real, t_fake)
        came = swap(sums, 2)
        dw0, dw1, dw2, dx_real, dx_fake, u0, u1, u2, v0, v1, v2, sigmas, loss = run_grads(x1, e1, x2, e2, x_real, x_fake, e0, dx, u0, u1, u2, v0, v1, v2, sig, cor)
        came, sigmas = lax.optimization_barrier((came, sigmas))
        came_mate = swap(came, 1)
        dx_real, dx_fake = run_finish(False, dx_real, dx_fake, both, came, sig)
        dx_real, dx_fake = run_finish(True, dx_real, dx_fake, both, came_mate, sig)
        return (loss[0], dx_real, dx_fake, dw0, dw1, dw2, u0, u1, u2, v0, v1, v2, sigmas)

    return jax.shard_map(local_step, mesh=mesh, in_specs=(rows_spec, rows_spec, weight_spec, weight_spec, weight_spec, left_spec, left_spec, left_spec, target_spec, target_spec), out_specs=(group_spec, rows_spec, rows_spec, weight_spec, weight_spec, weight_spec, left_spec, left_spec, left_spec, group_spec, group_spec, group_spec, group_spec), check_vma=False)
```

```python
import functools

import jax
import jax.numpy as jnp
from jax import lax
from jax.experimental import pallas as pl
from jax.experimental.pallas import tpu as pltpu
from jax.sharding import PartitionSpec as P


SLOPE = 0.2
EPSILON = 1e-12
MESH = pl.DeviceIdType.MESH
CHUNKS = 4
EARLY = 1
MIDDLE = 2
PIECES = 5
TILE = 256
BF16 = jnp.bfloat16
F32 = jnp.float32


def leaky_relu(values):
    return jnp.where(values > 0, values, SLOPE * values)


def leaky_slope(values):
    return jnp.where(values > 0, 1.0, SLOPE)


def dot_t(left, right):
    return lax.dot_general(left, right, (((1,), (1,)), ((), ())), preferred_element_type=F32)


def dot_n(left, right):
    return lax.dot_general(left, right, (((1,), (0,)), ((), ())), preferred_element_type=F32)


def fold(values):
    rows, cols = values.shape
    return jnp.sum(values.reshape(rows // 8, 8, cols), axis=0)


def total(values):
    return jnp.sum(jnp.sum(values, axis=1, keepdims=True), axis=0, keepdims=True)


def chain_kernel(x_real, x_fake, w0_in, w1_in, w2_in, u0_in, u1_in, u2_in, t_real, t_fake,
                 x1_out, x2_out, e2_out, e1_out, e0_out, got_out, mid_out, last_out, both_out, v0_out, v1_out, v2_out, u0_out, u1_out, u2_out, sig_out, cor_out,
                 w0, w1, w1x, w2, x0, x1, x2, y0, y1, tt, e2_t, h2_own, h2_put, h2_got, e1, e1_t, e0, e0_t, h0_put,
                 p_buf, p_sum, n_buf, c_buf,
                 eye, load_sem, put_sem, w_send, w_recv, w1x_send, w1x_recv, fwd_send, fwd_recv, small_send, small_recv,
                 x1_send, x1_recv, x2_send, x2_recv, h2_send, h2_recv, e1_send, e1_recv, h0_send, h0_recv, out_send, out_recv, sum_sem, both_sem, both_send, both_recv):
    me = lax.axis_index("model")
    chip = me // 2
    core = me % 2
    other = 1 - chip
    mate = me + 1 - 2 * core
    far = me + 2 - 4 * chip
    diag = mate + 2 - 4 * chip
    n_rows, n0 = x0.shape
    wide1 = w0.shape[0]
    rows1 = wide1 // 2
    wide2 = w2.shape[0]
    rows2 = wide2 // 2
    n1 = 2 * wide1
    step = n_rows // CHUNKS
    piece = rows2 // PIECES

    def send(src, dst, send_sem, recv_sem, device):
        return pltpu.make_async_remote_copy(src_ref=src, dst_ref=dst, send_sem=send_sem, recv_sem=recv_sem, device_id={"model": device}, device_id_type=MESH)

    def part(index, size):
        return pl.ds(pl.multiple_of(index * size, size), size)

    barrier = pltpu.get_barrier_semaphore()
    for device in (mate, far, diag):
        pl.semaphore_signal(barrier, inc=1, device_id={"model": device}, device_id_type=MESH)
    pl.semaphore_wait(barrier, 3)

    def w1x_copy(piece_no):
        return send(
            w1_in.at[pl.ds(piece_no * piece, piece), part(other, wide1)],
            w1x.at[pl.ds(pl.multiple_of(core * rows2 + piece_no * piece, piece), piece), :],
            w1x_send.at[piece_no], w1x_recv.at[piece_no], far)

    def w1x_forward(piece_no):
        rows = w1x.at[pl.ds(pl.multiple_of(core * rows2 + piece_no * piece, piece), piece), :]
        return send(rows, rows, fwd_send.at[piece_no], fwd_recv.at[piece_no], mate)

    own1, own2 = part(core, rows1), part(core, rows2)
    loads = [
        pltpu.make_async_copy(w0_in, w0.at[own1, :], load_sem.at[0]),
        pltpu.make_async_copy(w1_in, w1.at[own2, :], load_sem.at[1]),
        pltpu.make_async_copy(w2_in, w2.at[own2, :], load_sem.at[2]),
    ]
    gives = [
        send(w0.at[own1, :], w0.at[own1, :], w_send.at[0], w_recv.at[0], mate),
        send(w1.at[own2, :], w1.at[own2, :], w_send.at[1], w_recv.at[1], mate),
        send(w2.at[own2, :], w2.at[own2, :], w_send.at[2], w_recv.at[2], mate),
    ]
    w1x_copy(0).start()
    for copy in loads:
        copy.start()

    w1x_copy(1).start()

    def mine(x_in, t_own):
        return (
            pltpu.make_async_copy(x_in, x0, load_sem.at[3]),
            pltpu.make_async_copy(t_own, tt.at[own2, :], load_sem.at[4]),
        )

    @pl.when(core == 0)
    def _():
        for copy in mine(x_real, t_real):
            copy.start()

    @pl.when(core == 1)
    def _():
        for copy in mine(x_fake, t_fake):
            copy.start()

    def row(values):
        return jnp.broadcast_to(values.reshape(1, values.size).astype(BF16), (16, values.size))

    lanes = lax.broadcasted_iota(jnp.int32, eye.shape, 1)
    eye[...] = jnp.where(lanes == lax.broadcasted_iota(jnp.int32, eye.shape, 0), 1.0, 0.0).astype(BF16)

    def store_transposed(dst, first, rows, values):
        for begin in range(0, values.shape[1], eye.shape[0]):
            size = min(eye.shape[0], values.shape[1] - begin)
            block = dot_t(eye[0:size, 0:size], values[:, begin:begin + size])
            dst[pl.ds(pl.multiple_of(first + begin, 128), size), rows] = block.astype(BF16)

    u_rows = [row(u0_in[...]), row(u1_in[...]), row(u2_in[...])]
    loads[0].wait()
    p_buf[me, :, pl.ds(0, n0)] = dot_n(u_rows[0], w0[own1, :])[0:1]
    loads[1].wait()

    def p1_tile(tile_no, carry):
        cols = part(tile_no, wide1 // 2)
        p_buf[me, :, pl.ds(pl.multiple_of(n0 + tile_no * (wide1 // 2), 128), wide1 // 2)] = dot_n(u_rows[1], w1[own2, cols])[0:1]
        return carry

    lax.fori_loop(0, 4, p1_tile, 0)
    loads[2].wait()
    p_buf[me, :, pl.ds(n0 + n1, wide2 * 2)] = dot_n(u_rows[2], w2[own2, :])[0:1]

    def spread(buf, first):
        return [send(buf.at[me], buf.at[me], small_send.at[first + which], small_recv.at[first + which], device) for which, device in enumerate((mate, far, diag))]

    p_near = send(p_buf.at[me], p_buf.at[me], small_send.at[0], small_recv.at[0], mate)
    p_near.start()
    gives[0].start()
    p_near.wait()
    p_sum[chip] = p_buf[2 * chip] + p_buf[2 * chip + 1]
    p_far = send(p_sum.at[chip], p_sum.at[chip], small_send.at[1], small_recv.at[1], far)
    p_far.start()
    w1x_copy(2).start()
    w1x_copy(3).start()

    pltpu.make_async_copy(x_real, x0, load_sem.at[3]).wait()
    gives[0].wait_recv()

    def y0_tile(tile_no, carry):
        cols = part(tile_no, TILE)
        y0[:, cols] = dot_t(x0[...], w0[cols, :])
        return carry

    lax.fori_loop(0, wide1 // TILE, y0_tile, 0)
    p_far.wait()
    p_all = p_sum[0] + p_sum[1]
    spans = ((0, n0, v0_out), (n0, n1, v1_out), (n0 + n1, 2 * wide2, v2_out))
    for first, size, v_out in spans:
        p_vec = p_all[:, first:first + size]
        v_out[...] = p_vec / jnp.maximum(jnp.sqrt(total(p_vec * p_vec)), EPSILON)
    u0_out[...] = dot_t(row(v0_out[...]), w0[own1, :])[0:1]
    u1_out[...] = dot_t(row(v1_out[...]), w1[own2, :])[0:1]
    u2_out[...] = dot_t(row(v2_out[...]), w2[own2, :])[0:1]
    lane = lax.broadcasted_iota(jnp.int32, (8, 128), 1)

    def pack(values):
        packed = jnp.zeros((8, 128), F32)
        for place, value in enumerate(values):
            packed = jnp.where(lane == place, value, packed)
        return packed

    n_buf[me] = pack([total(u_out[...] * u_out[...]) for u_out in (u0_out, u1_out, u2_out)])
    n_copies = spread(n_buf, 3)
    for copy in n_copies:
        copy.start()
    for piece_no in range(4, PIECES):
        w1x_copy(piece_no).start()
    for copy in gives[1:]:
        copy.start()

    @pl.when(core == 0)
    def _():
        send(t_fake, tt.at[own2, :], w_send.at[3], w_recv.at[3], mate).start()

    @pl.when(core == 1)
    def _():
        send(t_real, tt.at[own2, :], w_send.at[3], w_recv.at[3], mate).start()

    for copy in n_copies:
        copy.wait()
    sigmas = jnp.sqrt(n_buf[0] + n_buf[1] + n_buf[2] + n_buf[3])
    sig_out[...] = sigmas
    sig0, sig1, sig2 = sigmas[0:1, 0:1], sigmas[0:1, 1:2], sigmas[0:1, 2:3]
    inv0, inv1, inv2 = 1.0 / sig0, 1.0 / sig1, 1.0 / sig2
    u0_out[...] = u0_out[...] / sig0
    u1_out[...] = u1_out[...] / sig1
    u2_out[...] = u2_out[...] / sig2

    def chunk_copy(buf, slot, chunk_no, send_sem, recv_sem):
        rows = buf.at[slot, part(chunk_no, step), :]
        return send(rows, rows, send_sem.at[chunk_no], recv_sem.at[chunk_no], far)

    def layer0(chunk_no, carry):
        rows = part(chunk_no, step)
        x1[chip, rows, :] = leaky_relu(y0[rows, :] * inv0).astype(BF16)
        chunk_copy(x1, chip, chunk_no, x1_send, x1_recv).start()
        return carry

    lax.fori_loop(0, CHUNKS, layer0, 0)

    batch = part(core, n_rows)

    def outputs(src, dst, which):
        return (
            pltpu.make_async_copy(src, dst, put_sem.at[which]),
            send(src, dst, out_send.at[which], out_recv.at[which], mate),
        )

    def halves(src, dst, size, which):
        return (
            pltpu.make_async_copy(src.at[part(core, size), :], dst.at[:, batch], put_sem.at[which]),
            send(src.at[part(1 - core, size), :], dst.at[:, batch], out_send.at[which], out_recv.at[which], mate),
        )

    x1_near = outputs(x1.at[chip], x1_out.at[batch, part(chip, wide1)], 0)
    for copy in x1_near:
        copy.start()
    for piece_no in range(PIECES):
        w1x_copy(piece_no).wait_recv()
        w1x_forward(piece_no).start()

    gives[1].wait_recv()

    def layer1(chunk_no, carry):
        rows = part(chunk_no, step)
        chunk_copy(x1, other, chunk_no, x1_send, x1_recv).wait_recv()
        y_val = (dot_t(x1[0, rows, :], w1[:, pl.ds(0, wide1)]) + dot_t(x1[1, rows, :], w1[:, pl.ds(wide1, wide1)])) * inv1
        y1[rows, :] = y_val
        x2[chip, rows, :] = leaky_relu(y_val).astype(BF16)
        chunk_copy(x2, chip, chunk_no, x2_send, x2_recv).start()
        return carry

    lax.fori_loop(0, CHUNKS, layer1, 0)
    x1_far = outputs(x1.at[other], x1_out.at[batch, part(other, wide1)], 1)
    for copy in x1_far:
        copy.start()

    gives[2].wait_recv()
    pltpu.make_async_copy(t_real, tt.at[own2, :], load_sem.at[4]).wait()
    t_give = send(t_real, tt.at[own2, :], w_send.at[3], w_recv.at[3], mate)
    t_give.wait_recv()

    def layer2(chunk_no, carry):
        corr2, loss = carry
        rows = part(chunk_no, step)
        chunk_copy(x2, other, chunk_no, x2_send, x2_recv).wait_recv()
        y_val = (dot_t(x2[0, rows, :], w2[:, pl.ds(0, wide2)]) + dot_t(x2[1, rows, :], w2[:, pl.ds(wide2, wide2)])) * inv2
        e_val = y_val - dot_t(eye[0:step, 0:step], tt[:, rows])
        corr2 = corr2 + fold(e_val * y_val)
        loss = loss + fold(e_val * e_val)
        e_half = e_val.astype(BF16)
        h2_put[rows, :] = dot_n(e_half, w2[:, part(other, wide2)]).astype(BF16)
        send(h2_put.at[rows, :], h2_got.at[rows, :], h2_send.at[chunk_no], h2_recv.at[chunk_no], far).start()
        h2_own[rows, :] = dot_n(e_half, w2[:, part(chip, wide2)])
        store_transposed(e2_t, 0, rows, e_half)
        return corr2, loss

    zero = jnp.zeros((8, wide2), F32)
    corr2, loss = lax.fori_loop(0, CHUNKS, layer2, (zero, zero))

    def back1(chunk_no, corr1):
        rows = part(chunk_no, step)
        send(h2_put.at[rows, :], h2_got.at[rows, :], h2_send.at[chunk_no], h2_recv.at[chunk_no], far).wait_recv()
        y_val = y1[rows, :]
        e_val = (h2_own[rows, :] + h2_got[rows, :].astype(F32)) * (inv2 * leaky_slope(y_val))
        e_half = e_val.astype(BF16)
        e1[chip, rows, :] = e_half
        chunk_copy(e1, chip, chunk_no, e1_send, e1_recv).start()
        store_transposed(e1_t, 0, rows, e_half)
        return corr1 + fold(e_val * y_val)

    corr1 = lax.fori_loop(0, CHUNKS, back1, zero)
    lesser = [
        outputs(x2.at[0], x2_out.at[batch, pl.ds(0, wide2)], 2),
        outputs(x2.at[1], x2_out.at[batch, pl.ds(wide2, wide2)], 3),
        halves(e2_t, e2_out, rows2, 4),
        halves(e1_t, e1_out, rows2, 5),
    ]
    for pair in lesser:
        for copy in pair:
            copy.start()
    for piece_no in range(PIECES):
        w1x_forward(piece_no).wait_recv()

    def h0_copy(chunk_no):
        rows = part(chunk_no, step)
        return send(h0_put.at[rows, :], got_out.at[rows, :], h0_send.at[chunk_no], h0_recv.at[chunk_no], far)

    def both_copies(chunk_no):
        src = h0_put.at[part(chunk_no, step), :]
        dst = both_out.at[pl.ds(pl.multiple_of(core * n_rows + chunk_no * step, step), step), :]
        return (
            pltpu.make_async_copy(src, dst, both_sem.at[chunk_no]),
            send(src, dst, both_send.at[chunk_no], both_recv.at[chunk_no], mate),
        )

    def late_copy(sum_out, start, chunk_no):
        dst = sum_out.at[part(chunk_no - start, step), :]
        return pltpu.make_async_copy(h0_put.at[part(chunk_no, step), :], dst, sum_sem.at[chunk_no])

    def back0(chunk_no, corr0):
        rows = part(chunk_no, step)
        chunk_copy(e1, other, chunk_no, e1_send, e1_recv).wait_recv()

        def h1_tile(tile_no, corr):
            cols = part(tile_no, wide2)
            own_cols = pl.ds(pl.multiple_of(chip * wide1 + tile_no * wide2, 128), wide2)
            h_val = dot_n(e1[chip, rows, :], w1[:, own_cols]) + dot_n(e1[other, rows, :], w1x[:, cols])
            y_val = y0[rows, cols]
            e_val = h_val * (inv1 * leaky_slope(y_val))
            e0[:, cols] = e_val.astype(BF16)
            return corr + fold(e_val * y_val)

        corr0 = lax.fori_loop(0, wide1 // wide2, h1_tile, corr0)
        h0_put[rows, :] = dot_n(e0[...], w0[...]).astype(BF16)
        return corr0

    def transpose0(chunk_no):
        rows = part(chunk_no, step)

        def tile(tile_no, carry):
            store_transposed(e0_t, tile_no * wide2, rows, e0[:, part(tile_no, wide2)])
            return carry

        lax.fori_loop(0, wide1 // wide2, tile, 0)

    def early_chunk(chunk_no, corr0):
        corr0 = back0(chunk_no, corr0)
        for copy in (h0_copy(chunk_no), *both_copies(chunk_no)):
            copy.start()
        transpose0(chunk_no)
        return corr0

    def late_chunk(sum_out, start, chunk_no, corr0):
        corr0 = back0(chunk_no, corr0)
        for copy in (late_copy(sum_out, start, chunk_no), *both_copies(chunk_no)):
            copy.start()
        transpose0(chunk_no)
        return corr0

    corr0 = jnp.zeros((8, wide2), F32)
    corr0 = lax.fori_loop(0, EARLY, early_chunk, corr0)
    corr0 = lax.fori_loop(EARLY, EARLY + MIDDLE, functools.partial(late_chunk, mid_out, EARLY), corr0)
    corr0 = lax.fori_loop(EARLY + MIDDLE, CHUNKS, functools.partial(late_chunk, last_out, EARLY + MIDDLE), corr0)
    e0_pair = halves(e0_t, e0_out, rows1, 6)
    for copy in e0_pair:
        copy.start()
    c_buf[me] = pack([total(corr0) * inv0, total(corr1), total(corr2), total(loss)])
    c_copies = spread(c_buf, 6)
    for copy in c_copies:
        copy.start()

    for copy in c_copies:
        copy.wait()
    cor_out[...] = c_buf[0] + c_buf[1] + c_buf[2] + c_buf[3]

    for copy in gives:
        copy.wait_send()
    t_give.wait_send()
    for piece_no in range(PIECES):
        w1x_copy(piece_no).wait_send()
        w1x_forward(piece_no).wait_send()
    for pair in (x1_near, x1_far, *lesser, e0_pair):
        for copy in pair:
            copy.wait()

    def drain(chunk_no, carry):
        rows = part(chunk_no, step)
        chunk_copy(x1, chip, chunk_no, x1_send, x1_recv).wait_send()
        chunk_copy(x2, chip, chunk_no, x2_send, x2_recv).wait_send()
        send(h2_put.at[rows, :], h2_got.at[rows, :], h2_send.at[chunk_no], h2_recv.at[chunk_no], far).wait_send()
        chunk_copy(e1, chip, chunk_no, e1_send, e1_recv).wait_send()
        return carry

    lax.fori_loop(0, CHUNKS, drain, 0)

    for chunk_no in range(CHUNKS):
        if chunk_no < EARLY:
            h0_copy(chunk_no).wait()
        elif chunk_no < EARLY + MIDDLE:
            late_copy(mid_out, EARLY, chunk_no).wait()
        else:
            late_copy(last_out, EARLY + MIDDLE, chunk_no).wait()
        for copy in both_copies(chunk_no):
            copy.wait()


def run_chain(x_real, x_fake, weight0, weight1, weight2, u_left0, u_left1, u_left2, t_real, t_fake):
    n_rows, n0 = x_real.shape
    rows1 = weight0.shape[0]
    rows2, n1 = weight1.shape
    wide1, wide2 = 2 * rows1, 2 * rows2
    n2 = 2 * wide2
    step = n_rows // CHUNKS
    early, middle = EARLY * step, MIDDLE * step
    last = n_rows - early - middle
    hbm = pl.BlockSpec(memory_space=pl.ANY)
    vmem = pl.BlockSpec(memory_space=pltpu.VMEM)
    shape = jax.ShapeDtypeStruct
    dma = pltpu.SemaphoreType.DMA
    return pl.pallas_call(
        chain_kernel,
        out_shape=(
            shape((2 * n_rows, n1), BF16), shape((2 * n_rows, n2), BF16), shape((rows2, 2 * n_rows), BF16), shape((rows2, 2 * n_rows), BF16),
            shape((rows1, 2 * n_rows), BF16), shape((early, n0), BF16), shape((middle, n0), BF16), shape((last, n0), BF16), shape((2 * n_rows, n0), BF16),
            shape((1, n0), F32), shape((1, n1), F32), shape((1, n2), F32),
            shape((1, rows1), F32), shape((1, rows2), F32), shape((1, rows2), F32),
            shape((8, 128), F32), shape((8, 128), F32),
        ),
        in_specs=[hbm] * 5 + [vmem] * 3 + [hbm] * 2,
        out_specs=[hbm] * 9 + [vmem] * 8,
        scratch_shapes=[
            pltpu.VMEM((wide1, n0), BF16), pltpu.VMEM((wide2, n1), BF16), pltpu.VMEM((wide2, wide1), BF16), pltpu.VMEM((wide2, n2), BF16),
            pltpu.VMEM((n_rows, n0), BF16), pltpu.VMEM((2, n_rows, wide1), BF16), pltpu.VMEM((2, n_rows, wide2), BF16),
            pltpu.VMEM((n_rows, wide1), F32), pltpu.VMEM((n_rows, wide2), F32), pltpu.VMEM((wide2, n_rows), BF16),
            pltpu.VMEM((wide2, n_rows), BF16), pltpu.VMEM((n_rows, wide2), F32), pltpu.VMEM((n_rows, wide2), BF16), pltpu.VMEM((n_rows, wide2), BF16),
            pltpu.VMEM((2, n_rows, wide2), BF16), pltpu.VMEM((wide2, n_rows), BF16), pltpu.VMEM((n_rows // CHUNKS, wide1), BF16), pltpu.VMEM((wide1, n_rows), BF16),
            pltpu.VMEM((n_rows, n0), BF16),
            pltpu.VMEM((4, 1, n0 + n1 + n2), F32), pltpu.VMEM((2, 1, n0 + n1 + n2), F32), pltpu.VMEM((4, 8, 128), F32), pltpu.VMEM((4, 8, 128), F32), pltpu.VMEM((256, 256), BF16),
            dma((5,)), dma((7,)), dma((4,)), dma((4,)), dma((PIECES,)), dma((PIECES,)), dma((PIECES,)), dma((PIECES,)), dma((9,)), dma((9,)),
            dma((CHUNKS,)), dma((CHUNKS,)), dma((CHUNKS,)), dma((CHUNKS,)), dma((CHUNKS,)), dma((CHUNKS,)),
            dma((CHUNKS,)), dma((CHUNKS,)), dma((EARLY,)), dma((EARLY,)), dma((7,)), dma((7,)),
            dma((CHUNKS,)), dma((CHUNKS,)), dma((CHUNKS,)), dma((CHUNKS,)),
        ],
        compiler_params=pltpu.CompilerParams(collective_id=0, has_side_effects=True, vmem_limit_bytes=67043328),
        name="chain",
    )(x_real, x_fake, weight0, weight1, weight2, u_left0, u_left1, u_left2, t_real.T, t_fake.T)


def grad_kernel(x1_in, e1_in, x2_in, e2_in, x_real, x_fake, e0_in, u0_in, u1_in, u2_in, v0_in, v1_in, v2_in, sig_in, cor_in,
                dw0_out, dw1_out, dw2_out, u0_out, u1_out, u2_out, v0_out, v1_out, v2_out, sig_out, loss_out,
                x1, e1, x2, e2, x0, e0, dw0, dw1, dw2, u0, u1, u2, v0, v1, v2, sig, cor, in_sem, x1_sem, out_sem, dw1_sem, dw0_sem):
    n_rows = x_real.shape[0]
    tiles1 = x1_sem.shape[0]
    tiles0 = dw0_sem.shape[0]

    def pull(src, dst, which):
        copy = pltpu.make_async_copy(src, dst, in_sem.at[which])
        copy.start()
        return copy

    small = [pull(src, dst, place) for place, (src, dst) in enumerate((
        (u0_in, u0), (u1_in, u1), (u2_in, u2), (v0_in, v0), (v1_in, v1), (v2_in, v2), (sig_in, sig), (cor_in, cor)))]

    def tile_of(size, tiles, tile_no):
        return pl.ds(tile_no * (size // tiles), size // tiles)

    def load(src, dst, which):
        return pltpu.make_async_copy(src, dst, in_sem.at[which])

    got_e1 = pull(e1_in, e1, 11)
    got_x1 = []
    for tile_no in range(tiles1):
        cols = tile_of(x1.shape[1], tiles1, tile_no)
        got_x1.append(pltpu.make_async_copy(x1_in.at[:, cols], x1.at[:, cols], x1_sem.at[tile_no]))
    got_e0 = load(e0_in, e0, 8)
    got_x0 = [load(x_real, x0.at[pl.ds(0, n_rows), :], 9), load(x_fake, x0.at[pl.ds(n_rows, n_rows), :], 10)]
    got_2 = [load(e2_in, e2, 13), load(x2_in, x2, 14)]
    queue = [*got_x1, *got_x0, got_e0, *got_2]

    def read_on(count=1):
        for _ in range(min(count, len(queue))):
            queue.pop(0).start()

    read_on(3)

    for copy in small:
        copy.wait()
    for src, dst in ((u0, u0_out), (u1, u1_out), (u2, u2_out), (v0, v0_out), (v1, v1_out), (v2, v2_out)):
        dst[...] = src[...].reshape(dst.shape)
    sig_out[...] = sig[0:1, 0:3].reshape(3)
    loss_out[...] = cor[0:1, 3:4] * (0.5 / n_rows)

    def column(u_new, layer_no):
        return jnp.broadcast_to(u_new[...] * cor[0:1, layer_no:layer_no + 1], (128, u_new.shape[1])).T[:, 0:1]

    def scale(layer_no):
        return 1.0 / (n_rows * sig[0:1, layer_no:layer_no + 1])

    pushes = []

    def gradient(errors, layer_in, cols, col, v_new, rate, dst, out, sem):
        dst[:, cols] = (dot_n(errors[...], layer_in[:, cols]) - col * v_new[:, cols]) * rate
        copy = pltpu.make_async_copy(dst.at[:, cols], out.at[:, cols], sem)
        copy.start()
        pushes.append(copy)

    got_e1.wait()
    col1, scale1 = column(u1, 1), scale(1)
    for tile_no in range(tiles1):
        got_x1[tile_no].wait()
        read_on()
        gradient(e1, x1, tile_of(x1.shape[1], tiles1, tile_no), col1, v1, scale1, dw1, dw1_out, dw1_sem.at[tile_no])
    got_e0.wait()
    read_on(3)
    for copy in got_x0:
        copy.wait()
    col0, scale0 = column(u0, 0), scale(0)
    for tile_no in range(tiles0):
        gradient(e0, x0, tile_of(x0.shape[1], tiles0, tile_no), col0, v0, scale0, dw0, dw0_out, dw0_sem.at[tile_no])
    for copy in got_2:
        copy.wait()
    col2, scale2 = column(u2, 2), scale(2)
    for tile_no in range(2):
        gradient(e2, x2, tile_of(x2.shape[1], 2, tile_no), col2, v2, scale2, dw2, dw2_out, out_sem.at[2 + tile_no])
    for copy in pushes:
        copy.wait()


def run_grads(x1, e1, x2, e2, x_real, x_fake, e0, u0, u1, u2, v0, v1, v2, sig, cor):
    both, n1 = x1.shape
    _, n0 = x_real.shape
    n2 = x2.shape[1]
    rows2 = e1.shape[0]
    rows1 = e0.shape[0]
    tiles1, tiles0 = 10, 5
    shape = jax.ShapeDtypeStruct
    hbm = pl.BlockSpec(memory_space=pltpu.HBM)
    vmem = pl.BlockSpec(memory_space=pltpu.VMEM)
    dma = pltpu.SemaphoreType.DMA
    flops = 2 * both * (rows2 * (n1 + n2) + rows1 * n0)
    inputs = (x1, e1, x2, e2, x_real, x_fake, e0, u0, u1, u2, v0, v1, v2, sig, cor)
    inputs = tuple(pltpu.with_memory_space_constraint(array, pltpu.HBM) for array in inputs)
    return pl.pallas_call(
        grad_kernel,
        out_shape=(
            shape((rows1, n0), F32), shape((rows2, n1), F32), shape((rows2, n2), F32),
            shape((rows1,), F32), shape((rows2,), F32), shape((rows2,), F32), shape((n0,), F32), shape((n1,), F32), shape((n2,), F32),
            shape((3,), F32), shape((1, 1), F32),
        ),
        in_specs=[hbm] * len(inputs),
        out_specs=[hbm] * 3 + [vmem] * 8,
        scratch_shapes=[
            pltpu.VMEM((both, n1), BF16), pltpu.VMEM((rows2, both), BF16), pltpu.VMEM((both, n2), BF16), pltpu.VMEM((rows2, both), BF16),
            pltpu.VMEM((both, n0), BF16), pltpu.VMEM((rows1, both), BF16),
            pltpu.VMEM((rows1, n0), F32), pltpu.VMEM((rows2, n1), F32), pltpu.VMEM((rows2, n2), F32),
            *[pltpu.VMEM(array.shape, F32) for array in (u0, u1, u2, v0, v1, v2, sig, cor)],
            dma((15,)), dma((tiles1,)), dma((4,)), dma((tiles1,)), dma((tiles0,)),
        ],
        compiler_params=pltpu.CompilerParams(vmem_limit_bytes=48 * 1024 * 1024),
        cost_estimate=pl.CostEstimate(flops=flops, bytes_accessed=45 * 1024 * 1024, transcendentals=0),
        name="grads",
    )(*inputs)


def finish_kernel(plan, in_place, *refs):
    refs = refs[2:] if in_place else refs
    both, sig = refs[:2]
    cames = refs[2:2 + len(plan)]
    real_out, fake_out, dx, out_sem = refs[2 + len(plan):]
    core = lax.axis_index("model") % 2
    n_rows = real_out.shape[0]
    inv0 = 1.0 / sig[0:1, 0:1]
    size = dx.shape[0] // out_sem.shape[0]
    jobs = []
    for came, (flip, first) in zip(cames, plan):
        batch = 1 - core if flip else core
        for begin in range(0, came.shape[0], size):
            jobs.append((came, begin, batch, first + begin))

    def push(dst, place, first):
        return pltpu.make_async_copy(dx.at[pl.ds(place * size, size), :], dst.at[pl.ds(first, size), :], out_sem.at[place])

    for place, (came, begin, batch, first) in enumerate(jobs):
        own = pl.ds(pl.multiple_of(batch * n_rows + first, size), size)
        dx[pl.ds(place * size, size), :] = (both[own, :].astype(F32) + came[pl.ds(begin, size), :].astype(F32)) * inv0

        @pl.when(batch == 0)
        def _():
            push(real_out, place, first).start()

        @pl.when(batch == 1)
        def _():
            push(fake_out, place, first).start()

    for place, (_, _, _, first) in enumerate(jobs):
        push(real_out, place, first).wait()


def run_finish(old, both, sig, parts):
    cames = [came for came, _, _ in parts]
    rows = sum(came.shape[0] for came in cames)
    n0 = both.shape[1]
    size = 64
    hbm = pl.BlockSpec(memory_space=pltpu.HBM)
    vmem = pl.BlockSpec(memory_space=pltpu.VMEM)
    shape = jax.ShapeDtypeStruct((both.shape[0] // 2, n0), F32)
    return pl.pallas_call(
        functools.partial(finish_kernel, tuple((flip, first) for _, flip, first in parts), bool(old)),
        out_shape=(shape, shape),
        in_specs=[hbm] * len(old) + [vmem] * (2 + len(cames)),
        out_specs=[hbm] * 2,
        scratch_shapes=[pltpu.VMEM((rows, n0), F32), pltpu.SemaphoreType.DMA((rows // size,))],
        input_output_aliases={0: 0, 1: 1} if old else {},
        compiler_params=pltpu.CompilerParams(vmem_limit_bytes=16 * 1024 * 1024),
        cost_estimate=pl.CostEstimate(flops=4 * rows * n0, bytes_accessed=8 * rows * n0, transcendentals=0),
        name="finish",
    )(*old, both, sig, *cames)


def swap(values, bits):
    return lax.ppermute(values, "model", [(dev, dev ^ bits) for dev in range(4)])


def solution(mesh):
    rows_spec = P("rep", None)
    weight_spec = P(("rep", "model"), None)
    left_spec = P(("rep", "model"))
    target_spec = P("rep", "model")
    group_spec = P("rep")

    def local_step(x_real, x_fake, weight0, weight1, weight2, u_left0, u_left1, u_left2, t_real, t_fake):
        x1, x2, e2, e1, e0, first, middle, last, both, v0, v1, v2, u0, u1, u2, sig, cor = run_chain(x_real, x_fake, weight0, weight1, weight2, u_left0, u_left1, u_left2, t_real, t_fake)
        row1 = first.shape[0]
        row2 = row1 + middle.shape[0]
        middle = swap(middle, 2)
        last = swap(last, 2)
        first_mate = swap(first, 1)
        grads = run_grads(x1, e1, x2, e2, x_real, x_fake, e0, u0, u1, u2, v0, v1, v2, sig, cor)
        dw0, dw1, dw2, u0, u1, u2, v0, v1, v2, sigmas, loss = grads
        middle, sigmas = lax.optimization_barrier((middle, sigmas))
        middle_mate = swap(middle, 1)
        dx = run_finish((), both, sig, ((first, False, 0), (first_mate, True, 0), (middle, False, row1)))
        dx = run_finish(dx, both, sig, ((middle_mate, True, row1),))
        last, *dx = lax.optimization_barrier((last, *dx))
        last_mate = swap(last, 1)
        dx = run_finish(dx, both, sig, ((last, False, row2),))
        dx_real, dx_fake = run_finish(dx, both, sig, ((last_mate, True, row2),))
        return (loss[0], dx_real, dx_fake, dw0, dw1, dw2, u0, u1, u2, v0, v1, v2, sigmas)

    return jax.shard_map(local_step, mesh=mesh, in_specs=(rows_spec, rows_spec, weight_spec, weight_spec, weight_spec, left_spec, left_spec, left_spec, target_spec, target_spec), out_specs=(group_spec, rows_spec, rows_spec, weight_spec, weight_spec, weight_spec, left_spec, left_spec, left_spec, group_spec, group_spec, group_spec, group_spec), check_vma=False)
```

```python
import functools

import jax
import jax.numpy as jnp
from jax import lax
from jax.experimental import pallas as pl
from jax.experimental.pallas import tpu as pltpu
from jax.sharding import PartitionSpec as P


SLOPE = 0.2
EPSILON = 1e-12
MESH = pl.DeviceIdType.MESH
CHUNKS = 4
EARLY = 1
MIDDLE = 2
PIECES = 5
TILE = 256
BF16 = jnp.bfloat16
F32 = jnp.float32


def leaky_relu(values):
    return jnp.where(values > 0, values, SLOPE * values)


def leaky_slope(values):
    return jnp.where(values > 0, 1.0, SLOPE)


def dot_t(left, right):
    return lax.dot_general(left, right, (((1,), (1,)), ((), ())), preferred_element_type=F32)


def dot_n(left, right):
    return lax.dot_general(left, right, (((1,), (0,)), ((), ())), preferred_element_type=F32)


def fold(values):
    rows, cols = values.shape
    return jnp.sum(values.reshape(rows // 8, 8, cols), axis=0)


def total(values):
    return jnp.sum(jnp.sum(values, axis=1, keepdims=True), axis=0, keepdims=True)


def chain_kernel(x_real, x_fake, w0_in, w1_in, w2_in, u0_in, u1_in, u2_in, t_real, t_fake,
                 x1_out, x2_out, e2_out, e1_out, e0_out, got_out, mid_out, last_out, both_out, v0_out, v1_out, v2_out, u0_out, u1_out, u2_out, sig_out, cor_out,
                 w0, w1, w1x, w2, x0, x1, x2, y0, y1, tt, e2_t, h2_own, h2_put, h2_got, e1, e1_t, e0, e0_t, h0_put,
                 p_buf, p_sum, n_buf, c_buf,
                 eye, load_sem, put_sem, w_send, w_recv, w1x_send, w1x_recv, fwd_send, fwd_recv, small_send, small_recv,
                 x1_send, x1_recv, x2_send, x2_recv, h2_send, h2_recv, e1_send, e1_recv, h0_send, h0_recv, out_send, out_recv, sum_sem, both_sem, both_send, both_recv, e0_sem, e0_send, e0_recv):
    me = lax.axis_index("model")
    chip = me // 2
    core = me % 2
    other = 1 - chip
    mate = me + 1 - 2 * core
    far = me + 2 - 4 * chip
    diag = mate + 2 - 4 * chip
    n_rows, n0 = x0.shape
    wide1 = w0.shape[0]
    rows1 = wide1 // 2
    wide2 = w2.shape[0]
    rows2 = wide2 // 2
    n1 = 2 * wide1
    step = n_rows // CHUNKS
    piece = rows2 // PIECES

    def send(src, dst, send_sem, recv_sem, device):
        return pltpu.make_async_remote_copy(src_ref=src, dst_ref=dst, send_sem=send_sem, recv_sem=recv_sem, device_id={"model": device}, device_id_type=MESH)

    def part(index, size):
        return pl.ds(pl.multiple_of(index * size, size), size)

    barrier = pltpu.get_barrier_semaphore()
    for device in (mate, far, diag):
        pl.semaphore_signal(barrier, inc=1, device_id={"model": device}, device_id_type=MESH)
    pl.semaphore_wait(barrier, 3)

    def w1x_copy(piece_no):
        return send(
            w1_in.at[pl.ds(piece_no * piece, piece), part(other, wide1)],
            w1x.at[pl.ds(pl.multiple_of(core * rows2 + piece_no * piece, piece), piece), :],
            w1x_send.at[piece_no], w1x_recv.at[piece_no], far)

    def w1x_forward(piece_no):
        rows = w1x.at[pl.ds(pl.multiple_of(core * rows2 + piece_no * piece, piece), piece), :]
        return send(rows, rows, fwd_send.at[piece_no], fwd_recv.at[piece_no], mate)

    own1, own2 = part(core, rows1), part(core, rows2)
    loads = [
        pltpu.make_async_copy(w0_in, w0.at[own1, :], load_sem.at[0]),
        pltpu.make_async_copy(w1_in, w1.at[own2, :], load_sem.at[1]),
        pltpu.make_async_copy(w2_in, w2.at[own2, :], load_sem.at[2]),
    ]
    gives = [
        send(w0.at[own1, :], w0.at[own1, :], w_send.at[0], w_recv.at[0], mate),
        send(w1.at[own2, :], w1.at[own2, :], w_send.at[1], w_recv.at[1], mate),
        send(w2.at[own2, :], w2.at[own2, :], w_send.at[2], w_recv.at[2], mate),
    ]
    w1x_copy(0).start()
    for copy in loads:
        copy.start()

    w1x_copy(1).start()

    def mine(x_in, t_own):
        return (
            pltpu.make_async_copy(x_in, x0, load_sem.at[3]),
            pltpu.make_async_copy(t_own, tt.at[own2, :], load_sem.at[4]),
        )

    @pl.when(core == 0)
    def _():
        for copy in mine(x_real, t_real):
            copy.start()

    @pl.when(core == 1)
    def _():
        for copy in mine(x_fake, t_fake):
            copy.start()

    def row(values):
        return jnp.broadcast_to(values.reshape(1, values.size).astype(BF16), (16, values.size))

    lanes = lax.broadcasted_iota(jnp.int32, eye.shape, 1)
    eye[...] = jnp.where(lanes == lax.broadcasted_iota(jnp.int32, eye.shape, 0), 1.0, 0.0).astype(BF16)

    def store_transposed(dst, first, rows, values):
        for begin in range(0, values.shape[1], eye.shape[0]):
            size = min(eye.shape[0], values.shape[1] - begin)
            block = dot_t(eye[0:size, 0:size], values[:, begin:begin + size])
            dst[pl.ds(pl.multiple_of(first + begin, 128), size), rows] = block.astype(BF16)

    u_rows = [row(u0_in[...]), row(u1_in[...]), row(u2_in[...])]
    loads[0].wait()
    p_buf[me, :, pl.ds(0, n0)] = dot_n(u_rows[0], w0[own1, :])[0:1]
    loads[1].wait()

    def p1_tile(tile_no, carry):
        cols = part(tile_no, wide1 // 2)
        p_buf[me, :, pl.ds(pl.multiple_of(n0 + tile_no * (wide1 // 2), 128), wide1 // 2)] = dot_n(u_rows[1], w1[own2, cols])[0:1]
        return carry

    lax.fori_loop(0, 4, p1_tile, 0)
    loads[2].wait()
    p_buf[me, :, pl.ds(n0 + n1, wide2 * 2)] = dot_n(u_rows[2], w2[own2, :])[0:1]

    def spread(buf, first):
        return [send(buf.at[me], buf.at[me], small_send.at[first + which], small_recv.at[first + which], device) for which, device in enumerate((mate, far, diag))]

    p_near = send(p_buf.at[me], p_buf.at[me], small_send.at[0], small_recv.at[0], mate)
    p_near.start()
    gives[0].start()
    p_near.wait()
    p_sum[chip] = p_buf[2 * chip] + p_buf[2 * chip + 1]
    p_far = send(p_sum.at[chip], p_sum.at[chip], small_send.at[1], small_recv.at[1], far)
    p_far.start()
    w1x_copy(2).start()
    w1x_copy(3).start()

    pltpu.make_async_copy(x_real, x0, load_sem.at[3]).wait()
    gives[0].wait_recv()

    def y0_tile(tile_no, carry):
        cols = part(tile_no, TILE)
        y0[:, cols] = dot_t(x0[...], w0[cols, :])
        return carry

    lax.fori_loop(0, wide1 // TILE, y0_tile, 0)
    p_far.wait()
    p_all = p_sum[0] + p_sum[1]
    spans = ((0, n0, v0_out), (n0, n1, v1_out), (n0 + n1, 2 * wide2, v2_out))
    for first, size, v_out in spans:
        p_vec = p_all[:, first:first + size]
        v_out[...] = p_vec / jnp.maximum(jnp.sqrt(total(p_vec * p_vec)), EPSILON)
    u0_out[...] = dot_t(row(v0_out[...]), w0[own1, :])[0:1]
    u1_out[...] = dot_t(row(v1_out[...]), w1[own2, :])[0:1]
    u2_out[...] = dot_t(row(v2_out[...]), w2[own2, :])[0:1]
    lane = lax.broadcasted_iota(jnp.int32, (8, 128), 1)

    def pack(values):
        packed = jnp.zeros((8, 128), F32)
        for place, value in enumerate(values):
            packed = jnp.where(lane == place, value, packed)
        return packed

    n_buf[me] = pack([total(u_out[...] * u_out[...]) for u_out in (u0_out, u1_out, u2_out)])
    n_copies = spread(n_buf, 3)
    for copy in n_copies:
        copy.start()
    for piece_no in range(4, PIECES):
        w1x_copy(piece_no).start()
    for copy in gives[1:]:
        copy.start()

    @pl.when(core == 0)
    def _():
        send(t_fake, tt.at[own2, :], w_send.at[3], w_recv.at[3], mate).start()

    @pl.when(core == 1)
    def _():
        send(t_real, tt.at[own2, :], w_send.at[3], w_recv.at[3], mate).start()

    for copy in n_copies:
        copy.wait()
    sigmas = jnp.sqrt(n_buf[0] + n_buf[1] + n_buf[2] + n_buf[3])
    sig_out[...] = sigmas
    sig0, sig1, sig2 = sigmas[0:1, 0:1], sigmas[0:1, 1:2], sigmas[0:1, 2:3]
    inv0, inv1, inv2 = 1.0 / sig0, 1.0 / sig1, 1.0 / sig2
    u0_out[...] = u0_out[...] / sig0
    u1_out[...] = u1_out[...] / sig1
    u2_out[...] = u2_out[...] / sig2

    def chunk_copy(buf, slot, chunk_no, send_sem, recv_sem):
        rows = buf.at[slot, part(chunk_no, step), :]
        return send(rows, rows, send_sem.at[chunk_no], recv_sem.at[chunk_no], far)

    def layer0(chunk_no, carry):
        rows = part(chunk_no, step)
        x1[chip, rows, :] = leaky_relu(y0[rows, :] * inv0).astype(BF16)
        chunk_copy(x1, chip, chunk_no, x1_send, x1_recv).start()
        return carry

    lax.fori_loop(0, CHUNKS, layer0, 0)

    batch = part(core, n_rows)

    def outputs(src, dst, which):
        return (
            pltpu.make_async_copy(src, dst, put_sem.at[which]),
            send(src, dst, out_send.at[which], out_recv.at[which], mate),
        )

    def halves(src, dst, size, which):
        return (
            pltpu.make_async_copy(src.at[part(core, size), :], dst.at[:, batch], put_sem.at[which]),
            send(src.at[part(1 - core, size), :], dst.at[:, batch], out_send.at[which], out_recv.at[which], mate),
        )

    x1_near = outputs(x1.at[chip], x1_out.at[batch, part(chip, wide1)], 0)
    for copy in x1_near:
        copy.start()
    for piece_no in range(PIECES):
        w1x_copy(piece_no).wait_recv()
        w1x_forward(piece_no).start()

    gives[1].wait_recv()

    def layer1(chunk_no, carry):
        rows = part(chunk_no, step)
        chunk_copy(x1, other, chunk_no, x1_send, x1_recv).wait_recv()
        y_val = (dot_t(x1[0, rows, :], w1[:, pl.ds(0, wide1)]) + dot_t(x1[1, rows, :], w1[:, pl.ds(wide1, wide1)])) * inv1
        y1[rows, :] = y_val
        x2[chip, rows, :] = leaky_relu(y_val).astype(BF16)
        chunk_copy(x2, chip, chunk_no, x2_send, x2_recv).start()
        return carry

    lax.fori_loop(0, CHUNKS, layer1, 0)
    x1_far = outputs(x1.at[other], x1_out.at[batch, part(other, wide1)], 1)
    for copy in x1_far:
        copy.start()

    gives[2].wait_recv()
    pltpu.make_async_copy(t_real, tt.at[own2, :], load_sem.at[4]).wait()
    t_give = send(t_real, tt.at[own2, :], w_send.at[3], w_recv.at[3], mate)
    t_give.wait_recv()

    def layer2(chunk_no, carry):
        corr2, loss = carry
        rows = part(chunk_no, step)
        chunk_copy(x2, other, chunk_no, x2_send, x2_recv).wait_recv()
        y_val = (dot_t(x2[0, rows, :], w2[:, pl.ds(0, wide2)]) + dot_t(x2[1, rows, :], w2[:, pl.ds(wide2, wide2)])) * inv2
        e_val = y_val - dot_t(eye[0:step, 0:step], tt[:, rows])
        corr2 = corr2 + fold(e_val * y_val)
        loss = loss + fold(e_val * e_val)
        e_half = e_val.astype(BF16)
        h2_put[rows, :] = dot_n(e_half, w2[:, part(other, wide2)]).astype(BF16)
        send(h2_put.at[rows, :], h2_got.at[rows, :], h2_send.at[chunk_no], h2_recv.at[chunk_no], far).start()
        h2_own[rows, :] = dot_n(e_half, w2[:, part(chip, wide2)])
        store_transposed(e2_t, 0, rows, e_half)
        return corr2, loss

    zero = jnp.zeros((8, wide2), F32)
    corr2, loss = lax.fori_loop(0, CHUNKS, layer2, (zero, zero))

    def back1(chunk_no, corr1):
        rows = part(chunk_no, step)
        send(h2_put.at[rows, :], h2_got.at[rows, :], h2_send.at[chunk_no], h2_recv.at[chunk_no], far).wait_recv()
        y_val = y1[rows, :]
        e_val = (h2_own[rows, :] + h2_got[rows, :].astype(F32)) * (inv2 * leaky_slope(y_val))
        e_half = e_val.astype(BF16)
        e1[chip, rows, :] = e_half
        chunk_copy(e1, chip, chunk_no, e1_send, e1_recv).start()
        store_transposed(e1_t, 0, rows, e_half)
        return corr1 + fold(e_val * y_val)

    corr1 = lax.fori_loop(0, CHUNKS, back1, zero)
    lesser = [
        outputs(x2.at[0], x2_out.at[batch, pl.ds(0, wide2)], 2),
        outputs(x2.at[1], x2_out.at[batch, pl.ds(wide2, wide2)], 3),
        halves(e2_t, e2_out, rows2, 4),
        halves(e1_t, e1_out, rows2, 5),
    ]
    for pair in lesser:
        for copy in pair:
            copy.start()
    for piece_no in range(PIECES):
        w1x_forward(piece_no).wait_recv()

    def h0_copy(chunk_no):
        rows = part(chunk_no, step)
        return send(h0_put.at[rows, :], got_out.at[rows, :], h0_send.at[chunk_no], h0_recv.at[chunk_no], far)

    def both_copies(chunk_no):
        src = h0_put.at[part(chunk_no, step), :]
        dst = both_out.at[pl.ds(pl.multiple_of(core * n_rows + chunk_no * step, step), step), :]
        return (
            pltpu.make_async_copy(src, dst, both_sem.at[chunk_no]),
            send(src, dst, both_send.at[chunk_no], both_recv.at[chunk_no], mate),
        )

    def late_copy(sum_out, start, chunk_no):
        dst = sum_out.at[part(chunk_no - start, step), :]
        return pltpu.make_async_copy(h0_put.at[part(chunk_no, step), :], dst, sum_sem.at[chunk_no])

    def back0(chunk_no, corr0):
        rows = part(chunk_no, step)
        chunk_copy(e1, other, chunk_no, e1_send, e1_recv).wait_recv()

        def h1_tile(tile_no, corr):
            cols = part(tile_no, wide2)
            own_cols = pl.ds(pl.multiple_of(chip * wide1 + tile_no * wide2, 128), wide2)
            h_val = dot_n(e1[chip, rows, :], w1[:, own_cols]) + dot_n(e1[other, rows, :], w1x[:, cols])
            y_val = y0[rows, cols] * inv0
            e_val = h_val * (inv1 * leaky_slope(y_val))
            e0[:, cols] = e_val.astype(BF16)
            return corr + fold(e_val * y_val)

        corr0 = lax.fori_loop(0, wide1 // wide2, h1_tile, corr0)
        h0_put[rows, :] = dot_n(e0[...], w0[...]).astype(BF16)
        return corr0

    def transpose0(chunk_no):
        rows = part(chunk_no, step)

        def tile(tile_no, carry):
            store_transposed(e0_t, tile_no * wide2, rows, e0[:, part(tile_no, wide2)])
            return carry

        lax.fori_loop(0, wide1 // wide2, tile, 0)
        for copy in e0_copies(chunk_no):
            copy.start()

    def e0_copies(chunk_no):
        rows = part(chunk_no, step)
        dst = e0_out.at[:, pl.ds(pl.multiple_of(core * n_rows + chunk_no * step, step), step)]
        return (
            pltpu.make_async_copy(e0_t.at[part(core, rows1), rows], dst, e0_sem.at[chunk_no]),
            send(e0_t.at[part(1 - core, rows1), rows], dst, e0_send.at[chunk_no], e0_recv.at[chunk_no], mate),
        )

    def early_chunk(chunk_no, corr0):
        corr0 = back0(chunk_no, corr0)
        for copy in (h0_copy(chunk_no), *both_copies(chunk_no)):
            copy.start()
        transpose0(chunk_no)
        return corr0

    def late_chunk(sum_out, start, chunk_no, corr0):
        corr0 = back0(chunk_no, corr0)
        for copy in (late_copy(sum_out, start, chunk_no), *both_copies(chunk_no)):
            copy.start()
        transpose0(chunk_no)
        return corr0

    corr0 = jnp.zeros((8, wide2), F32)
    corr0 = lax.fori_loop(0, EARLY, early_chunk, corr0)
    corr0 = lax.fori_loop(EARLY, EARLY + MIDDLE, functools.partial(late_chunk, mid_out, EARLY), corr0)
    corr0 = lax.fori_loop(EARLY + MIDDLE, CHUNKS, functools.partial(late_chunk, last_out, EARLY + MIDDLE), corr0)
    c_buf[me] = pack([total(corr) for corr in (corr0, corr1, corr2, loss)])
    c_copies = spread(c_buf, 6)
    for copy in c_copies:
        copy.start()

    for copy in c_copies:
        copy.wait()
    cor_out[...] = c_buf[0] + c_buf[1] + c_buf[2] + c_buf[3]

    for copy in gives:
        copy.wait_send()
    t_give.wait_send()
    for piece_no in range(PIECES):
        w1x_copy(piece_no).wait_send()
        w1x_forward(piece_no).wait_send()
    for pair in (x1_near, x1_far, *lesser):
        for copy in pair:
            copy.wait()

    def drain(chunk_no, carry):
        rows = part(chunk_no, step)
        chunk_copy(x1, chip, chunk_no, x1_send, x1_recv).wait_send()
        chunk_copy(x2, chip, chunk_no, x2_send, x2_recv).wait_send()
        send(h2_put.at[rows, :], h2_got.at[rows, :], h2_send.at[chunk_no], h2_recv.at[chunk_no], far).wait_send()
        chunk_copy(e1, chip, chunk_no, e1_send, e1_recv).wait_send()
        return carry

    lax.fori_loop(0, CHUNKS, drain, 0)

    for chunk_no in range(CHUNKS):
        if chunk_no < EARLY:
            h0_copy(chunk_no).wait()
        elif chunk_no < EARLY + MIDDLE:
            late_copy(mid_out, EARLY, chunk_no).wait()
        else:
            late_copy(last_out, EARLY + MIDDLE, chunk_no).wait()
        for copy in (*both_copies(chunk_no), *e0_copies(chunk_no)):
            copy.wait()


def run_chain(x_real, x_fake, weight0, weight1, weight2, u_left0, u_left1, u_left2, t_real, t_fake):
    n_rows, n0 = x_real.shape
    rows1 = weight0.shape[0]
    rows2, n1 = weight1.shape
    wide1, wide2 = 2 * rows1, 2 * rows2
    n2 = 2 * wide2
    step = n_rows // CHUNKS
    early, middle = EARLY * step, MIDDLE * step
    last = n_rows - early - middle
    hbm = pl.BlockSpec(memory_space=pl.ANY)
    vmem = pl.BlockSpec(memory_space=pltpu.VMEM)
    shape = jax.ShapeDtypeStruct
    dma = pltpu.SemaphoreType.DMA
    return pl.pallas_call(
        chain_kernel,
        out_shape=(
            shape((2 * n_rows, n1), BF16), shape((2 * n_rows, n2), BF16), shape((rows2, 2 * n_rows), BF16), shape((rows2, 2 * n_rows), BF16),
            shape((rows1, 2 * n_rows), BF16), shape((early, n0), BF16), shape((middle, n0), BF16), shape((last, n0), BF16), shape((2 * n_rows, n0), BF16),
            shape((1, n0), F32), shape((1, n1), F32), shape((1, n2), F32),
            shape((1, rows1), F32), shape((1, rows2), F32), shape((1, rows2), F32),
            shape((8, 128), F32), shape((8, 128), F32),
        ),
        in_specs=[hbm] * 5 + [vmem] * 3 + [hbm] * 2,
        out_specs=[hbm] * 9 + [vmem] * 8,
        scratch_shapes=[
            pltpu.VMEM((wide1, n0), BF16), pltpu.VMEM((wide2, n1), BF16), pltpu.VMEM((wide2, wide1), BF16), pltpu.VMEM((wide2, n2), BF16),
            pltpu.VMEM((n_rows, n0), BF16), pltpu.VMEM((2, n_rows, wide1), BF16), pltpu.VMEM((2, n_rows, wide2), BF16),
            pltpu.VMEM((n_rows, wide1), F32), pltpu.VMEM((n_rows, wide2), F32), pltpu.VMEM((wide2, n_rows), BF16),
            pltpu.VMEM((wide2, n_rows), BF16), pltpu.VMEM((n_rows, wide2), F32), pltpu.VMEM((n_rows, wide2), BF16), pltpu.VMEM((n_rows, wide2), BF16),
            pltpu.VMEM((2, n_rows, wide2), BF16), pltpu.VMEM((wide2, n_rows), BF16), pltpu.VMEM((n_rows // CHUNKS, wide1), BF16), pltpu.VMEM((wide1, n_rows), BF16),
            pltpu.VMEM((n_rows, n0), BF16),
            pltpu.VMEM((4, 1, n0 + n1 + n2), F32), pltpu.VMEM((2, 1, n0 + n1 + n2), F32), pltpu.VMEM((4, 8, 128), F32), pltpu.VMEM((4, 8, 128), F32), pltpu.VMEM((256, 256), BF16),
            dma((5,)), dma((7,)), dma((4,)), dma((4,)), dma((PIECES,)), dma((PIECES,)), dma((PIECES,)), dma((PIECES,)), dma((9,)), dma((9,)),
            dma((CHUNKS,)), dma((CHUNKS,)), dma((CHUNKS,)), dma((CHUNKS,)), dma((CHUNKS,)), dma((CHUNKS,)),
            dma((CHUNKS,)), dma((CHUNKS,)), dma((EARLY,)), dma((EARLY,)), dma((7,)), dma((7,)),
            dma((CHUNKS,)), dma((CHUNKS,)), dma((CHUNKS,)), dma((CHUNKS,)), dma((CHUNKS,)), dma((CHUNKS,)), dma((CHUNKS,)),
        ],
        compiler_params=pltpu.CompilerParams(collective_id=0, has_side_effects=True, vmem_limit_bytes=67043328),
        name="chain",
    )(x_real, x_fake, weight0, weight1, weight2, u_left0, u_left1, u_left2, t_real.T, t_fake.T)


def grad_kernel(x1_in, e1_in, x2_in, e2_in, x_real, x_fake, e0_in, u0_in, u1_in, u2_in, v0_in, v1_in, v2_in, sig_in, cor_in,
                dw0_out, dw1_out, dw2_out, u0_out, u1_out, u2_out, v0_out, v1_out, v2_out, sig_out, loss_out,
                x1, e1, x2, e2, x0, e0, dw0, dw1, dw2, u0, u1, u2, v0, v1, v2, sig, cor, in_sem, x1_sem, out_sem, dw1_sem, dw0_sem):
    n_rows = x_real.shape[0]
    tiles1 = x1_sem.shape[0]
    tiles0 = dw0_sem.shape[0]

    def pull(src, dst, which):
        copy = pltpu.make_async_copy(src, dst, in_sem.at[which])
        copy.start()
        return copy

    small = [pull(src, dst, place) for place, (src, dst) in enumerate((
        (u0_in, u0), (u1_in, u1), (u2_in, u2), (v0_in, v0), (v1_in, v1), (v2_in, v2), (sig_in, sig), (cor_in, cor)))]

    def tile_of(size, tiles, tile_no):
        return pl.ds(tile_no * (size // tiles), size // tiles)

    def load(src, dst, which):
        return pltpu.make_async_copy(src, dst, in_sem.at[which])

    got_e1 = pull(e1_in, e1, 11)
    got_x1 = []
    for tile_no in range(tiles1):
        cols = tile_of(x1.shape[1], tiles1, tile_no)
        got_x1.append(pltpu.make_async_copy(x1_in.at[:, cols], x1.at[:, cols], x1_sem.at[tile_no]))
    got_e0 = load(e0_in, e0, 8)
    got_x0 = [load(x_real, x0.at[pl.ds(0, n_rows), :], 9), load(x_fake, x0.at[pl.ds(n_rows, n_rows), :], 10)]
    got_2 = [load(e2_in, e2, 13), load(x2_in, x2, 14)]
    queue = [*got_x1, *got_x0, got_e0, *got_2]

    def read_on(count=1):
        for _ in range(min(count, len(queue))):
            queue.pop(0).start()

    read_on(3)

    for copy in small:
        copy.wait()
    for src, dst in ((u0, u0_out), (u1, u1_out), (u2, u2_out), (v0, v0_out), (v1, v1_out), (v2, v2_out)):
        dst[...] = src[...].reshape(dst.shape)
    sig_out[...] = sig[0:1, 0:3].reshape(3)
    loss_out[...] = cor[0:1, 3:4] * (0.5 / n_rows)

    def column(u_new, layer_no):
        return jnp.broadcast_to(u_new[...] * cor[0:1, layer_no:layer_no + 1], (128, u_new.shape[1])).T[:, 0:1]

    def scale(layer_no):
        return 1.0 / (n_rows * sig[0:1, layer_no:layer_no + 1])

    pushes = []

    def gradient(errors, layer_in, cols, col, v_new, rate, dst, out, sem):
        dst[:, cols] = (dot_n(errors[...], layer_in[:, cols]) - col * v_new[:, cols]) * rate
        copy = pltpu.make_async_copy(dst.at[:, cols], out.at[:, cols], sem)
        copy.start()
        pushes.append(copy)

    got_e1.wait()
    col1, scale1 = column(u1, 1), scale(1)
    for tile_no in range(tiles1):
        got_x1[tile_no].wait()
        read_on()
        gradient(e1, x1, tile_of(x1.shape[1], tiles1, tile_no), col1, v1, scale1, dw1, dw1_out, dw1_sem.at[tile_no])
    got_e0.wait()
    read_on(3)
    for copy in got_x0:
        copy.wait()
    col0, scale0 = column(u0, 0), scale(0)
    for tile_no in range(tiles0):
        gradient(e0, x0, tile_of(x0.shape[1], tiles0, tile_no), col0, v0, scale0, dw0, dw0_out, dw0_sem.at[tile_no])
    for copy in got_2:
        copy.wait()
    col2, scale2 = column(u2, 2), scale(2)
    for tile_no in range(2):
        gradient(e2, x2, tile_of(x2.shape[1], 2, tile_no), col2, v2, scale2, dw2, dw2_out, out_sem.at[2 + tile_no])
    for copy in pushes:
        copy.wait()


def run_grads(x1, e1, x2, e2, x_real, x_fake, e0, u0, u1, u2, v0, v1, v2, sig, cor):
    both, n1 = x1.shape
    _, n0 = x_real.shape
    n2 = x2.shape[1]
    rows2 = e1.shape[0]
    rows1 = e0.shape[0]
    tiles1, tiles0 = 10, 5
    shape = jax.ShapeDtypeStruct
    hbm = pl.BlockSpec(memory_space=pltpu.HBM)
    vmem = pl.BlockSpec(memory_space=pltpu.VMEM)
    dma = pltpu.SemaphoreType.DMA
    flops = 2 * both * (rows2 * (n1 + n2) + rows1 * n0)
    inputs = (x1, e1, x2, e2, x_real, x_fake, e0, u0, u1, u2, v0, v1, v2, sig, cor)
    inputs = tuple(pltpu.with_memory_space_constraint(array, pltpu.HBM) for array in inputs)
    return pl.pallas_call(
        grad_kernel,
        out_shape=(
            shape((rows1, n0), F32), shape((rows2, n1), F32), shape((rows2, n2), F32),
            shape((rows1,), F32), shape((rows2,), F32), shape((rows2,), F32), shape((n0,), F32), shape((n1,), F32), shape((n2,), F32),
            shape((3,), F32), shape((1, 1), F32),
        ),
        in_specs=[hbm] * len(inputs),
        out_specs=[hbm] * 3 + [vmem] * 8,
        scratch_shapes=[
            pltpu.VMEM((both, n1), BF16), pltpu.VMEM((rows2, both), BF16), pltpu.VMEM((both, n2), BF16), pltpu.VMEM((rows2, both), BF16),
            pltpu.VMEM((both, n0), BF16), pltpu.VMEM((rows1, both), BF16),
            pltpu.VMEM((rows1, n0), F32), pltpu.VMEM((rows2, n1), F32), pltpu.VMEM((rows2, n2), F32),
            *[pltpu.VMEM(array.shape, F32) for array in (u0, u1, u2, v0, v1, v2, sig, cor)],
            dma((15,)), dma((tiles1,)), dma((4,)), dma((tiles1,)), dma((tiles0,)),
        ],
        compiler_params=pltpu.CompilerParams(vmem_limit_bytes=48 * 1024 * 1024),
        cost_estimate=pl.CostEstimate(flops=flops, bytes_accessed=45 * 1024 * 1024, transcendentals=0),
        name="grads",
    )(*inputs)


def finish_kernel(plan, in_place, *refs):
    refs = refs[2:] if in_place else refs
    both, sig = refs[:2]
    cames = refs[2:2 + len(plan)]
    real_out, fake_out, dx, out_sem = refs[2 + len(plan):]
    core = lax.axis_index("model") % 2
    n_rows = real_out.shape[0]
    inv0 = 1.0 / sig[0:1, 0:1]
    size = dx.shape[0] // out_sem.shape[0]
    jobs = []
    for came, (flip, first) in zip(cames, plan):
        batch = 1 - core if flip else core
        for begin in range(0, came.shape[0], size):
            jobs.append((came, begin, batch, first + begin))

    def push(dst, place, first):
        return pltpu.make_async_copy(dx.at[pl.ds(place * size, size), :], dst.at[pl.ds(first, size), :], out_sem.at[place])

    for place, (came, begin, batch, first) in enumerate(jobs):
        own = pl.ds(pl.multiple_of(batch * n_rows + first, size), size)
        dx[pl.ds(place * size, size), :] = (both[own, :].astype(F32) + came[pl.ds(begin, size), :].astype(F32)) * inv0

        @pl.when(batch == 0)
        def _():
            push(real_out, place, first).start()

        @pl.when(batch == 1)
        def _():
            push(fake_out, place, first).start()

    for place, (_, _, _, first) in enumerate(jobs):
        push(real_out, place, first).wait()


def run_finish(old, both, sig, parts):
    cames = [came for came, _, _ in parts]
    rows = sum(came.shape[0] for came in cames)
    n0 = both.shape[1]
    size = 64
    hbm = pl.BlockSpec(memory_space=pltpu.HBM)
    vmem = pl.BlockSpec(memory_space=pltpu.VMEM)
    shape = jax.ShapeDtypeStruct((both.shape[0] // 2, n0), F32)
    return pl.pallas_call(
        functools.partial(finish_kernel, tuple((flip, first) for _, flip, first in parts), bool(old)),
        out_shape=(shape, shape),
        in_specs=[hbm] * len(old) + [vmem] * (2 + len(cames)),
        out_specs=[hbm] * 2,
        scratch_shapes=[pltpu.VMEM((rows, n0), F32), pltpu.SemaphoreType.DMA((rows // size,))],
        input_output_aliases={0: 0, 1: 1} if old else {},
        compiler_params=pltpu.CompilerParams(vmem_limit_bytes=16 * 1024 * 1024),
        cost_estimate=pl.CostEstimate(flops=4 * rows * n0, bytes_accessed=8 * rows * n0, transcendentals=0),
        name="finish",
    )(*old, both, sig, *cames)


def swap(values, bits):
    return lax.ppermute(values, "model", [(dev, dev ^ bits) for dev in range(4)])


def solution(mesh):
    rows_spec = P("rep", None)
    weight_spec = P(("rep", "model"), None)
    left_spec = P(("rep", "model"))
    target_spec = P("rep", "model")
    group_spec = P("rep")

    def local_step(x_real, x_fake, weight0, weight1, weight2, u_left0, u_left1, u_left2, t_real, t_fake):
        x1, x2, e2, e1, e0, first, middle, last, both, v0, v1, v2, u0, u1, u2, sig, cor = run_chain(x_real, x_fake, weight0, weight1, weight2, u_left0, u_left1, u_left2, t_real, t_fake)
        row1 = first.shape[0]
        row2 = row1 + middle.shape[0]
        middle = swap(middle, 2)
        last = swap(last, 2)
        first_mate = swap(first, 1)
        grads = run_grads(x1, e1, x2, e2, x_real, x_fake, e0, u0, u1, u2, v0, v1, v2, sig, cor)
        dw0, dw1, dw2, u0, u1, u2, v0, v1, v2, sigmas, loss = grads
        middle, sigmas = lax.optimization_barrier((middle, sigmas))
        middle_mate = swap(middle, 1)
        dx = run_finish((), both, sig, ((first, False, 0), (first_mate, True, 0), (middle, False, row1)))
        dx = run_finish(dx, both, sig, ((middle_mate, True, row1),))
        last, *dx = lax.optimization_barrier((last, *dx))
        last_mate = swap(last, 1)
        dx = run_finish(dx, both, sig, ((last, False, row2),))
        dx_real, dx_fake = run_finish(dx, both, sig, ((last_mate, True, row2),))
        return (loss[0], dx_real, dx_fake, dw0, dw1, dw2, u0, u1, u2, v0, v1, v2, sigmas)

    return jax.shard_map(local_step, mesh=mesh, in_specs=(rows_spec, rows_spec, weight_spec, weight_spec, weight_spec, left_spec, left_spec, left_spec, target_spec, target_spec), out_specs=(group_spec, rows_spec, rows_spec, weight_spec, weight_spec, weight_spec, left_spec, left_spec, left_spec, group_spec, group_spec, group_spec, group_spec), check_vma=False)
```

```python
import functools

import jax
import jax.numpy as jnp
from jax import lax
from jax.experimental import pallas as pl
from jax.experimental.pallas import tpu as pltpu
from jax.sharding import PartitionSpec as P


SLOPE = 0.2
EPSILON = 1e-12
MESH = pl.DeviceIdType.MESH
CHUNKS = 4
EARLY = 1
MIDDLE = 2
PIECES = 5
TILE = 256
BF16 = jnp.bfloat16
F32 = jnp.float32


def leaky_relu(values):
    return jnp.where(values > 0, values, SLOPE * values)


def leaky_slope(values):
    return jnp.where(values > 0, 1.0, SLOPE)


def dot_t(left, right):
    return lax.dot_general(left, right, (((1,), (1,)), ((), ())), preferred_element_type=F32)


def dot_n(left, right):
    return lax.dot_general(left, right, (((1,), (0,)), ((), ())), preferred_element_type=F32)


def fold(values):
    rows, cols = values.shape
    return jnp.sum(values.reshape(rows // 8, 8, cols), axis=0)


def total(values):
    return jnp.sum(jnp.sum(values, axis=1, keepdims=True), axis=0, keepdims=True)


def chain_kernel(x_real, x_fake, w0_in, w1_in, w2_in, u0_hbm, u1_hbm, u2_hbm, t_real, t_fake,
                 x1_out, x2_out, e2_out, e1_out, e0_out, got_out, mid_out, last_out, both_out, v0_hbm, v1_hbm, v2_hbm, u0_new, u1_new, u2_new, sig_hbm, cor_hbm,
                 w0, w1, w1x, w2, x0, x1, x2, y0, y1, tt, e2_t, h2_own, h2_put, h2_got, e1, e1_t, e0, e0_t, h0_put,
                 p_buf, p_sum, n_buf, c_buf,
                 eye, u0_in, u1_in, u2_in, v0_out, v1_out, v2_out, u0_out, u1_out, u2_out, sig_out, small_sem, load_sem, put_sem, w_send, w_recv, w1x_send, w1x_recv, fwd_send, fwd_recv, small_send, small_recv,
                 x1_send, x1_recv, x2_send, x2_recv, h2_send, h2_recv, e1_send, e1_recv, h0_send, h0_recv, out_send, out_recv, sum_sem, both_sem, both_send, both_recv, e0_sem, e0_send, e0_recv):
    me = lax.axis_index("model")
    chip = me // 2
    core = me % 2
    other = 1 - chip
    mate = me + 1 - 2 * core
    far = me + 2 - 4 * chip
    diag = mate + 2 - 4 * chip
    n_rows, n0 = x0.shape
    wide1 = w0.shape[0]
    rows1 = wide1 // 2
    wide2 = w2.shape[0]
    rows2 = wide2 // 2
    n1 = 2 * wide1
    step = n_rows // CHUNKS
    piece = rows2 // PIECES

    def send(src, dst, send_sem, recv_sem, device):
        return pltpu.make_async_remote_copy(src_ref=src, dst_ref=dst, send_sem=send_sem, recv_sem=recv_sem, device_id={"model": device}, device_id_type=MESH)

    def part(index, size):
        return pl.ds(pl.multiple_of(index * size, size), size)

    barrier = pltpu.get_barrier_semaphore()
    for device in (mate, far, diag):
        pl.semaphore_signal(barrier, inc=1, device_id={"model": device}, device_id_type=MESH)
    pl.semaphore_wait(barrier, 3)

    def w1x_copy(piece_no):
        return send(
            w1_in.at[pl.ds(piece_no * piece, piece), part(other, wide1)],
            w1x.at[pl.ds(pl.multiple_of(core * rows2 + piece_no * piece, piece), piece), :],
            w1x_send.at[piece_no], w1x_recv.at[piece_no], far)

    def w1x_forward(piece_no):
        rows = w1x.at[pl.ds(pl.multiple_of(core * rows2 + piece_no * piece, piece), piece), :]
        return send(rows, rows, fwd_send.at[piece_no], fwd_recv.at[piece_no], mate)

    own1, own2 = part(core, rows1), part(core, rows2)
    loads = [
        pltpu.make_async_copy(w0_in, w0.at[own1, :], load_sem.at[0]),
        pltpu.make_async_copy(w1_in, w1.at[own2, :], load_sem.at[1]),
        pltpu.make_async_copy(w2_in, w2.at[own2, :], load_sem.at[2]),
    ]
    gives = [
        send(w0.at[own1, :], w0.at[own1, :], w_send.at[0], w_recv.at[0], mate),
        send(w1.at[own2, :], w1.at[own2, :], w_send.at[1], w_recv.at[1], mate),
        send(w2.at[own2, :], w2.at[own2, :], w_send.at[2], w_recv.at[2], mate),
    ]
    w1x_copy(0).start()
    for copy in loads:
        copy.start()

    w1x_copy(1).start()
    u_loads = [pltpu.make_async_copy(src, dst, small_sem.at[place]) for place, (src, dst) in enumerate(((u0_hbm, u0_in), (u1_hbm, u1_in), (u2_hbm, u2_in)))]
    for copy in u_loads:
        copy.start()

    def mine(x_in, t_own):
        return (
            pltpu.make_async_copy(x_in, x0, load_sem.at[3]),
            pltpu.make_async_copy(t_own, tt.at[own2, :], load_sem.at[4]),
        )

    @pl.when(core == 0)
    def _():
        for copy in mine(x_real, t_real):
            copy.start()

    @pl.when(core == 1)
    def _():
        for copy in mine(x_fake, t_fake):
            copy.start()

    def row(values):
        return jnp.broadcast_to(values.reshape(1, values.size).astype(BF16), (16, values.size))

    lanes = lax.broadcasted_iota(jnp.int32, eye.shape, 1)
    eye[...] = jnp.where(lanes == lax.broadcasted_iota(jnp.int32, eye.shape, 0), 1.0, 0.0).astype(BF16)

    def store_transposed(dst, first, rows, values):
        for begin in range(0, values.shape[1], eye.shape[0]):
            size = min(eye.shape[0], values.shape[1] - begin)
            block = dot_t(eye[0:size, 0:size], values[:, begin:begin + size])
            dst[pl.ds(pl.multiple_of(first + begin, 128), size), rows] = block.astype(BF16)

    for copy in u_loads:
        copy.wait()
    u_rows = [row(u0_in[...]), row(u1_in[...]), row(u2_in[...])]
    loads[0].wait()
    p_buf[me, :, pl.ds(0, n0)] = dot_n(u_rows[0], w0[own1, :])[0:1]
    loads[1].wait()

    def p1_tile(tile_no, carry):
        cols = part(tile_no, wide1 // 2)
        p_buf[me, :, pl.ds(pl.multiple_of(n0 + tile_no * (wide1 // 2), 128), wide1 // 2)] = dot_n(u_rows[1], w1[own2, cols])[0:1]
        return carry

    lax.fori_loop(0, 4, p1_tile, 0)
    loads[2].wait()
    p_buf[me, :, pl.ds(n0 + n1, wide2 * 2)] = dot_n(u_rows[2], w2[own2, :])[0:1]

    def spread(buf, first):
        return [send(buf.at[me], buf.at[me], small_send.at[first + which], small_recv.at[first + which], device) for which, device in enumerate((mate, far, diag))]

    p_near = send(p_buf.at[me], p_buf.at[me], small_send.at[0], small_recv.at[0], mate)
    p_near.start()
    gives[0].start()
    p_near.wait()
    p_sum[chip] = p_buf[2 * chip] + p_buf[2 * chip + 1]
    p_far = send(p_sum.at[chip], p_sum.at[chip], small_send.at[1], small_recv.at[1], far)
    p_far.start()
    w1x_copy(2).start()
    w1x_copy(3).start()

    pltpu.make_async_copy(x_real, x0, load_sem.at[3]).wait()
    gives[0].wait_recv()

    def y0_tile(tile_no, carry):
        cols = part(tile_no, TILE)
        y0[:, cols] = dot_t(x0[...], w0[cols, :])
        return carry

    lax.fori_loop(0, wide1 // TILE, y0_tile, 0)
    p_far.wait()
    p_all = p_sum[0] + p_sum[1]
    spans = ((0, n0, v0_out), (n0, n1, v1_out), (n0 + n1, 2 * wide2, v2_out))
    for first, size, v_out in spans:
        p_vec = p_all[:, first:first + size]
        v_out[...] = p_vec / jnp.maximum(jnp.sqrt(total(p_vec * p_vec)), EPSILON)
    u0_out[...] = dot_t(row(v0_out[...]), w0[own1, :])[0:1]
    u1_out[...] = dot_t(row(v1_out[...]), w1[own2, :])[0:1]
    u2_out[...] = dot_t(row(v2_out[...]), w2[own2, :])[0:1]
    lane = lax.broadcasted_iota(jnp.int32, (8, 128), 1)

    def pack(values):
        packed = jnp.zeros((8, 128), F32)
        for place, value in enumerate(values):
            packed = jnp.where(lane == place, value, packed)
        return packed

    n_buf[me] = pack([total(u_out[...] * u_out[...]) for u_out in (u0_out, u1_out, u2_out)])
    n_copies = spread(n_buf, 3)
    for copy in n_copies:
        copy.start()
    for piece_no in range(4, PIECES):
        w1x_copy(piece_no).start()
    for copy in gives[1:]:
        copy.start()

    @pl.when(core == 0)
    def _():
        send(t_fake, tt.at[own2, :], w_send.at[3], w_recv.at[3], mate).start()

    @pl.when(core == 1)
    def _():
        send(t_real, tt.at[own2, :], w_send.at[3], w_recv.at[3], mate).start()

    for copy in n_copies:
        copy.wait()
    sigmas = jnp.sqrt(n_buf[0] + n_buf[1] + n_buf[2] + n_buf[3])
    sig_out[...] = sigmas
    sig0, sig1, sig2 = sigmas[0:1, 0:1], sigmas[0:1, 1:2], sigmas[0:1, 2:3]
    inv0, inv1, inv2 = 1.0 / sig0, 1.0 / sig1, 1.0 / sig2
    u0_out[...] = u0_out[...] / sig0
    u1_out[...] = u1_out[...] / sig1
    u2_out[...] = u2_out[...] / sig2
    results = [pltpu.make_async_copy(src, dst, small_sem.at[3 + place]) for place, (src, dst) in enumerate((
        (v0_out, v0_hbm), (v1_out, v1_hbm), (v2_out, v2_hbm), (u0_out, u0_new), (u1_out, u1_new), (u2_out, u2_new), (sig_out, sig_hbm)))]
    for copy in results:
        copy.start()

    def chunk_copy(buf, slot, chunk_no, send_sem, recv_sem):
        rows = buf.at[slot, part(chunk_no, step), :]
        return send(rows, rows, send_sem.at[chunk_no], recv_sem.at[chunk_no], far)

    def layer0(chunk_no, carry):
        rows = part(chunk_no, step)
        x1[chip, rows, :] = leaky_relu(y0[rows, :] * inv0).astype(BF16)
        chunk_copy(x1, chip, chunk_no, x1_send, x1_recv).start()
        return carry

    lax.fori_loop(0, CHUNKS, layer0, 0)

    batch = part(core, n_rows)

    def outputs(src, dst, which):
        return (
            pltpu.make_async_copy(src, dst, put_sem.at[which]),
            send(src, dst, out_send.at[which], out_recv.at[which], mate),
        )

    def halves(src, dst, size, which):
        return (
            pltpu.make_async_copy(src.at[part(core, size), :], dst.at[:, batch], put_sem.at[which]),
            send(src.at[part(1 - core, size), :], dst.at[:, batch], out_send.at[which], out_recv.at[which], mate),
        )

    x1_near = outputs(x1.at[chip], x1_out.at[batch, part(chip, wide1)], 0)
    for copy in x1_near:
        copy.start()
    for piece_no in range(PIECES):
        w1x_copy(piece_no).wait_recv()
        w1x_forward(piece_no).start()

    gives[1].wait_recv()

    def layer1(chunk_no, carry):
        rows = part(chunk_no, step)
        chunk_copy(x1, other, chunk_no, x1_send, x1_recv).wait_recv()
        y_val = (dot_t(x1[0, rows, :], w1[:, pl.ds(0, wide1)]) + dot_t(x1[1, rows, :], w1[:, pl.ds(wide1, wide1)])) * inv1
        y1[rows, :] = y_val
        x2[chip, rows, :] = leaky_relu(y_val).astype(BF16)
        chunk_copy(x2, chip, chunk_no, x2_send, x2_recv).start()
        return carry

    lax.fori_loop(0, CHUNKS, layer1, 0)
    x1_far = outputs(x1.at[other], x1_out.at[batch, part(other, wide1)], 1)
    for copy in x1_far:
        copy.start()

    gives[2].wait_recv()
    pltpu.make_async_copy(t_real, tt.at[own2, :], load_sem.at[4]).wait()
    t_give = send(t_real, tt.at[own2, :], w_send.at[3], w_recv.at[3], mate)
    t_give.wait_recv()

    def layer2(chunk_no, carry):
        corr2, loss = carry
        rows = part(chunk_no, step)
        chunk_copy(x2, other, chunk_no, x2_send, x2_recv).wait_recv()
        y_val = (dot_t(x2[0, rows, :], w2[:, pl.ds(0, wide2)]) + dot_t(x2[1, rows, :], w2[:, pl.ds(wide2, wide2)])) * inv2
        e_val = y_val - dot_t(eye[0:step, 0:step], tt[:, rows])
        corr2 = corr2 + fold(e_val * y_val)
        loss = loss + fold(e_val * e_val)
        e_half = e_val.astype(BF16)
        h2_put[rows, :] = dot_n(e_half, w2[:, part(other, wide2)]).astype(BF16)
        send(h2_put.at[rows, :], h2_got.at[rows, :], h2_send.at[chunk_no], h2_recv.at[chunk_no], far).start()
        h2_own[rows, :] = dot_n(e_half, w2[:, part(chip, wide2)])
        store_transposed(e2_t, 0, rows, e_half)
        return corr2, loss

    zero = jnp.zeros((8, wide2), F32)
    corr2, loss = lax.fori_loop(0, CHUNKS, layer2, (zero, zero))

    def back1(chunk_no, corr1):
        rows = part(chunk_no, step)
        send(h2_put.at[rows, :], h2_got.at[rows, :], h2_send.at[chunk_no], h2_recv.at[chunk_no], far).wait_recv()
        y_val = y1[rows, :]
        e_val = (h2_own[rows, :] + h2_got[rows, :].astype(F32)) * (inv2 * leaky_slope(y_val))
        e_half = e_val.astype(BF16)
        e1[chip, rows, :] = e_half
        chunk_copy(e1, chip, chunk_no, e1_send, e1_recv).start()
        store_transposed(e1_t, 0, rows, e_half)
        return corr1 + fold(e_val * y_val)

    corr1 = lax.fori_loop(0, CHUNKS, back1, zero)
    lesser = [
        outputs(x2.at[0], x2_out.at[batch, pl.ds(0, wide2)], 2),
        outputs(x2.at[1], x2_out.at[batch, pl.ds(wide2, wide2)], 3),
        halves(e2_t, e2_out, rows2, 4),
        halves(e1_t, e1_out, rows2, 5),
    ]
    for pair in lesser:
        for copy in pair:
            copy.start()
    for piece_no in range(PIECES):
        w1x_forward(piece_no).wait_recv()

    def h0_copy(chunk_no):
        rows = part(chunk_no, step)
        return send(h0_put.at[rows, :], got_out.at[rows, :], h0_send.at[chunk_no], h0_recv.at[chunk_no], far)

    def both_copies(chunk_no):
        src = h0_put.at[part(chunk_no, step), :]
        dst = both_out.at[pl.ds(pl.multiple_of(core * n_rows + chunk_no * step, step), step), :]
        return (
            pltpu.make_async_copy(src, dst, both_sem.at[chunk_no]),
            send(src, dst, both_send.at[chunk_no], both_recv.at[chunk_no], mate),
        )

    def late_copy(sum_out, start, chunk_no):
        dst = sum_out.at[part(chunk_no - start, step), :]
        return pltpu.make_async_copy(h0_put.at[part(chunk_no, step), :], dst, sum_sem.at[chunk_no])

    def back0(chunk_no, corr0):
        rows = part(chunk_no, step)
        chunk_copy(e1, other, chunk_no, e1_send, e1_recv).wait_recv()

        def h1_tile(tile_no, corr):
            cols = part(tile_no, wide2)
            own_cols = pl.ds(pl.multiple_of(chip * wide1 + tile_no * wide2, 128), wide2)
            h_val = dot_n(e1[chip, rows, :], w1[:, own_cols]) + dot_n(e1[other, rows, :], w1x[:, cols])
            y_val = y0[rows, cols] * inv0
            e_val = h_val * (inv1 * leaky_slope(y_val))
            e0[:, cols] = e_val.astype(BF16)
            return corr + fold(e_val * y_val)

        corr0 = lax.fori_loop(0, wide1 // wide2, h1_tile, corr0)
        h0_put[rows, :] = dot_n(e0[...], w0[...]).astype(BF16)
        return corr0

    def transpose0(chunk_no):
        rows = part(chunk_no, step)

        def tile(tile_no, carry):
            store_transposed(e0_t, tile_no * wide2, rows, e0[:, part(tile_no, wide2)])
            return carry

        lax.fori_loop(0, wide1 // wide2, tile, 0)
        for copy in e0_copies(chunk_no):
            copy.start()

    def e0_copies(chunk_no):
        rows = part(chunk_no, step)
        dst = e0_out.at[:, pl.ds(pl.multiple_of(core * n_rows + chunk_no * step, step), step)]
        return (
            pltpu.make_async_copy(e0_t.at[part(core, rows1), rows], dst, e0_sem.at[chunk_no]),
            send(e0_t.at[part(1 - core, rows1), rows], dst, e0_send.at[chunk_no], e0_recv.at[chunk_no], mate),
        )

    def early_chunk(chunk_no, corr0):
        corr0 = back0(chunk_no, corr0)
        for copy in (h0_copy(chunk_no), *both_copies(chunk_no)):
            copy.start()
        transpose0(chunk_no)
        return corr0

    def late_chunk(sum_out, start, chunk_no, corr0):
        corr0 = back0(chunk_no, corr0)
        for copy in (late_copy(sum_out, start, chunk_no), *both_copies(chunk_no)):
            copy.start()
        transpose0(chunk_no)
        return corr0

    corr0 = jnp.zeros((8, wide2), F32)
    corr0 = lax.fori_loop(0, EARLY, early_chunk, corr0)
    corr0 = lax.fori_loop(EARLY, EARLY + MIDDLE, functools.partial(late_chunk, mid_out, EARLY), corr0)
    corr0 = lax.fori_loop(EARLY + MIDDLE, CHUNKS, functools.partial(late_chunk, last_out, EARLY + MIDDLE), corr0)
    c_buf[me] = pack([total(corr) for corr in (corr0, corr1, corr2, loss)])
    c_copies = [send(c_buf.at[me], cor_hbm.at[me], small_send.at[6 + which], small_recv.at[6 + which], device) for which, device in enumerate((mate, far, diag))]
    c_copies.append(pltpu.make_async_copy(c_buf.at[me], cor_hbm.at[me], small_sem.at[10]))
    for copy in c_copies:
        copy.start()

    for copy in c_copies:
        copy.wait()
    for copy in results:
        copy.wait()

    for copy in gives:
        copy.wait_send()
    t_give.wait_send()
    for piece_no in range(PIECES):
        w1x_copy(piece_no).wait_send()
        w1x_forward(piece_no).wait_send()
    for pair in (x1_near, x1_far, *lesser):
        for copy in pair:
            copy.wait()

    def drain(chunk_no, carry):
        rows = part(chunk_no, step)
        chunk_copy(x1, chip, chunk_no, x1_send, x1_recv).wait_send()
        chunk_copy(x2, chip, chunk_no, x2_send, x2_recv).wait_send()
        send(h2_put.at[rows, :], h2_got.at[rows, :], h2_send.at[chunk_no], h2_recv.at[chunk_no], far).wait_send()
        chunk_copy(e1, chip, chunk_no, e1_send, e1_recv).wait_send()
        return carry

    lax.fori_loop(0, CHUNKS, drain, 0)

    for chunk_no in range(CHUNKS):
        if chunk_no < EARLY:
            h0_copy(chunk_no).wait()
        elif chunk_no < EARLY + MIDDLE:
            late_copy(mid_out, EARLY, chunk_no).wait()
        else:
            late_copy(last_out, EARLY + MIDDLE, chunk_no).wait()
        for copy in (*both_copies(chunk_no), *e0_copies(chunk_no)):
            copy.wait()


def run_chain(x_real, x_fake, weight0, weight1, weight2, u_left0, u_left1, u_left2, t_real, t_fake):
    n_rows, n0 = x_real.shape
    rows1 = weight0.shape[0]
    rows2, n1 = weight1.shape
    wide1, wide2 = 2 * rows1, 2 * rows2
    n2 = 2 * wide2
    step = n_rows // CHUNKS
    early, middle = EARLY * step, MIDDLE * step
    last = n_rows - early - middle
    hbm = pl.BlockSpec(memory_space=pl.ANY)
    vmem = pl.BlockSpec(memory_space=pltpu.VMEM)
    shape = jax.ShapeDtypeStruct
    dma = pltpu.SemaphoreType.DMA
    return pl.pallas_call(
        chain_kernel,
        out_shape=(
            shape((2 * n_rows, n1), BF16), shape((2 * n_rows, n2), BF16), shape((rows2, 2 * n_rows), BF16), shape((rows2, 2 * n_rows), BF16),
            shape((rows1, 2 * n_rows), BF16), shape((early, n0), BF16), shape((middle, n0), BF16), shape((last, n0), BF16), shape((2 * n_rows, n0), BF16),
            shape((1, n0), F32), shape((1, n1), F32), shape((1, n2), F32),
            shape((1, rows1), F32), shape((1, rows2), F32), shape((1, rows2), F32),
            shape((8, 128), F32), shape((4, 8, 128), F32),
        ),
        in_specs=[hbm] * 10,
        out_specs=[hbm] * 17,
        scratch_shapes=[
            pltpu.VMEM((wide1, n0), BF16), pltpu.VMEM((wide2, n1), BF16), pltpu.VMEM((wide2, wide1), BF16), pltpu.VMEM((wide2, n2), BF16),
            pltpu.VMEM((n_rows, n0), BF16), pltpu.VMEM((2, n_rows, wide1), BF16), pltpu.VMEM((2, n_rows, wide2), BF16),
            pltpu.VMEM((n_rows, wide1), F32), pltpu.VMEM((n_rows, wide2), F32), pltpu.VMEM((wide2, n_rows), BF16),
            pltpu.VMEM((wide2, n_rows), BF16), pltpu.VMEM((n_rows, wide2), F32), pltpu.VMEM((n_rows, wide2), BF16), pltpu.VMEM((n_rows, wide2), BF16),
            pltpu.VMEM((2, n_rows, wide2), BF16), pltpu.VMEM((wide2, n_rows), BF16), pltpu.VMEM((n_rows // CHUNKS, wide1), BF16), pltpu.VMEM((wide1, n_rows), BF16),
            pltpu.VMEM((n_rows, n0), BF16),
            pltpu.VMEM((4, 1, n0 + n1 + n2), F32), pltpu.VMEM((2, 1, n0 + n1 + n2), F32), pltpu.VMEM((4, 8, 128), F32), pltpu.VMEM((4, 8, 128), F32), pltpu.VMEM((256, 256), BF16),
            *[pltpu.VMEM(array.shape, F32) for array in (u_left0, u_left1, u_left2)],
            *[pltpu.VMEM((1, size), F32) for size in (n0, n1, n2, rows1, rows2, rows2)], pltpu.VMEM((8, 128), F32), dma((11,)),
            dma((5,)), dma((7,)), dma((4,)), dma((4,)), dma((PIECES,)), dma((PIECES,)), dma((PIECES,)), dma((PIECES,)), dma((9,)), dma((9,)),
            dma((CHUNKS,)), dma((CHUNKS,)), dma((CHUNKS,)), dma((CHUNKS,)), dma((CHUNKS,)), dma((CHUNKS,)),
            dma((CHUNKS,)), dma((CHUNKS,)), dma((EARLY,)), dma((EARLY,)), dma((7,)), dma((7,)),
            dma((CHUNKS,)), dma((CHUNKS,)), dma((CHUNKS,)), dma((CHUNKS,)), dma((CHUNKS,)), dma((CHUNKS,)), dma((CHUNKS,)),
        ],
        compiler_params=pltpu.CompilerParams(collective_id=0, has_side_effects=True, vmem_limit_bytes=67043328),
        name="chain",
    )(x_real, x_fake, weight0, weight1, weight2, u_left0, u_left1, u_left2, t_real.T, t_fake.T)


def grad_kernel(x1_in, e1_in, x2_in, e2_in, x_real, x_fake, e0_in, u0_in, u1_in, u2_in, v0_in, v1_in, v2_in, sig_in, cor_in,
                dw0_out, dw1_out, dw2_out, u0_out, u1_out, u2_out, v0_out, v1_out, v2_out, sig_out, loss_out,
                x1, e1, x2, e2, x0, e0, dw0, dw1, dw2, u0, u1, u2, v0, v1, v2, sig, cor_all, in_sem, x1_sem, out_sem, dw1_sem, dw0_sem):
    n_rows = x_real.shape[0]
    tiles1 = x1_sem.shape[0]
    tiles0 = dw0_sem.shape[0]

    def pull(src, dst, which):
        copy = pltpu.make_async_copy(src, dst, in_sem.at[which])
        copy.start()
        return copy

    small = [pull(src, dst, place) for place, (src, dst) in enumerate((
        (u0_in, u0), (u1_in, u1), (u2_in, u2), (v0_in, v0), (v1_in, v1), (v2_in, v2), (sig_in, sig), (cor_in, cor_all)))]

    def tile_of(size, tiles, tile_no):
        return pl.ds(tile_no * (size // tiles), size // tiles)

    def load(src, dst, which):
        return pltpu.make_async_copy(src, dst, in_sem.at[which])

    got_e1 = pull(e1_in, e1, 11)
    got_x1 = []
    for tile_no in range(tiles1):
        cols = tile_of(x1.shape[1], tiles1, tile_no)
        got_x1.append(pltpu.make_async_copy(x1_in.at[:, cols], x1.at[:, cols], x1_sem.at[tile_no]))
    got_e0 = load(e0_in, e0, 8)
    got_x0 = [load(x_real, x0.at[pl.ds(0, n_rows), :], 9), load(x_fake, x0.at[pl.ds(n_rows, n_rows), :], 10)]
    got_2 = [load(e2_in, e2, 13), load(x2_in, x2, 14)]
    queue = [*got_x1, *got_x0, got_e0, *got_2]

    def read_on(count=1):
        for _ in range(min(count, len(queue))):
            queue.pop(0).start()

    read_on(3)

    for copy in small:
        copy.wait()
    cor = cor_all[0] + cor_all[1] + cor_all[2] + cor_all[3]
    for src, dst in ((u0, u0_out), (u1, u1_out), (u2, u2_out), (v0, v0_out), (v1, v1_out), (v2, v2_out)):
        dst[...] = src[...].reshape(dst.shape)
    sig_out[...] = sig[0:1, 0:3].reshape(3)
    loss_out[...] = cor[0:1, 3:4] * (0.5 / n_rows)

    def column(u_new, layer_no):
        return jnp.broadcast_to(u_new[...] * cor[0:1, layer_no:layer_no + 1], (128, u_new.shape[1])).T[:, 0:1]

    def scale(layer_no):
        return 1.0 / (n_rows * sig[0:1, layer_no:layer_no + 1])

    pushes = []

    def gradient(errors, layer_in, cols, col, v_new, rate, dst, out, sem):
        dst[:, cols] = (dot_n(errors[...], layer_in[:, cols]) - col * v_new[:, cols]) * rate
        copy = pltpu.make_async_copy(dst.at[:, cols], out.at[:, cols], sem)
        copy.start()
        pushes.append(copy)

    got_e1.wait()
    col1, scale1 = column(u1, 1), scale(1)
    for tile_no in range(tiles1):
        got_x1[tile_no].wait()
        read_on()
        gradient(e1, x1, tile_of(x1.shape[1], tiles1, tile_no), col1, v1, scale1, dw1, dw1_out, dw1_sem.at[tile_no])
    got_e0.wait()
    read_on(3)
    for copy in got_x0:
        copy.wait()
    col0, scale0 = column(u0, 0), scale(0)
    for tile_no in range(tiles0):
        gradient(e0, x0, tile_of(x0.shape[1], tiles0, tile_no), col0, v0, scale0, dw0, dw0_out, dw0_sem.at[tile_no])
    for copy in got_2:
        copy.wait()
    col2, scale2 = column(u2, 2), scale(2)
    for tile_no in range(2):
        gradient(e2, x2, tile_of(x2.shape[1], 2, tile_no), col2, v2, scale2, dw2, dw2_out, out_sem.at[2 + tile_no])
    for copy in pushes:
        copy.wait()


def run_grads(x1, e1, x2, e2, x_real, x_fake, e0, u0, u1, u2, v0, v1, v2, sig, cor):
    both, n1 = x1.shape
    _, n0 = x_real.shape
    n2 = x2.shape[1]
    rows2 = e1.shape[0]
    rows1 = e0.shape[0]
    tiles1, tiles0 = 10, 5
    shape = jax.ShapeDtypeStruct
    hbm = pl.BlockSpec(memory_space=pltpu.HBM)
    vmem = pl.BlockSpec(memory_space=pltpu.VMEM)
    dma = pltpu.SemaphoreType.DMA
    flops = 2 * both * (rows2 * (n1 + n2) + rows1 * n0)
    inputs = (x1, e1, x2, e2, x_real, x_fake, e0, u0, u1, u2, v0, v1, v2, sig, cor)
    inputs = tuple(pltpu.with_memory_space_constraint(array, pltpu.HBM) for array in inputs)
    return pl.pallas_call(
        grad_kernel,
        out_shape=(
            shape((rows1, n0), F32), shape((rows2, n1), F32), shape((rows2, n2), F32),
            shape((rows1,), F32), shape((rows2,), F32), shape((rows2,), F32), shape((n0,), F32), shape((n1,), F32), shape((n2,), F32),
            shape((3,), F32), shape((1, 1), F32),
        ),
        in_specs=[hbm] * len(inputs),
        out_specs=[hbm] * 3 + [vmem] * 8,
        scratch_shapes=[
            pltpu.VMEM((both, n1), BF16), pltpu.VMEM((rows2, both), BF16), pltpu.VMEM((both, n2), BF16), pltpu.VMEM((rows2, both), BF16),
            pltpu.VMEM((both, n0), BF16), pltpu.VMEM((rows1, both), BF16),
            pltpu.VMEM((rows1, n0), F32), pltpu.VMEM((rows2, n1), F32), pltpu.VMEM((rows2, n2), F32),
            *[pltpu.VMEM(array.shape, F32) for array in (u0, u1, u2, v0, v1, v2, sig, cor)],
            dma((15,)), dma((tiles1,)), dma((4,)), dma((tiles1,)), dma((tiles0,)),
        ],
        compiler_params=pltpu.CompilerParams(vmem_limit_bytes=48 * 1024 * 1024),
        cost_estimate=pl.CostEstimate(flops=flops, bytes_accessed=45 * 1024 * 1024, transcendentals=0),
        name="grads",
    )(*inputs)


def finish_kernel(plan, in_place, *refs):
    refs = refs[2:] if in_place else refs
    both, sig = refs[:2]
    cames = refs[2:2 + len(plan)]
    real_out, fake_out, dx, out_sem = refs[2 + len(plan):]
    core = lax.axis_index("model") % 2
    n_rows = real_out.shape[0]
    inv0 = 1.0 / sig[0:1, 0:1]
    size = dx.shape[0] // out_sem.shape[0]
    jobs = []
    for came, (flip, first) in zip(cames, plan):
        batch = 1 - core if flip else core
        for begin in range(0, came.shape[0], size):
            jobs.append((came, begin, batch, first + begin))

    def push(dst, place, first):
        return pltpu.make_async_copy(dx.at[pl.ds(place * size, size), :], dst.at[pl.ds(first, size), :], out_sem.at[place])

    for place, (came, begin, batch, first) in enumerate(jobs):
        own = pl.ds(pl.multiple_of(batch * n_rows + first, size), size)
        dx[pl.ds(place * size, size), :] = (both[own, :].astype(F32) + came[pl.ds(begin, size), :].astype(F32)) * inv0

        @pl.when(batch == 0)
        def _():
            push(real_out, place, first).start()

        @pl.when(batch == 1)
        def _():
            push(fake_out, place, first).start()

    for place, (_, _, _, first) in enumerate(jobs):
        push(real_out, place, first).wait()


def run_finish(old, both, sig, parts):
    cames = [came for came, _, _ in parts]
    rows = sum(came.shape[0] for came in cames)
    n0 = both.shape[1]
    size = 64
    hbm = pl.BlockSpec(memory_space=pltpu.HBM)
    vmem = pl.BlockSpec(memory_space=pltpu.VMEM)
    shape = jax.ShapeDtypeStruct((both.shape[0] // 2, n0), F32)
    return pl.pallas_call(
        functools.partial(finish_kernel, tuple((flip, first) for _, flip, first in parts), bool(old)),
        out_shape=(shape, shape),
        in_specs=[hbm] * len(old) + [vmem] * (2 + len(cames)),
        out_specs=[hbm] * 2,
        scratch_shapes=[pltpu.VMEM((rows, n0), F32), pltpu.SemaphoreType.DMA((rows // size,))],
        input_output_aliases={0: 0, 1: 1} if old else {},
        compiler_params=pltpu.CompilerParams(vmem_limit_bytes=16 * 1024 * 1024),
        cost_estimate=pl.CostEstimate(flops=4 * rows * n0, bytes_accessed=8 * rows * n0, transcendentals=0),
        name="finish",
    )(*old, both, sig, *cames)


def swap(values, bits):
    return lax.ppermute(values, "model", [(dev, dev ^ bits) for dev in range(4)])


def solution(mesh):
    rows_spec = P("rep", None)
    weight_spec = P(("rep", "model"), None)
    left_spec = P(("rep", "model"))
    target_spec = P("rep", "model")
    group_spec = P("rep")

    def local_step(x_real, x_fake, weight0, weight1, weight2, u_left0, u_left1, u_left2, t_real, t_fake):
        x1, x2, e2, e1, e0, first, middle, last, both, v0, v1, v2, u0, u1, u2, sig, cor = run_chain(x_real, x_fake, weight0, weight1, weight2, u_left0, u_left1, u_left2, t_real, t_fake)
        row1 = first.shape[0]
        row2 = row1 + middle.shape[0]
        middle = swap(middle, 2)
        last = swap(last, 2)
        first_mate = swap(first, 1)
        grads = run_grads(x1, e1, x2, e2, x_real, x_fake, e0, u0, u1, u2, v0, v1, v2, sig, cor)
        dw0, dw1, dw2, u0, u1, u2, v0, v1, v2, sigmas, loss = grads
        middle, sigmas = lax.optimization_barrier((middle, sigmas))
        middle_mate = swap(middle, 1)
        dx = run_finish((), both, sig, ((first, False, 0), (first_mate, True, 0), (middle, False, row1)))
        dx = run_finish(dx, both, sig, ((middle_mate, True, row1),))
        last, *dx = lax.optimization_barrier((last, *dx))
        last_mate = swap(last, 1)
        dx = run_finish(dx, both, sig, ((last, False, row2),))
        dx_real, dx_fake = run_finish(dx, both, sig, ((last_mate, True, row2),))
        return (loss[0], dx_real, dx_fake, dw0, dw1, dw2, u0, u1, u2, v0, v1, v2, sigmas)

    return jax.shard_map(local_step, mesh=mesh, in_specs=(rows_spec, rows_spec, weight_spec, weight_spec, weight_spec, left_spec, left_spec, left_spec, target_spec, target_spec), out_specs=(group_spec, rows_spec, rows_spec, weight_spec, weight_spec, weight_spec, left_spec, left_spec, left_spec, group_spec, group_spec, group_spec, group_spec), check_vma=False)
```
